32 devices in a mesh: replica: 4 (over y, z), ep: 8 (over x, core).
Axes of the slice: x: 4, y: 2, z: 2, core: 2. Of those that a mesh axis runs over, the one named last changes fastest.
The devices are a block of a 4x4x8 slice.
Arguments:
- x: bfloat16 [32, 1024, 2048], P(('replica', 'ep')), parts along dimension 0
- wq: bfloat16 [2048, 2048], P('ep')
- wk: bfloat16 [2048, 2048], P('ep')
- wv: bfloat16 [2048, 2048], P('ep')
- wo: bfloat16 [2048, 2048], P('ep')
- wr: float32 [2048, 64], replicated
- w1: bfloat16 [64, 2048, 1024], P('ep')
- w3: bfloat16 [64, 2048, 1024], P('ep')
- w2: bfloat16 [64, 1024, 2048], P('ep')
- idx: int32 [32, 1024, 8], P(('replica', 'ep')), parts along dimension 0
Outputs:
- output: bfloat16 [32, 1024, 2048], P(('replica', 'ep')), parts along dimension 0
There are 4 independent parts. The reference program is written for one: setup_inputs(seed, part) draws one part's arguments, and reference() takes and returns one part's arrays. A program takes and returns all parts, laid end to end along the dimension named above; an argument that names none is the same for every part.
All inputs are finite; a program needn't handle non-finite values.
Results may differ from the reference program's by a relative error of at most 0.011257.
Values are sent between devices in bfloat16 or wider.
A program may use at most 768 MiB of HBM per device.

```python
import math
import jax
import jax.numpy as jnp
from jax import lax

D = 2048
HEADS = 16
HEAD = 128
EXPERTS = 64
TOP = 8
FF = 1024
SEQ = 1024
NSEQ = 8
BLOCK = 128

T = NSEQ * SEQ
NHOT = max(1, TOP // 4)
EPS = 1e-6
THETA = 10000.0


def setup_inputs(seed: int = 0, part: int = 0) -> dict:
    key = jax.random.PRNGKey(seed)
    ks = jax.random.split(key, 9)
    kp = jax.random.fold_in(ks[8], part)
    kx, _, _ = jax.random.split(kp, 3)
    kh, kg = jax.random.split(jax.random.fold_in(kp, 7), 2)
    hd = HEADS * HEAD

    def w(k, shape, scale):
        return (jax.random.normal(k, shape, jnp.float32) * scale).astype(jnp.bfloat16)

    x = jax.random.normal(kx, (NSEQ, SEQ, D), jnp.float32).astype(jnp.bfloat16)
    wq = w(ks[0], (D, hd), 1.6 / math.sqrt(D))
    wk = w(ks[1], (D, hd), 1.6 / math.sqrt(D))
    wv = w(ks[2], (D, hd), 1.0 / math.sqrt(D))
    wo = w(ks[3], (hd, D), 1.5 / math.sqrt(hd))
    wr = jax.random.normal(ks[4], (D, EXPERTS), jnp.float32) / math.sqrt(D)
    w1 = w(ks[5], (EXPERTS, D, FF), 1.0 / math.sqrt(D))
    w3 = w(ks[6], (EXPERTS, D, FF), 1.0 / math.sqrt(D))
    w2 = w(ks[7], (EXPERTS, FF, D), 2.0 / math.sqrt(FF))
    nhot = max(1, TOP // 2)
    start = jax.random.randint(kh, (), 0, EXPERTS)
    hot = (start + jnp.arange(nhot)) % EXPERTS
    t = jnp.arange(T)
    int_noise = (jax.random.bits(kg, (T, EXPERTS), jnp.uint32) >> 12).astype(jnp.int32)
    hot_bonus = jnp.zeros((EXPERTS,), jnp.int32).at[hot].set((9 << 20) // 10)
    int_score = (int_noise + hot_bonus).at[t, t % EXPERTS].set(1 << 24)
    int_score = int_score * EXPERTS + jnp.arange(EXPERTS, dtype=jnp.int32)
    idx = lax.top_k(int_score, TOP)[1].astype(jnp.int32).reshape(NSEQ, SEQ, TOP)
    return dict(x=x, wq=wq, wk=wk, wv=wv, wo=wo, wr=wr, w1=w1, w3=w3, w2=w2, idx=idx)


def rmsnorm(v):
    v = v.astype(jnp.float32)
    return v * lax.rsqrt(jnp.mean(v * v, axis=-1, keepdims=True) + EPS)


def rope(z):
    n = z.shape[-3]
    half = HEAD // 2
    freq = THETA ** (-jnp.arange(half, dtype=jnp.float32) / half)
    ang = jnp.arange(n, dtype=jnp.float32)[:, None] * freq
    c = jnp.cos(ang)[:, None, :]
    s = jnp.sin(ang)[:, None, :]
    z1, z2 = z[..., :half], z[..., half:]
    return jnp.concatenate([z1 * c - z2 * s, z2 * c + z1 * s], axis=-1)


def block_plan(eid, ne, cap):
    m = eid.shape[0]
    nb = (cap + ne * (BLOCK - 1)) // BLOCK + 1
    counts = jnp.bincount(eid, length=ne + 1)[:ne]
    nblk = (counts + BLOCK - 1) // BLOCK
    bend = jnp.cumsum(nblk)
    first = jnp.cumsum(counts) - counts
    order = jnp.argsort(eid)
    se = eid[order]
    sc = jnp.minimum(se, ne - 1)
    slot = jnp.where(se < ne, (bend[sc] - nblk[sc]) * BLOCK + jnp.arange(m) - first[sc], nb * BLOCK)
    cand = jnp.full((nb * BLOCK,), m, jnp.int32).at[slot].set(order.astype(jnp.int32), mode='drop')
    blk_e = jnp.minimum(jnp.searchsorted(bend, jnp.arange(nb), side='right'), ne - 1)
    return cand.reshape(nb, BLOCK), blk_e, bend[-1]


def expert_sum(rows, eid, gates, k, w1, w3, w2, cap):
    n, d = rows.shape
    ne = w1.shape[0]
    m = n * k
    cand, blk_e, nused = block_plan(eid, ne, cap)
    ok = cand < m
    row = jnp.where(ok, cand // k, 0)
    gate = jnp.where(ok, gates[jnp.minimum(cand, m - 1)], 0.0)

    def body(acc, xs):
        b, rb, gb, e = xs

        def work(acc):
            xb = rows[rb]
            a1 = jnp.dot(xb, w1[e], preferred_element_type=jnp.float32)
            a3 = jnp.dot(xb, w3[e], preferred_element_type=jnp.float32)
            act = (jax.nn.silu(a1) * a3).astype(jnp.bfloat16)
            o = jnp.dot(act, w2[e], preferred_element_type=jnp.float32).astype(jnp.bfloat16)
            return acc.at[rb].add(gb[:, None] * o.astype(jnp.float32))

        return lax.cond(b < nused, work, lambda acc: acc, acc), None

    acc, _ = lax.scan(body, jnp.zeros((n, d), jnp.float32), (jnp.arange(cand.shape[0]), row, gate, blk_e))
    return acc


def reference(x, wq, wk, wv, wo, wr, w1, w3, w2, idx):
    xf = x.reshape(T, D)
    a = rmsnorm(xf).astype(jnp.bfloat16)

    def proj(w):
        return jnp.dot(a, w, preferred_element_type=jnp.float32).reshape(NSEQ, SEQ, HEADS, HEAD)

    q = rope(proj(wq)).astype(jnp.bfloat16)
    k = rope(proj(wk)).astype(jnp.bfloat16)
    v = proj(wv).astype(jnp.bfloat16)
    causal = jnp.tril(jnp.ones((SEQ, SEQ), bool))

    def one_seq(qkv):
        qs, ks, vs = qkv
        s = jnp.einsum('qhe,khe->hqk', qs.astype(jnp.float32), ks.astype(jnp.float32)) / math.sqrt(HEAD)
        p = jax.nn.softmax(jnp.where(causal, s, -jnp.inf), axis=-1).astype(jnp.bfloat16)
        return jnp.einsum('hqk,khe->qhe', p.astype(jnp.float32), vs.astype(jnp.float32)).astype(jnp.bfloat16)

    o = lax.map(one_seq, (q, k, v))
    ao = jnp.dot(o.reshape(T, HEADS * HEAD), wo, preferred_element_type=jnp.float32)
    h = (xf.astype(jnp.float32) + ao).astype(jnp.bfloat16)
    ids = idx.reshape(T, TOP)
    r = rmsnorm(h)
    logits = jnp.dot(r, wr, precision=lax.Precision.HIGHEST, preferred_element_type=jnp.float32)
    g = jax.nn.softmax(jnp.take_along_axis(logits, ids, axis=1), axis=-1)
    moe = expert_sum(r.astype(jnp.bfloat16), ids.reshape(-1), g.reshape(-1), TOP, w1, w3, w2, T * TOP)
    return (h.astype(jnp.float32) + moe).astype(jnp.bfloat16).reshape(NSEQ, SEQ, D)
```

```python
import functools
import math
import jax
import jax.numpy as jnp
from jax import lax
from jax.experimental import pallas as pl
from jax.experimental.pallas import tpu as pltpu
from jax.sharding import PartitionSpec as P

HEAD = 128
EPS = 1e-6
THETA = 10000.0
PIECE = 16
CHUNK = 256
MT = 384
HM = 256
VMEM = 66_000_000
BF, F32, I32 = jnp.bfloat16, jnp.float32, jnp.int32


def rmsnorm(v):
    v = v.astype(F32)
    return v * lax.rsqrt(jnp.mean(v * v, axis=-1, keepdims=True) + EPS)


def dot(a, b):
    return jnp.dot(a, b, preferred_element_type=F32)


def params(**kw):
    return pltpu.CompilerParams(vmem_limit_bytes=VMEM, **kw)


def proj_kernel(rope, a_ref, w_ref, c_ref, s_ref, o_ref):
    tm = min(512, a_ref.shape[0])

    @pl.loop(0, a_ref.shape[0] // tm)
    def _(i):
        rows = pl.ds(pl.multiple_of(i * tm, tm), tm)
        z = dot(a_ref[rows, :], w_ref[...])
        for j in range(z.shape[1] // HEAD):
            zj = z[:, j * HEAD:(j + 1) * HEAD]
            if rope:
                zj = zj * c_ref[rows, :] + pltpu.roll(zj, HEAD // 2, 1) * s_ref[rows, :]
            o_ref[rows, j * HEAD:(j + 1) * HEAD] = zj.astype(BF)


def proj(a, w, cos, sin, rope):
    t, d = a.shape
    n = w.shape[1]
    tn = min(512, n)
    whole = lambda i: (0, 0)
    return pl.pallas_call(
        functools.partial(proj_kernel, rope),
        grid=(n // tn,),
        in_specs=[pl.BlockSpec((t, d), whole), pl.BlockSpec((d, tn), lambda i: (0, i)),
                  pl.BlockSpec((t, HEAD), whole), pl.BlockSpec((t, HEAD), whole)],
        out_specs=pl.BlockSpec((t, tn), lambda i: (0, i)),
        out_shape=jax.ShapeDtypeStruct((t, n), BF),
        compiler_params=params(),
        cost_estimate=pl.CostEstimate(flops=2 * t * d * n, bytes_accessed=2 * (t * d + d * n + t * n), transcendentals=0),
    )(a, w, cos, sin)


def attn_kernel(tq, q_ref, k_ref, v_ref, o_ref):
    t = q_ref.shape[0]
    scale = 1.0 / math.sqrt(HEAD)
    nt = (((1,), (1,)), ((), ()))
    row = lax.broadcasted_iota(I32, (tq, tq), 0)
    col = lax.broadcasted_iota(I32, (tq, tq), 1)
    for j in range(q_ref.shape[1] // HEAD):
        hs = slice(j * HEAD, (j + 1) * HEAD)
        for i in range(t // tq):
            q = q_ref[i * tq:(i + 1) * tq, hs]
            sd = lax.dot_general(q, k_ref[i * tq:(i + 1) * tq, hs], nt, preferred_element_type=F32)
            sd = jnp.where(col <= row, sd, -jnp.inf)
            m = jnp.max(sd, axis=1, keepdims=True)
            if i:
                so = lax.dot_general(q, k_ref[:i * tq, hs], nt, preferred_element_type=F32)
                m = jnp.maximum(m, jnp.max(so, axis=1, keepdims=True))
            pd = jnp.exp((sd - m) * scale)
            l = jnp.sum(pd, axis=1, keepdims=True)
            if i:
                po = jnp.exp((so - m) * scale)
                l = l + jnp.sum(po, axis=1, keepdims=True)
            inv = 1.0 / l
            o = dot((pd * inv).astype(BF), v_ref[i * tq:(i + 1) * tq, hs])
            if i:
                o = o + dot((po * inv).astype(BF), v_ref[:i * tq, hs])
            o_ref[i * tq:(i + 1) * tq, hs] = o.astype(BF)


def attn(q, k, v):
    t, n = q.shape
    tn = min(256, n)
    spec = pl.BlockSpec((t, tn), lambda i: (0, i))
    return pl.pallas_call(
        functools.partial(attn_kernel, min(256, t)),
        grid=(n // tn,), in_specs=[spec] * 3, out_specs=spec,
        out_shape=jax.ShapeDtypeStruct((t, n), BF),
        compiler_params=params(),
        cost_estimate=pl.CostEstimate(flops=4 * t * t * n, bytes_accessed=8 * t * n, transcendentals=t * t * n // HEAD),
    )(q, k, v)


def wo_kernel(o_ref, w_ref, x_ref, h_ref):
    tm = min(512, o_ref.shape[0])

    @pl.loop(0, o_ref.shape[0] // tm)
    def _(i):
        rows = pl.ds(pl.multiple_of(i * tm, tm), tm)
        h_ref[rows, :] = (x_ref[rows, :].astype(F32) + dot(o_ref[rows, :], w_ref[...])).astype(BF)


def wo_proj(o, w, x):
    t, n = o.shape
    d = w.shape[1]
    tn = min(512, d)
    return pl.pallas_call(
        wo_kernel,
        grid=(d // tn,),
        in_specs=[pl.BlockSpec((t, n), lambda i: (0, 0)), pl.BlockSpec((n, tn), lambda i: (0, i)),
                  pl.BlockSpec((t, tn), lambda i: (0, i))],
        out_specs=pl.BlockSpec((t, tn), lambda i: (0, i)),
        out_shape=jax.ShapeDtypeStruct((t, d), BF),
        compiler_params=params(),
        cost_estimate=pl.CostEstimate(flops=2 * t * d * n, bytes_accessed=2 * (t * n + d * n + 2 * t * d), transcendentals=0),
    )(o, w, x)


def fetch_expert(l, slot, own, other, bufs, sem):
    ne = own[0].shape[0]

    @pl.when(l < ne)
    def _():
        for src, dst in zip(own, bufs):
            pltpu.make_async_copy(src.at[l], dst.at[slot], sem.at[slot]).start()

    @pl.when(l >= ne)
    def _():
        for src, dst in zip(other, bufs):
            pltpu.make_async_copy(src.at[l - ne], dst.at[slot], sem.at[slot]).start()


def wait_expert(slot, own, bufs, sem):
    for src, dst in zip(own, bufs):
        pltpu.make_async_copy(src.at[0], dst.at[slot], sem.at[slot]).wait()


def ffn(x, w1, w3, w2):
    a1 = dot(x, w1)
    a3 = dot(x, w3)
    act = (jax.nn.silu(a1) * a3).astype(BF)
    return dot(act, w2).astype(BF)


def hot_kernel(has_acc, nh_ref, hl_ref, g_ref, ut_ref, ub_ref, *refs):
    if has_acc:
        acc_in, refs = refs[0], refs[1:]
    own, other, (ot_ref, ob_ref), refs = refs[:3], refs[3:6], refs[6:8], refs[8:]
    bufs, (ubuf, acc, sem, usem, asem) = refs[:3], refs[3:]
    half = ut_ref.shape[0]
    nh = nh_ref[0]
    tm = min(HM, half)

    @pl.when(nh > 0)
    def _():
        fetch_expert(hl_ref[0], 0, own, other, bufs, sem)

    ucp = [pltpu.make_async_copy(v, ubuf.at[pl.ds(p * half, half), :], usem) for p, v in enumerate((ut_ref, ub_ref))]
    for cp in ucp:
        cp.start()
    if has_acc:
        acp = pltpu.make_async_copy(acc_in, acc, asem)
        acp.start()
    else:
        acc[...] = jnp.zeros_like(acc)
    for cp in ucp:
        cp.wait()
    if has_acc:
        acp.wait()

    @pl.loop(0, nh)
    def _(i):
        slot = lax.rem(i, 2)
        wait_expert(slot, own, bufs, sem)

        @pl.when(i + 1 < nh)
        def _():
            fetch_expert(hl_ref[i + 1], 1 - slot, own, other, bufs, sem)

        e = hl_ref[i]

        @pl.loop(0, 2 * half // tm)
        def _(m):
            rows = pl.ds(pl.multiple_of(m * tm, tm), tm)
            z = ffn(ubuf[rows, :], bufs[0][slot], bufs[1][slot], bufs[2][slot])
            g = g_ref[rows, :]
            lane = lax.broadcasted_iota(I32, g.shape, 1)
            gc = jnp.sum(jnp.where(lane == e, g, 0.0), axis=1, keepdims=True)
            acc[rows, :] += gc * z.astype(F32)

    ot_ref[...] = acc[:half, :].astype(ot_ref.dtype)
    ob_ref[...] = acc[half:, :].astype(ob_ref.dtype)


def hot(nh, hl, ut, ub, g, acc, own, other, dtype):
    half, d = ut.shape
    ff = own[0].shape[2]
    vm = pl.BlockSpec(memory_space=pltpu.VMEM)
    sm = pl.BlockSpec(memory_space=pltpu.SMEM)
    hb = pl.BlockSpec(memory_space=pl.ANY)
    has = acc is not None
    out = jax.ShapeDtypeStruct((half, d), dtype)
    return pl.pallas_call(
        functools.partial(hot_kernel, has),
        in_specs=[sm, sm, vm] + [hb] * (9 if has else 8),
        out_specs=[vm, vm], out_shape=[out, out],
        scratch_shapes=[pltpu.VMEM((2, d, ff), BF), pltpu.VMEM((2, d, ff), BF), pltpu.VMEM((2, ff, d), BF),
                        pltpu.VMEM((2 * half, d), BF), pltpu.VMEM((2 * half, d), F32),
                        pltpu.SemaphoreType.DMA((2,)), pltpu.SemaphoreType.DMA, pltpu.SemaphoreType.DMA],
        compiler_params=params(),
        cost_estimate=pl.CostEstimate(flops=half * d, bytes_accessed=6 * d * ff, transcendentals=0),
    )(nh, hl, g, ut, ub, *([acc] if has else []), *own, *other)


def split3(g):
    hi = g.astype(BF)
    r = g - hi.astype(F32)
    mid = r.astype(BF)
    lo = (r - mid.astype(F32)).astype(BF)
    return hi, mid, lo


def selection(i, eg_ref, pos_ref, write):
    t = pos_ref.shape[1]
    it = lax.broadcasted_iota(I32, (PIECE, t), 0)

    @pl.loop(0, CHUNK // PIECE)
    def _(p):
        l = eg_ref[i * (CHUNK // PIECE) + p]
        row0 = i * CHUNK + p * PIECE
        write(pl.ds(pl.multiple_of(p * PIECE, PIECE), PIECE), pos_ref[pl.ds(l, 1), :] - row0 == it, l)


def gather_kernel(nch_ref, eg_ref, pos_ref, ut_ref, ub_ref, x_ref, pbuf, xbuf, sem):
    half = ut_ref.shape[0]
    nch = nch_ref[0]

    def out(i, slot):
        return pltpu.make_async_copy(xbuf.at[slot], x_ref.at[pl.ds(pl.multiple_of(i * CHUNK, CHUNK), CHUNK), :], sem.at[slot])

    def put(rows, hit, l):
        pbuf[rows, :] = jnp.where(hit, 1.0, 0.0).astype(BF)

    @pl.loop(0, nch)
    def _(i):
        slot = lax.rem(i, 2)

        @pl.when(i >= 2)
        def _():
            out(i - 2, slot).wait()

        selection(i, eg_ref, pos_ref, put)
        x = dot(pbuf[:, :half], ut_ref[...]) + dot(pbuf[:, half:], ub_ref[...])
        xbuf[slot] = x.astype(BF)
        out(i, slot).start()

    for k in (2, 1):
        @pl.when(nch >= k)
        def _():
            out(nch - k, lax.rem(nch - k, 2)).wait()


def gather(nch, eg, pos, ut, ub):
    half, d = ut.shape
    rows = eg.shape[0] * PIECE
    vm = pl.BlockSpec(memory_space=pltpu.VMEM)
    sm = pl.BlockSpec(memory_space=pltpu.SMEM)
    return pl.pallas_call(
        gather_kernel,
        in_specs=[sm, sm] + [vm] * 3,
        out_specs=pl.BlockSpec(memory_space=pl.ANY),
        out_shape=jax.ShapeDtypeStruct((rows, d), BF),
        scratch_shapes=[pltpu.VMEM((CHUNK, 2 * half), BF), pltpu.VMEM((2, CHUNK, d), BF), pltpu.SemaphoreType.DMA((2,))],
        compiler_params=params(),
        cost_estimate=pl.CostEstimate(flops=2 * CHUNK * half * d, bytes_accessed=4 * CHUNK * d, transcendentals=0),
    )(nch, eg, pos, ut, ub)


def cold_kernel(nb, nt_ref, tl_ref, tp_ref, tn_ref, tw_ref, tf_ref, nx_ref, pc_ref, *refs):
    xs, own, other, zs, refs = refs[:nb], refs[nb:nb + 3], refs[nb + 3:nb + 6], refs[nb + 6:2 * nb + 6], refs[2 * nb + 6:]
    bufs, (xbuf, zbuf, wsem, xsem, zsem) = refs[:3], refs[3:]
    nt = nt_ref[0]
    npb = xs[0].shape[0] // PIECE

    def pieces(q, fn):
        p0, n = tp_ref[q], tn_ref[q]

        @pl.loop(0, n)
        def _(i):
            c = pc_ref[p0 + i]
            for b in range(nb):
                @pl.when(jnp.logical_and(c >= b * npb, c < (b + 1) * npb))
                def _():
                    fn(b, pl.multiple_of((c - b * npb) * PIECE, PIECE), pl.multiple_of(i * PIECE, PIECE))

    def xin(q, slot):
        pieces(q, lambda b, src, dst: pltpu.make_async_copy(
            xs[b].at[pl.ds(src, PIECE), :], xbuf.at[slot, pl.ds(dst, PIECE), :], xsem.at[slot]).start())

    def zout(q, slot):
        pieces(q, lambda b, src, dst: pltpu.make_async_copy(
            zbuf.at[slot, pl.ds(dst, PIECE), :], zs[b].at[pl.ds(src, PIECE), :], zsem.at[slot]).start())

    def xwait(q, slot):
        @pl.loop(0, tn_ref[q])
        def _(i):
            pltpu.make_async_copy(xs[0].at[pl.ds(0, PIECE), :], xbuf.at[slot, pl.ds(0, PIECE), :], xsem.at[slot]).wait()

    def zwait(q, slot):
        @pl.loop(0, tn_ref[q])
        def _(i):
            pltpu.make_async_copy(zbuf.at[slot, pl.ds(0, PIECE), :], zs[0].at[pl.ds(0, PIECE), :], zsem.at[slot]).wait()

    @pl.when(nt > 0)
    def _():
        fetch_expert(tl_ref[0], 0, own, other, bufs, wsem)
        xin(0, 0)

    @pl.loop(0, nt)
    def _(q):
        slot = lax.rem(q, 2)
        ws = lax.rem(tw_ref[q], 2)

        @pl.when(tf_ref[q] == 1)
        def _():
            wait_expert(ws, own, bufs, wsem)

            @pl.when(nx_ref[q] >= 0)
            def _():
                fetch_expert(nx_ref[q], 1 - ws, own, other, bufs, wsem)

        @pl.when(q + 1 < nt)
        def _():
            xin(q + 1, 1 - slot)

        xwait(q, slot)

        @pl.when(q >= 2)
        def _():
            zwait(q - 2, slot)

        zbuf[slot] = ffn(xbuf[slot], bufs[0][ws], bufs[1][ws], bufs[2][ws])
        zout(q, slot)

    for k in (2, 1):
        @pl.when(nt >= k)
        def _():
            zwait(nt - k, lax.rem(nt - k, 2))


def cold(plan, xs, own, other):
    nb = len(xs)
    d, ff = own[0].shape[1:]
    sm = pl.BlockSpec(memory_space=pltpu.SMEM)
    hb = pl.BlockSpec(memory_space=pl.ANY)
    return pl.pallas_call(
        functools.partial(cold_kernel, nb),
        in_specs=[sm] * len(plan) + [hb] * (nb + 6),
        out_specs=[hb] * nb,
        out_shape=[jax.ShapeDtypeStruct(x.shape, BF) for x in xs],
        scratch_shapes=[pltpu.VMEM((2, d, ff), BF), pltpu.VMEM((2, d, ff), BF), pltpu.VMEM((2, ff, d), BF),
                        pltpu.VMEM((2, MT, d), BF), pltpu.VMEM((2, MT, d), BF),
                        pltpu.SemaphoreType.DMA((2,)), pltpu.SemaphoreType.DMA((2,)), pltpu.SemaphoreType.DMA((2,))],
        input_output_aliases={len(plan) + b: b for b in range(nb)},
        compiler_params=params(),
        cost_estimate=pl.CostEstimate(flops=6 * 16 * MT * d * ff, bytes_accessed=96 * d * ff, transcendentals=0),
    )(*plan, *xs, *own, *other)


def combine_kernel(nch_ref, eg_ref, pos_ref, gt_ref, z_ref, acc_ref, cbuf, zbuf, sem):
    t = acc_ref.shape[0]
    nch = nch_ref[0]
    tm = min(256, t)

    def get(i, slot):
        return pltpu.make_async_copy(z_ref.at[pl.ds(pl.multiple_of(i * CHUNK, CHUNK), CHUNK), :], zbuf.at[slot], sem.at[slot])

    def put(rows, hit, l):
        for j, g in enumerate(split3(gt_ref[pl.ds(l, 1), :])):
            cbuf[j, rows, :] = jnp.where(hit, g.astype(F32), 0.0).astype(BF)

    get(0, 0).start()
    acc_ref[...] = jnp.zeros_like(acc_ref)

    @pl.loop(0, nch)
    def _(i):
        slot = lax.rem(i, 2)

        @pl.when(i + 1 < nch)
        def _():
            get(i + 1, 1 - slot).start()

        selection(i, eg_ref, pos_ref, put)
        get(i, slot).wait()

        @pl.loop(0, t // tm)
        def _(m):
            ts = pl.ds(pl.multiple_of(m * tm, tm), tm)
            z = zbuf[slot]
            c = jnp.concatenate([cbuf[j, :, ts] for j in range(3)], axis=0)
            acc_ref[ts, :] += lax.dot_general(c, jnp.concatenate([z, z, z], axis=0), (((0,), (0,)), ((), ())),
                                              preferred_element_type=F32)


def combine(nch, eg, pos, gt, z):
    d = z.shape[1]
    t = pos.shape[1]
    vm = pl.BlockSpec(memory_space=pltpu.VMEM)
    sm = pl.BlockSpec(memory_space=pltpu.SMEM)
    return pl.pallas_call(
        combine_kernel,
        in_specs=[sm, sm, vm, vm, pl.BlockSpec(memory_space=pl.ANY)],
        out_specs=vm,
        out_shape=jax.ShapeDtypeStruct((t, d), F32),
        scratch_shapes=[pltpu.VMEM((3, CHUNK, t), BF), pltpu.VMEM((2, CHUNK, d), BF), pltpu.SemaphoreType.DMA((2,))],
        compiler_params=params(),
        cost_estimate=pl.CostEstimate(flops=t * d, bytes_accessed=4 * CHUNK * d, transcendentals=0),
    )(nch, eg, pos, gt, z)


def routing_plan(lid, local, nl):
    nb, t, k = lid.shape
    le = jnp.arange(nl, dtype=I32)
    hit = jnp.any((lid[:, None] == le[:, None, None]) & local[:, None], axis=-1)
    tri = (jnp.arange(t)[:, None] <= jnp.arange(t)[None, :]).astype(BF)
    rank = lax.dot_general(hit.astype(BF), tri, (((2,), (0,)), ((), ())), preferred_element_type=F32).astype(I32)
    cnt = rank[:, :, -1]
    hotm = cnt >= t // 2
    scnt = jnp.where(hotm, 0, cnt)
    pcs = (scnt + PIECE - 1) // PIECE
    pend = jnp.cumsum(pcs, axis=1)
    base = (pend - pcs) * PIECE
    pos = jnp.where(hit & ~hotm[..., None], base[..., None] + rank - 1, -1)
    rows = t * k + nl * PIECE
    npb = -(-rows // CHUNK) * CHUNK // PIECE
    nch = jnp.maximum(-(-pend[:, -1] * PIECE // CHUNK), 1)
    below = lambda ends, q: jnp.sum((ends <= q).astype(I32), axis=-1)
    eg = jnp.minimum(below(pend[:, None, :], jnp.arange(npb, dtype=I32)[None, :, None]), nl - 1)
    flat = pcs.T.reshape(-1)
    fend = jnp.cumsum(flat)
    p = jnp.arange(nb * npb, dtype=I32)[:, None]
    seg = jnp.minimum(below(fend[None, :], p), nl * nb - 1)
    inseg = seg[:, None] == jnp.arange(nl * nb, dtype=I32)
    shift_ = jnp.tile(jnp.arange(nb, dtype=I32) * npb, nl) + (pend - pcs).T.reshape(-1) - (fend - flat)
    pc = jnp.clip(p[:, 0] + jnp.sum(jnp.where(inseg, shift_, 0), axis=1), 0, nb * npb - 1)
    ppt = MT // PIECE
    ptot = jnp.sum(pcs, axis=0)
    pstart = jnp.cumsum(ptot) - ptot
    tiles = (ptot + ppt - 1) // ppt
    tend = jnp.cumsum(tiles)
    nq = -(-(nb * npb) // ppt) + nl
    q = jnp.arange(nq, dtype=I32)
    tl = jnp.minimum(below(tend[None, :], q[:, None]), nl - 1)
    one = tl[:, None] == le
    pick = lambda v: jnp.sum(jnp.where(one, v[None, :], 0), axis=1)
    ti = q - pick(tend - tiles)
    tp = pick(pstart) + ti * ppt
    tn = jnp.clip(pick(ptot) - ti * ppt, 0, ppt)
    active = (tiles > 0).astype(I32)
    tw = pick(jnp.cumsum(active) - active)
    tf = (ti == 0).astype(I32)
    later = (le[None, :] > tl[:, None]) & (active[None, :] > 0)
    nxt = jnp.min(jnp.where(later, le[None, :], nl), axis=1)
    nxt = jnp.where(nxt < nl, nxt, -1)
    plan = tuple(v.astype(I32) for v in (tend[-1:], tl, tp, tn, tw, tf, nxt, pc))
    hend = jnp.cumsum(hotm.astype(I32), axis=1)
    hl = jnp.minimum(below(hend[:, None, :], le[None, :, None]), nl - 1)
    return hend[:, -1], hl, nch, eg, pos, plan


def solution(mesh):
    nd = mesh.shape['ep']
    nx = nd // 2
    tok_spec = P(('replica', 'ep'), None, None)
    rows_ep = P('ep', None)
    by_expert = P('ep', None, None)

    def shift(v, s):
        return lax.ppermute(v, 'ep', [(2 * i + c, 2 * ((i + s) % nx) + c) for i in range(nx) for c in range(2)])

    def partner(v):
        return lax.ppermute(v, 'ep', [(i, i ^ 1) for i in range(nd)])

    def local(x, wq, wk, wv, wo, wr, w1, w3, w2, idx):
        b, s, d = x.shape
        t, k, ne = b * s, idx.shape[-1], w1.shape[0]
        nl = 2 * ne
        half = t // 2
        me = lax.axis_index('ep')
        x = x.reshape(t, d)
        ids = idx.reshape(t, k)

        wq, wk, wv, wo = [lax.all_gather(w, 'ep', axis=0, tiled=True) for w in (wq, wk, wv, wo)]
        own = (w1, w3, w2)
        other = tuple(partner(w) for w in own)

        ids4 = jnp.stack([ids, shift(ids, 1), shift(ids, -1), shift(ids, 2)])
        is_local = ids4 // nl == me // 2
        lid = (ids4 - me * ne) % nl
        nh, hl, nch, eg, pos, plan = routing_plan(lid, is_local, nl)

        hd = HEAD // 2
        freq = THETA ** (-jnp.arange(hd, dtype=F32) / hd)
        ang = (jnp.arange(t) % s).astype(F32)[:, None] * freq
        c, sn = jnp.cos(ang), jnp.sin(ang)
        cos, sin = jnp.concatenate([c, c], axis=1), jnp.concatenate([-sn, sn], axis=1)
        a = rmsnorm(x).astype(BF)
        q = proj(a, wq, cos, sin, True)
        kk = proj(a, wk, cos, sin, True)
        v = proj(a, wv, cos, sin, False)
        o = attn(q, kk, v)
        h = wo_proj(o, wo, x)

        r = rmsnorm(h)
        logits = jnp.dot(r, wr, precision=lax.Precision.HIGHEST, preferred_element_type=F32)
        oh = ids[..., None] == jnp.arange(wr.shape[1], dtype=I32)
        g = jax.nn.softmax(jnp.sum(jnp.where(oh, logits[:, None, :], 0.0), axis=-1), axis=-1)
        u = r.astype(BF)

        ut, ub = u[:half], u[half:]
        u1t, u2b = shift(ut, 1), shift(ub, -1)
        u1b, u2t = shift(ub, 1), shift(ut, -1)
        g4 = jnp.stack([g, shift(g, 1), shift(g, -1), shift(g, 2)])
        ohl = (lid[:, None] == jnp.arange(nl, dtype=I32)[:, None, None]) & is_local[:, None]
        gt = jnp.sum(jnp.where(ohl, g4[:, None], 0.0), axis=3)
        gd = jnp.swapaxes(gt, 1, 2)

        acc0 = hot(nh[0:1], hl[0], ut, ub, gd[0], None, own, other, F32)
        x0 = gather(nch[0:1], eg[0], pos[0], ut, ub)
        acc0, x0, u1t, u2b = lax.optimization_barrier((acc0, x0, u1t, u2b))
        u3t, u3b = shift(u1t, 1), shift(u2b, -1)
        us = [(ut, ub), (u1t, u1b), (u2t, u2b), (u3t, u3b)]
        xg = [x0] + [gather(nch[j:j + 1], eg[j], pos[j], *us[j]) for j in range(1, 4)]
        z = cold(plan, xg, own, other)

        def part(j, pj):
            accj = combine(nch[j:j + 1], eg[j], pj, gt[j], z[j])
            return hot(nh[j:j + 1], hl[j], *us[j], gd[j], accj, own, other, BF)

        b3t, b3b = part(3, pos[3])
        p1, b3t, b3b = lax.optimization_barrier((pos[1], b3t, b3b))
        r3t, r3b = shift(b3t, 1), shift(b3b, -1)
        b1 = part(1, p1)
        p2, b1, r3t, r3b = lax.optimization_barrier((pos[2], b1, r3t, r3b))
        r1 = [shift(v, -1) for v in b1]
        r3 = [shift(r3t, 1), shift(r3b, -1)]
        b2 = part(2, p2)
        p0, b2 = lax.optimization_barrier((pos[0], b2))
        r2 = [shift(v, 1) for v in b2]
        acc1 = combine(nch[0:1], eg[0], p0, gt[0], z[0])
        ys = []
        for p in range(2):
            rs = slice(p * half, (p + 1) * half)
            y = h[rs].astype(F32) + acc0[p] + acc1[rs]
            for v in (r1[p], r2[p], r3[p]):
                y = y + v.astype(F32)
            ys.append(y.astype(BF))
        return jnp.concatenate(ys, axis=0).reshape(b, s, d)

    return jax.shard_map(local, mesh=mesh,
                         in_specs=(tok_spec, rows_ep, rows_ep, rows_ep, rows_ep, P(None, None),
                                   by_expert, by_expert, by_expert, tok_spec),
                         out_specs=tok_spec, check_vma=False)
```

```python
import functools
import math
import typing
import jax
import jax.numpy as jnp
from jax import lax
from jax.experimental import pallas as pl
from jax.experimental.pallas import tpu as pltpu
from jax.sharding import PartitionSpec as P

HEAD = 128
EPS = 1e-6
THETA = 10000.0
PIECE = 16
CHUNK = 256
MT = 416
HM = 256
VMEM = 66_000_000
BF, F32, I32 = jnp.bfloat16, jnp.float32, jnp.int32


def rmsnorm(v):
    v = v.astype(F32)
    return v * lax.rsqrt(jnp.mean(v * v, axis=-1, keepdims=True) + EPS)


def dot(a, b):
    return jnp.dot(a, b, preferred_element_type=F32)


def params(**kw):
    return pltpu.CompilerParams(vmem_limit_bytes=VMEM, **kw)


def proj_kernel(rope, a_ref, w_ref, c_ref, s_ref, o_ref):
    tm = min(512, a_ref.shape[0])

    @pl.loop(0, a_ref.shape[0] // tm)
    def _(i):
        rows = pl.ds(pl.multiple_of(i * tm, tm), tm)
        z = dot(a_ref[rows, :], w_ref[...])
        for j in range(z.shape[1] // HEAD):
            zj = z[:, j * HEAD:(j + 1) * HEAD]
            if rope:
                zj = zj * c_ref[rows, :] + pltpu.roll(zj, HEAD // 2, 1) * s_ref[rows, :]
            o_ref[rows, j * HEAD:(j + 1) * HEAD] = zj.astype(BF)


def proj(a, w, cos, sin, rope):
    t, d = a.shape
    n = w.shape[1]
    tn = min(512, n)
    whole = lambda i: (0, 0)
    return pl.pallas_call(
        functools.partial(proj_kernel, rope),
        grid=(n // tn,),
        in_specs=[pl.BlockSpec((t, d), whole), pl.BlockSpec((d, tn), lambda i: (0, i)),
                  pl.BlockSpec((t, HEAD), whole), pl.BlockSpec((t, HEAD), whole)],
        out_specs=pl.BlockSpec((t, tn), lambda i: (0, i)),
        out_shape=jax.ShapeDtypeStruct((t, n), BF),
        compiler_params=params(),
        cost_estimate=pl.CostEstimate(flops=2 * t * d * n, bytes_accessed=2 * (t * d + d * n + t * n), transcendentals=0),
    )(a, w, cos, sin)


def attn_kernel(tq, q_ref, k_ref, v_ref, o_ref):
    t = q_ref.shape[0]
    scale = 1.0 / math.sqrt(HEAD)
    nt = (((1,), (1,)), ((), ()))
    row = lax.broadcasted_iota(I32, (tq, tq), 0)
    col = lax.broadcasted_iota(I32, (tq, tq), 1)
    for j in range(q_ref.shape[1] // HEAD):
        hs = slice(j * HEAD, (j + 1) * HEAD)
        for i in range(t // tq):
            q = q_ref[i * tq:(i + 1) * tq, hs]
            sd = lax.dot_general(q, k_ref[i * tq:(i + 1) * tq, hs], nt, preferred_element_type=F32)
            sd = jnp.where(col <= row, sd, -jnp.inf)
            m = jnp.max(sd, axis=1, keepdims=True)
            if i:
                so = lax.dot_general(q, k_ref[:i * tq, hs], nt, preferred_element_type=F32)
                m = jnp.maximum(m, jnp.max(so, axis=1, keepdims=True))
            pd = jnp.exp((sd - m) * scale)
            l = jnp.sum(pd, axis=1, keepdims=True)
            if i:
                po = jnp.exp((so - m) * scale)
                l = l + jnp.sum(po, axis=1, keepdims=True)
            inv = 1.0 / l
            o = dot((pd * inv).astype(BF), v_ref[i * tq:(i + 1) * tq, hs])
            if i:
                o = o + dot((po * inv).astype(BF), v_ref[:i * tq, hs])
            o_ref[i * tq:(i + 1) * tq, hs] = o.astype(BF)


def attn(q, k, v):
    t, n = q.shape
    tn = min(256, n)
    spec = pl.BlockSpec((t, tn), lambda i: (0, i))
    return pl.pallas_call(
        functools.partial(attn_kernel, min(256, t)),
        grid=(n // tn,), in_specs=[spec] * 3, out_specs=spec,
        out_shape=jax.ShapeDtypeStruct((t, n), BF),
        compiler_params=params(),
        cost_estimate=pl.CostEstimate(flops=4 * t * t * n, bytes_accessed=8 * t * n, transcendentals=t * t * n // HEAD),
    )(q, k, v)


def wo_kernel(o_ref, w_ref, x_ref, h_ref):
    tm = min(512, o_ref.shape[0])

    @pl.loop(0, o_ref.shape[0] // tm)
    def _(i):
        rows = pl.ds(pl.multiple_of(i * tm, tm), tm)
        h_ref[rows, :] = (x_ref[rows, :].astype(F32) + dot(o_ref[rows, :], w_ref[...])).astype(BF)


def wo_proj(o, w, x):
    t, n = o.shape
    d = w.shape[1]
    tn = min(512, d)
    return pl.pallas_call(
        wo_kernel,
        grid=(d // tn,),
        in_specs=[pl.BlockSpec((t, n), lambda i: (0, 0)), pl.BlockSpec((n, tn), lambda i: (0, i)),
                  pl.BlockSpec((t, tn), lambda i: (0, i))],
        out_specs=pl.BlockSpec((t, tn), lambda i: (0, i)),
        out_shape=jax.ShapeDtypeStruct((t, d), BF),
        compiler_params=params(),
        cost_estimate=pl.CostEstimate(flops=2 * t * d * n, bytes_accessed=2 * (t * n + d * n + 2 * t * d), transcendentals=0),
    )(o, w, x)


def fetch_expert(l, slot, own, other, bufs, sem):
    ne = own[0].shape[0]

    @pl.when(l < ne)
    def _():
        for src, dst in zip(own, bufs):
            pltpu.make_async_copy(src.at[l], dst.at[slot], sem.at[slot]).start()

    @pl.when(l >= ne)
    def _():
        for src, dst in zip(other, bufs):
            pltpu.make_async_copy(src.at[l - ne], dst.at[slot], sem.at[slot]).start()


def wait_expert(slot, own, bufs, sem):
    for src, dst in zip(own, bufs):
        pltpu.make_async_copy(src.at[0], dst.at[slot], sem.at[slot]).wait()


def ffn(x, w1, w3, w2):
    a1 = dot(x, w1)
    a3 = dot(x, w3)
    act = (jax.nn.silu(a1) * a3).astype(BF)
    return dot(act, w2).astype(BF)


def block_kernel(js, has_acc, comb, dense, *refs):
    refs = list(refs)
    nblk = len(js)
    take = lambda n: [refs.pop(0) for _ in range(n)]
    if dense:
        n_ref, ent_ref = take(2)
    gt_ref, = take(1)
    if comb:
        nch_ref, eg_ref, pos_ref, z_ref = take(4)
        cap = z_ref.shape[0] // pos_ref.shape[0]
    if dense:
        us = take(nblk)
        own, other = take(3), take(3)
        nl = 2 * own[0].shape[0]
    accs = [take(1)[0] if h else None for h in has_acc]
    outs = take(nblk)
    acc, asem = take(2)
    if comb:
        cbuf, zbuf, zsem = take(3)
    if dense:
        bufs, (ubuf, sem, usem) = take(3), take(3)
    t, d = outs[0].shape

    if dense:
        n = n_ref[0]

        @pl.when(n > 0)
        def _():
            fetch_expert(lax.rem(ent_ref[0], nl), 0, own, other, bufs, sem)

        ucp = [pltpu.make_async_copy(us[p], ubuf.at[pl.ds(p * t, t), :], usem) for p in range(nblk)]
        for cp in ucp:
            cp.start()
    for p in range(nblk):
        rows = pl.ds(p * t, t)
        if has_acc[p]:
            pltpu.make_async_copy(accs[p], acc.at[rows, :], asem.at[p]).start()
        else:
            acc[rows, :] = jnp.zeros((t, d), F32)
    for p in range(nblk):
        if has_acc[p]:
            pltpu.make_async_copy(accs[p], acc.at[pl.ds(p * t, t), :], asem.at[p]).wait()

    if comb:
        for p, j in enumerate(js):
            nch = nch_ref[j]

            def get(i, slot):
                src = pl.multiple_of(j * cap + i * CHUNK, CHUNK)
                return pltpu.make_async_copy(z_ref.at[pl.ds(src, CHUNK), :], zbuf.at[slot], zsem.at[slot])

            get(0, 0).start()

            @pl.loop(0, nch)
            def _(i):
                slot = lax.rem(i, 2)

                @pl.when(i + 1 < nch)
                def _():
                    get(i + 1, 1 - slot).start()

                for q, (hit, l) in enumerate(selection(j, i, eg_ref, pos_ref)):
                    for k, g in enumerate(split3(gt_ref[j, pl.ds(l, 1), :])):
                        cbuf[pl.ds(k * CHUNK + q * PIECE, PIECE), :] = jnp.where(hit, g.astype(F32), 0.0).astype(BF)
                get(i, slot).wait()
                tn = min(1024, d)

                @pl.loop(0, d // tn)
                def _(m):
                    cs = pl.ds(pl.multiple_of(m * tn, tn), tn)
                    z = zbuf[slot, :, cs]
                    acc[p * t:(p + 1) * t, cs] += lax.dot_general(
                        cbuf[...], jnp.concatenate([z, z, z], axis=0), (((0,), (0,)), ((), ())), preferred_element_type=F32)

    if dense:
        for cp in ucp:
            cp.wait()
        tm = min(HM, t)

        @pl.loop(0, n)
        def _(i):
            slot = lax.rem(i, 2)
            wait_expert(slot, own, bufs, sem)

            @pl.when(i + 1 < n)
            def _():
                fetch_expert(lax.rem(ent_ref[i + 1], nl), 1 - slot, own, other, bufs, sem)

            e = lax.rem(ent_ref[i], nl)
            p = lax.div(ent_ref[i], nl)
            blk = jnp.where(p == 0, js[0], js[-1])

            @pl.loop(0, t // tm)
            def _(m):
                rows = pl.ds(pl.multiple_of(p * t + m * tm, tm), tm)
                z = ffn(ubuf[rows, :], bufs[0][slot], bufs[1][slot], bufs[2][slot])
                g = gt_ref[blk, pl.ds(e, 1), pl.ds(pl.multiple_of(m * tm, tm), tm)]
                eye = lax.broadcasted_iota(I32, (tm, tm), 0) == lax.broadcasted_iota(I32, (tm, tm), 1)
                gc = jnp.sum(jnp.where(eye, g, 0.0), axis=1, keepdims=True)
                acc[rows, :] += gc * z.astype(F32)

    for p in range(nblk):
        outs[p][...] = acc[p * t:(p + 1) * t, :].astype(outs[p].dtype)


def block(js, r, z, us, accs, own, other, dtype, comb=True, ents=None):
    nblk = len(js)
    t = r.pos.shape[2]
    d = own[0].shape[1]
    ff = own[0].shape[2]
    dense = ents is not None
    vm = pl.BlockSpec(memory_space=pltpu.VMEM)
    sm = pl.BlockSpec(memory_space=pltpu.SMEM)
    hb = pl.BlockSpec(memory_space=pl.ANY)
    args, specs, scratch = [], [], []
    if dense:
        args += list(ents)
        specs += [sm, sm]
    args += [r.gt]
    specs += [vm]
    if comb:
        args += [r.nch, r.eg.reshape(-1), r.pos, z]
        specs += [sm, sm, vm, hb]
    if dense:
        args += list(us) + list(own) + list(other)
        specs += [hb] * (nblk + 6)
    args += [v for v in accs if v is not None]
    specs += [hb for v in accs if v is not None]
    scratch += [pltpu.VMEM((nblk * t, d), F32), pltpu.SemaphoreType.DMA((nblk,))]
    if comb:
        scratch += [pltpu.VMEM((3 * CHUNK, t), BF), pltpu.VMEM((2, CHUNK, d), BF), pltpu.SemaphoreType.DMA((2,))]
    if dense:
        scratch += [pltpu.VMEM((2, d, ff), BF), pltpu.VMEM((2, d, ff), BF), pltpu.VMEM((2, ff, d), BF),
                    pltpu.VMEM((nblk * t, d), BF), pltpu.SemaphoreType.DMA((2,)), pltpu.SemaphoreType.DMA]
    out = jax.ShapeDtypeStruct((t, d), dtype)
    return pl.pallas_call(
        functools.partial(block_kernel, js, [v is not None for v in accs], comb, dense),
        in_specs=specs, out_specs=[vm] * nblk, out_shape=[out] * nblk, scratch_shapes=scratch,
        compiler_params=params(),
        cost_estimate=pl.CostEstimate(flops=t * d, bytes_accessed=6 * d * ff, transcendentals=0),
    )(*args)


def split3(g):
    hi = g.astype(BF)
    r = g - hi.astype(F32)
    mid = r.astype(BF)
    lo = (r - mid.astype(F32)).astype(BF)
    return hi, mid, lo


def selection(j, i, eg_ref, pos_ref):
    t = pos_ref.shape[2]
    it = lax.broadcasted_iota(I32, (PIECE, t), 0)
    npc = CHUNK // PIECE
    npb = eg_ref.shape[0] // pos_ref.shape[0]
    for q in range(npc):
        l = eg_ref[j * npb + i * npc + q]
        yield pos_ref[j, pl.ds(l, 1), :] - (i * CHUNK + q * PIECE) == it, l


def gather_kernel(js, nch_ref, eg_ref, pos_ref, *refs):
    us = refs[:len(js)]
    x_ref, xbuf, sem = refs[-3:]
    cap = x_ref.shape[0] // pos_ref.shape[0]
    for p, j in enumerate(js):
        nch = nch_ref[j]

        def out(i, slot):
            dst = pl.multiple_of(j * cap + i * CHUNK, CHUNK)
            return pltpu.make_async_copy(xbuf.at[slot], x_ref.at[pl.ds(dst, CHUNK), :], sem.at[slot])

        @pl.loop(0, nch)
        def _(i):
            slot = lax.rem(i, 2)

            @pl.when(i >= 2)
            def _():
                out(i - 2, slot).wait()

            pm = jnp.concatenate([jnp.where(hit, 1.0, 0.0).astype(BF) for hit, _ in selection(j, i, eg_ref, pos_ref)], axis=0)
            xbuf[slot] = dot(pm, us[p][...]).astype(BF)
            out(i, slot).start()

        for k in (2, 1):
            @pl.when(nch >= k)
            def _():
                out(nch - k, lax.rem(nch - k, 2)).wait()


def gather(js, r, us, x):
    nblk = len(js)
    t, d = us[0].shape
    nb = r.eg.shape[0]
    cap = r.eg.shape[1] * PIECE
    vm = pl.BlockSpec(memory_space=pltpu.VMEM)
    sm = pl.BlockSpec(memory_space=pltpu.SMEM)
    hb = pl.BlockSpec(memory_space=pl.ANY)
    return pl.pallas_call(
        functools.partial(gather_kernel, js),
        in_specs=[sm, sm, vm] + [vm] * nblk + ([hb] if x is not None else []),
        out_specs=hb,
        out_shape=jax.ShapeDtypeStruct((nb * cap, d), BF),
        input_output_aliases={3 + nblk: 0} if x is not None else {},
        scratch_shapes=[pltpu.VMEM((2, CHUNK, d), BF), pltpu.SemaphoreType.DMA((2,))],
        compiler_params=params(),
        cost_estimate=pl.CostEstimate(flops=t * d, bytes_accessed=4 * CHUNK * d, transcendentals=0),
    )(r.nch, r.eg.reshape(-1), r.pos, *us, *([x] if x is not None else []))


def cold_kernel(nt_ref, tl_ref, tp_ref, tn_ref, tw_ref, tf_ref, nx_ref, pc_ref, x_ref, *refs):
    own, other, z_ref, refs = refs[:3], refs[3:6], refs[6], refs[7:]
    bufs, (xbuf, zbuf, wsem, xsem, zsem) = refs[:3], refs[3:]
    nt = nt_ref[0]

    def xin(q, slot):
        p0 = tp_ref[q]

        @pl.loop(0, tn_ref[q])
        def _(i):
            src = pl.ds(pl.multiple_of(pc_ref[p0 + i] * PIECE, PIECE), PIECE)
            dst = pl.ds(pl.multiple_of(i * PIECE, PIECE), PIECE)
            pltpu.make_async_copy(x_ref.at[src, :], xbuf.at[slot, dst, :], xsem.at[slot]).start()

    def zout(q, slot):
        p0 = tp_ref[q]

        @pl.loop(0, tn_ref[q])
        def _(i):
            src = pl.ds(pl.multiple_of(i * PIECE, PIECE), PIECE)
            dst = pl.ds(pl.multiple_of(pc_ref[p0 + i] * PIECE, PIECE), PIECE)
            pltpu.make_async_copy(zbuf.at[slot, src, :], z_ref.at[dst, :], zsem.at[slot]).start()

    def xwait(q, slot):
        @pl.loop(0, tn_ref[q])
        def _(i):
            pltpu.make_async_copy(x_ref.at[pl.ds(0, PIECE), :], xbuf.at[slot, pl.ds(0, PIECE), :], xsem.at[slot]).wait()

    def zwait(q, slot):
        @pl.loop(0, tn_ref[q])
        def _(i):
            pltpu.make_async_copy(zbuf.at[slot, pl.ds(0, PIECE), :], z_ref.at[pl.ds(0, PIECE), :], zsem.at[slot]).wait()

    @pl.when(nt > 0)
    def _():
        fetch_expert(tl_ref[0], 0, own, other, bufs, wsem)
        xin(0, 0)

    @pl.loop(0, nt)
    def _(q):
        slot = lax.rem(q, 2)
        ws = lax.rem(tw_ref[q], 2)

        @pl.when(tf_ref[q] == 1)
        def _():
            wait_expert(ws, own, bufs, wsem)

            @pl.when(nx_ref[q] >= 0)
            def _():
                fetch_expert(nx_ref[q], 1 - ws, own, other, bufs, wsem)

        @pl.when(q + 1 < nt)
        def _():
            xin(q + 1, 1 - slot)

        xwait(q, slot)

        @pl.when(q >= 2)
        def _():
            zwait(q - 2, slot)

        zbuf[slot] = ffn(xbuf[slot], bufs[0][ws], bufs[1][ws], bufs[2][ws])
        zout(q, slot)

    for k in (2, 1):
        @pl.when(nt >= k)
        def _():
            zwait(nt - k, lax.rem(nt - k, 2))


def cold(plan, x, own, other):
    d, ff = own[0].shape[1:]
    sm = pl.BlockSpec(memory_space=pltpu.SMEM)
    hb = pl.BlockSpec(memory_space=pl.ANY)
    return pl.pallas_call(
        cold_kernel,
        in_specs=[sm] * len(plan) + [hb] * 7,
        out_specs=hb,
        out_shape=jax.ShapeDtypeStruct(x.shape, BF),
        scratch_shapes=[pltpu.VMEM((2, d, ff), BF), pltpu.VMEM((2, d, ff), BF), pltpu.VMEM((2, ff, d), BF),
                        pltpu.VMEM((2, MT, d), BF), pltpu.VMEM((2, MT, d), BF),
                        pltpu.SemaphoreType.DMA((2,)), pltpu.SemaphoreType.DMA((2,)), pltpu.SemaphoreType.DMA((2,))],
        input_output_aliases={len(plan): 0},
        compiler_params=params(),
        cost_estimate=pl.CostEstimate(flops=6 * 16 * MT * d * ff, bytes_accessed=96 * d * ff, transcendentals=0),
    )(*plan, x, *own, *other)


def final_kernel(h_ref, *refs):
    y_ref = refs[-1]
    acc, parts = refs[0], refs[1:-1]
    y = h_ref[...].astype(F32) + acc[...]
    for v in parts:
        y = y + v[...].astype(F32)
    y_ref[...] = y.astype(BF)


def final(h, accs, parts):
    t, d = h.shape
    half = t // 2
    tm = min(128, half)
    n = half // tm

    def body(h_ref, *refs):
        for p in range(2):
            @pl.when(pl.program_id(0) // n == p)
            def _():
                final_kernel(h_ref, refs[p], *refs[2 + p:-1:2], refs[-1])

    spec = lambda p: pl.BlockSpec((tm, d), lambda i: (jnp.minimum(i, n - 1) if p == 0 else jnp.maximum(i - n, 0), 0))
    return pl.pallas_call(
        body, grid=(2 * n,),
        in_specs=[pl.BlockSpec((tm, d), lambda i: (i, 0))] + [spec(0), spec(1)] * (1 + len(parts)),
        out_specs=pl.BlockSpec((tm, d), lambda i: (i, 0)),
        out_shape=jax.ShapeDtypeStruct((t, d), BF),
        compiler_params=params(),
        cost_estimate=pl.CostEstimate(flops=6 * t * d, bytes_accessed=20 * t * d, transcendentals=0),
    )(h, *accs, *[v for part in parts for v in part])


def entries(nh, hl):
    nblk, nl = hl.shape
    end = jnp.cumsum(nh)
    i = jnp.arange(nblk * nl, dtype=I32)
    p = jnp.minimum(jnp.sum((end[None, :] <= i[:, None]).astype(I32), axis=1), nblk - 1)
    mine = p[:, None] == jnp.arange(nblk)
    k = i - jnp.sum(jnp.where(mine, (end - nh)[None, :], 0), axis=1)
    row = jnp.sum(jnp.where(mine[..., None], hl[None], 0), axis=1)
    e = jnp.sum(jnp.where(jnp.arange(nl)[None, :] == k[:, None], row, 0), axis=1)
    return end[-1:].astype(I32), (p * nl + e).astype(I32)


class Routing(typing.NamedTuple):
    nh: typing.Any
    hl: typing.Any
    nch: typing.Any
    eg: typing.Any
    pos: typing.Any
    gt: typing.Any


def routing_plan(lid, local, nl):
    nb, t, k = lid.shape
    le = jnp.arange(nl, dtype=I32)
    hit = jnp.any((lid[:, None] == le[:, None, None]) & local[:, None], axis=-1)
    tri = (jnp.arange(t)[:, None] <= jnp.arange(t)[None, :]).astype(BF)
    rank = lax.dot_general(hit.astype(BF), tri, (((2,), (0,)), ((), ())), preferred_element_type=F32).astype(I32)
    cnt = rank[:, :, -1]
    hotm = cnt >= t // 2
    scnt = jnp.where(hotm, 0, cnt)
    pcs = (scnt + PIECE - 1) // PIECE
    pend = jnp.cumsum(pcs, axis=1)
    base = (pend - pcs) * PIECE
    pos = jnp.where(hit & ~hotm[..., None], base[..., None] + rank - 1, -1)
    rows = t * k + nl * PIECE
    npb = -(-rows // CHUNK) * CHUNK // PIECE
    nch = jnp.maximum(-(-pend[:, -1] * PIECE // CHUNK), 1)
    below = lambda ends, q: jnp.sum((ends <= q).astype(I32), axis=-1)
    eg = jnp.minimum(below(pend[:, None, :], jnp.arange(npb, dtype=I32)[None, :, None]), nl - 1)
    flat = pcs.T.reshape(-1)
    fend = jnp.cumsum(flat)
    p = jnp.arange(nb * npb, dtype=I32)[:, None]
    seg = jnp.minimum(below(fend[None, :], p), nl * nb - 1)
    inseg = seg[:, None] == jnp.arange(nl * nb, dtype=I32)
    shift_ = jnp.tile(jnp.arange(nb, dtype=I32) * npb, nl) + (pend - pcs).T.reshape(-1) - (fend - flat)
    pc = jnp.clip(p[:, 0] + jnp.sum(jnp.where(inseg, shift_, 0), axis=1), 0, nb * npb - 1)
    ppt = MT // PIECE
    ptot = jnp.sum(pcs, axis=0)
    pstart = jnp.cumsum(ptot) - ptot
    tiles = (ptot + ppt - 1) // ppt
    tend = jnp.cumsum(tiles)
    nq = -(-(nb * npb) // ppt) + nl
    q = jnp.arange(nq, dtype=I32)
    tl = jnp.minimum(below(tend[None, :], q[:, None]), nl - 1)
    one = tl[:, None] == le
    pick = lambda v: jnp.sum(jnp.where(one, v[None, :], 0), axis=1)
    ti = q - pick(tend - tiles)
    tp = pick(pstart) + ti * ppt
    tn = jnp.clip(pick(ptot) - ti * ppt, 0, ppt)
    active = (tiles > 0).astype(I32)
    tw = pick(jnp.cumsum(active) - active)
    tf = (ti == 0).astype(I32)
    later = (le[None, :] > tl[:, None]) & (active[None, :] > 0)
    nxt = jnp.min(jnp.where(later, le[None, :], nl), axis=1)
    nxt = jnp.where(nxt < nl, nxt, -1)
    plan = tuple(v.astype(I32) for v in (tend[-1:], tl, tp, tn, tw, tf, nxt, pc))
    hend = jnp.cumsum(hotm.astype(I32), axis=1)
    hl = jnp.minimum(below(hend[:, None, :], le[None, :, None]), nl - 1)
    return Routing(hend[:, -1], hl, nch, eg, pos, None), plan


def solution(mesh):
    nd = mesh.shape['ep']
    nx = nd // 2
    tok_spec = P(('replica', 'ep'), None, None)
    rows_ep = P('ep', None)
    by_expert = P('ep', None, None)

    def shift(v, s):
        return lax.ppermute(v, 'ep', [(2 * i + c, 2 * ((i + s) % nx) + c) for i in range(nx) for c in range(2)])

    def partner(v):
        return lax.ppermute(v, 'ep', [(i, i ^ 1) for i in range(nd)])

    def local(x, wq, wk, wv, wo, wr, w1, w3, w2, idx):
        b, s, d = x.shape
        t, k, ne = b * s, idx.shape[-1], w1.shape[0]
        nl = 2 * ne
        half = t // 2
        me = lax.axis_index('ep')
        x = x.reshape(t, d)
        ids = idx.reshape(t, k)

        wq, wk, wv, wo = [lax.all_gather(w, 'ep', axis=0, tiled=True) for w in (wq, wk, wv, wo)]
        own = (w1, w3, w2)
        other = tuple(partner(w) for w in own)

        halves = lambda v: v.reshape(2 * v.shape[0], half, *v.shape[2:])
        ids4 = jnp.stack([ids, shift(ids, 1), shift(ids, -1), shift(ids, 2)])
        is_local = halves(ids4 // nl == me // 2)
        lid = halves((ids4 - me * ne) % nl)
        r, plan = routing_plan(lid, is_local, nl)
        ohl = (lid[:, None] == jnp.arange(nl, dtype=I32)[:, None, None]) & is_local[:, None]
        A, R, L, O = (0, 1), (2, 3), (4, 5), (6, 7)
        solo = lambda j: entries(r.nh[j:j + 1], r.hl[j:j + 1])
        ents = {j: solo(j) for j in (0, 2, 3, 4, 5)}
        ents[1] = entries(jnp.where(jnp.arange(2) == 1, r.nh[:2], 0), r.hl[:2])
        ents[6] = entries(r.nh[6:8], r.hl[6:8])
        ra = Routing(None, None, None, None, r.pos[:2], None)

        hd = HEAD // 2
        freq = THETA ** (-jnp.arange(hd, dtype=F32) / hd)
        ang = (jnp.arange(t) % s).astype(F32)[:, None] * freq
        c, sn = jnp.cos(ang), jnp.sin(ang)
        cos, sin = jnp.concatenate([c, c], axis=1), jnp.concatenate([-sn, sn], axis=1)
        a = rmsnorm(x).astype(BF)
        a, cos, sin, r, plan, ents, ids4 = lax.optimization_barrier((a, cos, sin, r._replace(gt=ohl), plan, ents, ids4))
        ohl = r.gt
        q = proj(a, wq, cos, sin, True)
        kk = proj(a, wk, cos, sin, True)
        v = proj(a, wv, cos, sin, False)
        o = attn(q, kk, v)
        h = wo_proj(o, wo, x)

        rn = rmsnorm(h)
        logits = jnp.dot(rn, wr, precision=lax.Precision.HIGHEST, preferred_element_type=F32)
        oh = ids[..., None] == jnp.arange(wr.shape[1], dtype=I32)
        g = jax.nn.softmax(jnp.sum(jnp.where(oh, logits[:, None, :], 0.0), axis=-1), axis=-1)
        u = rn.astype(BF)

        ut, ub = u[:half], u[half:]
        u1t, u2b = shift(ut, 1), shift(ub, -1)
        ut2, ub2, g = lax.optimization_barrier((ut, ub, g))
        g4 = [g, shift(g, 1), shift(g, -1), shift(g, 2)]
        u1b, u2t = shift(ub2, 1), shift(ut2, -1)
        spread = lambda o, v: jnp.sum(jnp.where(o, halves(v)[:, None], 0.0), axis=3)
        ra = ra._replace(gt=spread(ohl[:2], g[None]))
        r = r._replace(gt=spread(ohl, jnp.stack(g4)))

        x = gather(A, r, (ut, ub), None)
        a0, = block((0,), ra, None, (ut,), (None,), own, other, F32, comb=False, ents=ents[0])
        a0, x, u1t, u2b = lax.optimization_barrier((a0, x, u1t, u2b))
        u3t, u3b = shift(u1t, 1), shift(u2b, -1)
        d2, = block((2,), r, None, (u1t,), (None,), own, other, F32, comb=False, ents=ents[2])
        u1b, d2 = lax.optimization_barrier((u1b, d2))
        x = gather(R, r, (u1t, u1b), x)
        x = gather(L, r, (u2t, u2b), x)
        u2bx, x = lax.optimization_barrier((u2b, x))
        d5, = block((5,), r, None, (u2bx,), (None,), own, other, F32, comb=False, ents=ents[5])
        u3t, d5 = lax.optimization_barrier((u3t, d5))
        x = gather(O, r, (u3t, u3b), x)
        z = cold(plan, x, own, other)

        tie = lambda r, *v: (lambda w: (r._replace(nch=w[0]), *w[1:]))(lax.optimization_barrier((r.nch, *v)))
        b6, b7 = block(O, r, z, (u3t, u3b), (None, None), own, other, BF, ents=ents[6])
        r, b6, b7 = tie(r, b6, b7)
        c6, c7 = shift(b6, 1), shift(b7, -1)
        b2, b5 = block((2, 5), r, z, (), (d2, d5), own, other, BF)
        r, b2, b5 = tie(r, b2, b5)
        b2, b5 = shift(b2, -1), shift(b5, 1)
        b3, = block((3,), r, z, (u1b,), (None,), own, other, BF, ents=ents[3])
        r, b3, c6, c7 = tie(r, b3, c6, c7)
        b6, b7 = shift(c6, 1), shift(c7, -1)
        b3 = shift(b3, -1)
        b4, = block((4,), r, z, (u2t,), (None,), own, other, BF, ents=ents[4])
        r, b4 = tie(r, b4)
        b4 = shift(b4, 1)
        accs = block(A, r, z, (ut, ub), (a0, None), own, other, F32, ents=ents[1])
        y = final(h, accs, [(b2, b3), (b4, b5), (b6, b7)])
        return y.reshape(b, s, d)

    return jax.shard_map(local, mesh=mesh,
                         in_specs=(tok_spec, rows_ep, rows_ep, rows_ep, rows_ep, P(None, None),
                                   by_expert, by_expert, by_expert, tok_spec),
                         out_specs=tok_spec, check_vma=False)
```

```python
import functools
import math
import typing
import jax
import jax.numpy as jnp
from jax import lax
from jax.experimental import pallas as pl
from jax.experimental.pallas import tpu as pltpu
from jax.sharding import PartitionSpec as P

HEAD = 128
EPS = 1e-6
THETA = 10000.0
PIECE = 16
CHUNK = 256
MT = 416
HM = 256
VMEM = 66_000_000
BF, F32, I32 = jnp.bfloat16, jnp.float32, jnp.int32


def rmsnorm(v):
    v = v.astype(F32)
    return v * lax.rsqrt(jnp.mean(v * v, axis=-1, keepdims=True) + EPS)


def dot(a, b):
    return jnp.dot(a, b, preferred_element_type=F32)


NT = (((1,), (1,)), ((), ()))
DMA2 = pltpu.SemaphoreType.DMA((2,))


def cost(flops, bytes_):
    return pl.CostEstimate(flops=flops, bytes_accessed=bytes_, transcendentals=0)


def parity(i):
    return lax.rem(i, 2)


def expert_buffers(d, ff):
    return [pltpu.VMEM((2, *v), BF) for v in ((d, ff), (d, ff), (ff, d))]


def loop(n):
    return pl.loop(0, n)


def params(**kw):
    return pltpu.CompilerParams(vmem_limit_bytes=VMEM, **kw)


LT, LB, RT, RB, OT, OB, PO, PASS = 0, 1, 2, 3, 4, 5, 6, 7
MESH = pl.DeviceIdType.MESH


def layer_kernel(nx, x_ref, wv_ref, wk_ref, wq_ref, wo_ref, cos_ref, sin_ref, w1_ref, w3_ref, h_ref, ut_ref, ub_ref,
                 o1_ref, o3_ref, w_ref, ab, qb, kb, vb, ssem, rsem, lsem, iosem, swap_send, swap_recv):
    shards = (wv_ref, wk_ref, wq_ref, wo_ref)
    sh = wv_ref.shape[0]
    hs = sh // 2
    t, d = ab.shape
    me = lax.axis_index("ep")
    chip, core = me // 2, me % 2
    right, left, opp = [2 * ((chip + k) % nx) + core for k in (1, nx - 1, 2)]
    partner = 2 * chip + 1 - core

    barrier = pltpu.get_barrier_semaphore()
    for dev in (right, left, partner):
        pl.semaphore_signal(barrier, inc=1, device_id={"ep": dev}, device_id_type=MESH)
    pl.semaphore_wait(barrier, 3)

    def rows(e, half=None):
        if half is None:
            return pl.ds(pl.multiple_of(e * sh, sh), sh)
        return pl.ds(pl.multiple_of(e * sh + half * hs, hs), hs)

    def remote(w, src, dst, dev, s, r):
        return pltpu.make_async_remote_copy(src_ref=src, dst_ref=w_ref.at[w, dst, :], send_sem=ssem.at[w, s],
                                            recv_sem=rsem.at[w, r], device_id={"ep": dev}, device_id_type=MESH)

    def own(w):
        src = shards[w]
        top, bot = src.at[pl.ds(0, hs), :], src.at[pl.ds(hs, hs), :]
        return [remote(w, top, rows(me, 0), right, 0, LT), remote(w, bot, rows(me, 1), left, 1, RB),
                remote(w, bot, rows(me, 1), right, 2, LB), remote(w, top, rows(me, 0), left, 3, RT),
                remote(w, src, rows(me), partner, 6, PO)]

    def mine(w):
        return pltpu.make_async_copy(shards[w], w_ref.at[w, rows(me), :], lsem.at[w])

    where = {LT: (left, 0), LB: (left, 1), RT: (right, 0), RB: (right, 1), OT: (opp, 0), OB: (opp, 1)}

    def onward(w, k):
        e, half = where[LT if k == OT else RB]
        return remote(w, w_ref.at[w, rows(e, half), :], rows(e, half), right if k == OT else left, 4 if k == OT else 5, k)

    def across(w, k):
        r = rows(*where[k])
        return remote(w, w_ref.at[w, r, :], r, partner, PASS + k, PASS + k)

    def arrive(w, k):
        r = rows(me) if k == PO else rows(*where[k % PASS])
        remote(w, w_ref.at[w, r, :], r, partner, 0, k).wait_recv()

    def begin(w):
        for c in own(w):
            c.start()
        mine(w).start()

    def stage_a(w):
        arrive(w, LT)
        onward(w, OT).start()
        arrive(w, RB)
        onward(w, OB).start()
        if w + 1 < 4:
            begin(w + 1)
        across(w, LT).start()
        across(w, RB).start()
        swap()

    def stage_b(w):
        for k in (LB, RT):
            arrive(w, k)
            across(w, k).start()
        swap()

    def stage_c(w):
        for k in (OT, OB):
            arrive(w, k)
            across(w, k).start()
        swap()

    def stage_d(w):
        for k in (PO, PASS + LT, PASS + RB, PASS + LB, PASS + RT, PASS + OT, PASS + OB):
            arrive(w, k)
        mine(w).wait()

    pieces = [(src.at[e], dst.at[e]) for e in range(w1_ref.shape[0]) for src, dst in ((w1_ref, o1_ref), (w3_ref, o3_ref))]
    swaps = [pltpu.make_async_remote_copy(src_ref=src, dst_ref=dst, send_sem=swap_send.at[i], recv_sem=swap_recv.at[i],
                                          device_id={"ep": partner}, device_id_type=MESH) for i, (src, dst) in enumerate(pieces)]
    waiting = list(swaps)

    def swap():
        if waiting:
            waiting.pop(0).start()

    begin(0)
    swap()
    xin = pltpu.make_async_copy(x_ref, kb, iosem.at[0])
    xin.start()
    xin.wait()
    rb = min(128, t)

    @loop(t // rb)
    def _(i):
        r = pl.ds(pl.multiple_of(i * rb, rb), rb)
        ab[r, :] = rmsnorm(kb[r, :]).astype(BF)

    tm, tn = min(512, t), min(512, d)

    def project(w, dst, rope):
        @loop(d // tn)
        def _(n):
            @loop(t // tm)
            def _(m):
                r = pl.ds(pl.multiple_of(m * tm, tm), tm)
                z = dot(ab[r, :], w_ref[w, :, pl.ds(pl.multiple_of(n * tn, tn), tn)])
                for j in range(tn // HEAD):
                    zj = z[:, j * HEAD:(j + 1) * HEAD]
                    if rope:
                        zj = zj * cos_ref[r, :] + pltpu.roll(zj, HEAD // 2, 1) * sin_ref[r, :]
                    dst[r, pl.ds(pl.multiple_of(n * tn + j * HEAD, HEAD), HEAD)] = zj.astype(BF)

    for w, (dst, rope) in enumerate(((vb, False), (kb, True), (qb, True))):
        stage_a(w)
        stage_b(w)
        stage_c(w)
        stage_d(w)
        swap()
        project(w, dst, rope)
    stage_a(3)

    tq = min(256, t)
    scale = 1.0 / math.sqrt(HEAD)
    causal = lax.broadcasted_iota(I32, (tq, tq), 1) <= lax.broadcasted_iota(I32, (tq, tq), 0)

    def heads(lo, hi):
        @pl.loop(lo, hi)
        def _(j):
            c = pl.ds(pl.multiple_of(j * HEAD, HEAD), HEAD)
            for i in range(t // tq):
                r = slice(i * tq, (i + 1) * tq)
                q = qb[r, c]
                sd = lax.dot_general(q, kb[r, c], NT, preferred_element_type=F32)
                sd = jnp.where(causal, sd, -jnp.inf)
                m = jnp.max(sd, axis=1, keepdims=True)
                if i:
                    so = lax.dot_general(q, kb[:i * tq, c], NT, preferred_element_type=F32)
                    m = jnp.maximum(m, jnp.max(so, axis=1, keepdims=True))
                pd = jnp.exp((sd - m) * scale)
                l = jnp.sum(pd, axis=1, keepdims=True)
                if i:
                    po = jnp.exp((so - m) * scale)
                    l = l + jnp.sum(po, axis=1, keepdims=True)
                inv = 1.0 / l
                o = dot((pd * inv).astype(BF), vb[r, c])
                if i:
                    o = o + dot((po * inv).astype(BF), vb[:i * tq, c])
                qb[r, c] = o.astype(BF)

    nh = d // HEAD
    cut1, cut2 = nh * 3 // 8, nh * 3 // 4
    heads(0, cut1)
    stage_b(3)
    heads(cut1, cut2)
    stage_c(3)
    heads(cut2, nh)
    xin = pltpu.make_async_copy(x_ref, vb, iosem.at[0])
    xin.start()
    stage_d(3)
    xin.wait()

    @loop(d // tn)
    def _(n):
        c = pl.ds(pl.multiple_of(n * tn, tn), tn)

        @loop(t // tm)
        def _(m):
            r = pl.ds(pl.multiple_of(m * tm, tm), tm)
            ab[r, c] = (vb[r, c].astype(F32) + dot(qb[r, :], w_ref[3, :, c])).astype(BF)

    hout = pltpu.make_async_copy(ab, h_ref, iosem.at[0])
    hout.start()

    @loop(t // rb)
    def _(i):
        r = pl.ds(pl.multiple_of(i * rb, rb), rb)
        kb[r, :] = rmsnorm(ab[r, :]).astype(BF)

    uout = [pltpu.make_async_copy(kb.at[pl.ds(p * t // 2, t // 2), :], o, iosem.at[1 + p]) for p, o in enumerate((ut_ref, ub_ref))]
    for c in uout:
        c.start()
    while waiting:
        swap()
    for c in swaps:
        c.wait()
    for w in range(4):
        for c in own(w) + [onward(w, OT), onward(w, OB)] + [across(w, k) for k in where]:
            c.wait_send()
    hout.wait()
    for c in uout:
        c.wait()


def attention_layer(nx, x, wv, wk, wq, wo, cos, sin, w1, w3):
    t, d = x.shape
    hb = pl.BlockSpec(memory_space=pl.ANY)
    vm = pl.BlockSpec(memory_space=pltpu.VMEM)
    half = jax.ShapeDtypeStruct((t // 2, d), BF)
    act = pltpu.VMEM((t, d), BF)
    return pl.pallas_call(
        functools.partial(layer_kernel, nx),
        in_specs=[hb] * 5 + [vm] * 2 + [hb] * 2,
        out_specs=[hb] * 5,
        out_shape=[jax.ShapeDtypeStruct((t, d), BF), half, half, jax.ShapeDtypeStruct(w1.shape, BF),
                   jax.ShapeDtypeStruct(w3.shape, BF)],
        scratch_shapes=[pltpu.VMEM((4, d, d), BF), act, act, act, act,
                        pltpu.SemaphoreType.DMA((4, 13)), pltpu.SemaphoreType.DMA((4, 13)),
                        pltpu.SemaphoreType.DMA((4,)), pltpu.SemaphoreType.DMA((3,)),
                        pltpu.SemaphoreType.DMA((2 * w1.shape[0],)), pltpu.SemaphoreType.DMA((2 * w1.shape[0],))],
        compiler_params=params(collective_id=0, has_side_effects=True),
        cost_estimate=cost(8 * t * d * d, 24 * t * d),
    )(x, wv, wk, wq, wo, cos, sin, w1, w3)


def fetch_expert(l, slot, own, other, bufs, sem):
    ne = own[0].shape[0]

    @pl.when(l < ne)
    def _():
        for src, dst in zip(own, bufs):
            pltpu.make_async_copy(src.at[l], dst.at[slot], sem.at[slot]).start()

    @pl.when(l >= ne)
    def _():
        for src, dst in zip(other, bufs):
            pltpu.make_async_copy(src.at[l - ne], dst.at[slot], sem.at[slot]).start()


def wait_expert(slot, own, bufs, sem):
    for src, dst in zip(own, bufs):
        pltpu.make_async_copy(src.at[0], dst.at[slot], sem.at[slot]).wait()


def ffn(x, w1, w3, w2):
    a1 = dot(x, w1)
    a3 = dot(x, w3)
    act = (jax.nn.silu(a1) * a3).astype(BF)
    return dot(act, w2).astype(BF)


def block_kernel(js, has_acc, comb, dense, *refs):
    refs = list(refs)
    nblk = len(js)
    take = lambda n: [refs.pop(0) for _ in range(n)]
    if any(dense):
        nh_ref, hl_ref = take(2)
    gt_ref, = take(1)
    if comb:
        nch_ref, eg_ref, pos_ref, z_ref = take(4)
        cap = z_ref.shape[0] // pos_ref.shape[0]
    if any(dense):
        us = take(nblk)
        own, other = take(3), take(3)
        nl = 2 * own[0].shape[0]
    accs = [take(1)[0] if h else None for h in has_acc]
    outs = take(nblk)
    acc, asem = take(2)
    if comb:
        cbuf, zbuf, zsem = take(3)
    if any(dense):
        bufs, (ubuf, sem, usem) = take(3), take(3)
    t, d = outs[0].shape

    if any(dense):
        ns = [nh_ref[j] if on else 0 for j, on in zip(js, dense)]
        n = sum(ns)

        def entry(i):
            p = jnp.where(i < ns[0], 0, nblk - 1)
            return p, hl_ref[jnp.where(p == 0, js[0], js[-1]) * nl + i - jnp.where(p == 0, 0, ns[0])]

        @pl.when(n > 0)
        def _():
            fetch_expert(entry(0)[1], 0, own, other, bufs, sem)

        ucp = [pltpu.make_async_copy(us[p], ubuf.at[pl.ds(p * t, t), :], usem) for p in range(nblk)]
        for cp in ucp:
            cp.start()
    for p in range(nblk):
        rows = pl.ds(p * t, t)
        if has_acc[p]:
            pltpu.make_async_copy(accs[p], acc.at[rows, :], asem.at[p]).start()
        else:
            acc[rows, :] = jnp.zeros((t, d), F32)
    for p in range(nblk):
        if has_acc[p]:
            pltpu.make_async_copy(accs[p], acc.at[pl.ds(p * t, t), :], asem.at[p]).wait()

    if comb:
        for p, j in enumerate(js):
            nch = nch_ref[j]

            def get(i, slot):
                src = pl.multiple_of(j * cap + i * CHUNK, CHUNK)
                return pltpu.make_async_copy(z_ref.at[pl.ds(src, CHUNK), :], zbuf.at[slot], zsem.at[slot])

            get(0, 0).start()
            nl = gt_ref.shape[1]
            lane = lax.broadcasted_iota(I32, (1, CHUNK), 1)
            ti = lax.broadcasted_iota(I32, (PIECE, t), 1)
            si = lax.broadcasted_iota(I32, (PIECE, t), 0)
            tparts = jnp.where(si == 0, ti % 256, jnp.where(si == 1, ti // 256, 0)).astype(F32).astype(BF)
            table = jnp.concatenate([*split3(gt_ref[j]), tparts], axis=0)

            @loop(nch)
            def _(i):
                slot = parity(i)

                @pl.when(i + 1 < nch)
                def _():
                    get(i + 1, 1 - slot).start()

                ps, el = [], jnp.zeros((1, CHUNK), I32)
                for q, (hit, l) in enumerate(selection(j, i, eg_ref, pos_ref)):
                    ps.append(jnp.where(hit, 1.0, 0.0).astype(BF))
                    el = jnp.where(lane // PIECE == q, l, el)
                sel = lax.dot_general(table, jnp.concatenate(ps, axis=0), NT, preferred_element_type=F32)
                tok = (sel[3 * nl:3 * nl + 1] + 256.0 * sel[3 * nl + 1:3 * nl + 2]).astype(I32)
                hot_ = lax.broadcasted_iota(I32, (t, CHUNK), 0) == tok
                sub = lax.broadcasted_iota(I32, (nl, CHUNK), 0) == el
                for k in range(3):
                    gk = jnp.sum(jnp.where(sub, sel[k * nl:(k + 1) * nl], 0.0), axis=0, keepdims=True)
                    cbuf[:, k * CHUNK:(k + 1) * CHUNK] = jnp.where(hot_, gk, 0.0).astype(BF)
                get(i, slot).wait()
                tn = min(1024, d)

                @loop(d // tn)
                def _(m):
                    cs = pl.ds(pl.multiple_of(m * tn, tn), tn)
                    z = zbuf[slot, :, cs]
                    acc[p * t:(p + 1) * t, cs] += dot(cbuf[:], jnp.concatenate([z, z, z], axis=0))

    if any(dense):
        for cp in ucp:
            cp.wait()
        tm = min(HM, t)

        @loop(n)
        def _(i):
            slot = parity(i)
            wait_expert(slot, own, bufs, sem)

            @pl.when(i + 1 < n)
            def _():
                fetch_expert(entry(i + 1)[1], 1 - slot, own, other, bufs, sem)

            p, e = entry(i)
            blk = jnp.where(p == 0, js[0], js[-1])

            @loop(t // tm)
            def _(m):
                rows = pl.ds(pl.multiple_of(p * t + m * tm, tm), tm)
                z = ffn(ubuf[rows, :], bufs[0][slot], bufs[1][slot], bufs[2][slot])
                g = gt_ref[blk, pl.ds(e, 1), pl.ds(pl.multiple_of(m * tm, tm), tm)]
                eye = lax.broadcasted_iota(I32, (tm, tm), 0) == lax.broadcasted_iota(I32, (tm, tm), 1)
                gc = jnp.sum(jnp.where(eye, g, 0.0), axis=1, keepdims=True)
                acc[rows, :] += gc * z.astype(F32)

    for p in range(nblk):
        outs[p][:] = acc[p * t:(p + 1) * t, :].astype(outs[p].dtype)


def block(js, r, z, us, accs, own, other, dtype, dense, comb=True):
    nblk = len(js)
    t = r.pos.shape[2]
    d = own[0].shape[1]
    ff = own[0].shape[2]
    vm = pl.BlockSpec(memory_space=pltpu.VMEM)
    sm = pl.BlockSpec(memory_space=pltpu.SMEM)
    hb = pl.BlockSpec(memory_space=pl.ANY)
    args, specs, scratch = [], [], []
    if any(dense):
        args += [r.nh, r.hl.reshape(-1)]
        specs += [sm, sm]
    args += [r.gt]
    specs += [vm]
    if comb:
        args += [r.nch, r.eg.reshape(-1), r.pos, z]
        specs += [sm, sm, vm, hb]
    if any(dense):
        args += list(us) + list(own) + list(other)
        specs += [hb] * (nblk + 6)
    args += [v for v in accs if v is not None]
    specs += [hb for v in accs if v is not None]
    scratch += [pltpu.VMEM((nblk * t, d), F32), pltpu.SemaphoreType.DMA((nblk,))]
    if comb:
        scratch += [pltpu.VMEM((t, 3 * CHUNK), BF), pltpu.VMEM((2, CHUNK, d), BF), DMA2]
    if any(dense):
        scratch += [*expert_buffers(d, ff),
                    pltpu.VMEM((nblk * t, d), BF), DMA2, pltpu.SemaphoreType.DMA]
    out = jax.ShapeDtypeStruct((t, d), dtype)
    return pl.pallas_call(
        functools.partial(block_kernel, js, [v is not None for v in accs], comb, dense),
        in_specs=specs, out_specs=[vm] * nblk, out_shape=[out] * nblk, scratch_shapes=scratch,
        compiler_params=params(),
        cost_estimate=cost(t * d, 6 * d * ff),
    )(*args)


def split3(g):
    hi = g.astype(BF)
    r = g - hi.astype(F32)
    mid = r.astype(BF)
    lo = (r - mid.astype(F32)).astype(BF)
    return hi, mid, lo


def selection(j, i, eg_ref, pos_ref):
    t = pos_ref.shape[2]
    it = lax.broadcasted_iota(I32, (PIECE, t), 0)
    npc = CHUNK // PIECE
    npb = eg_ref.shape[0] // pos_ref.shape[0]
    for q in range(npc):
        l = eg_ref[j * npb + i * npc + q]
        yield pos_ref[j, pl.ds(l, 1), :] - (i * CHUNK + q * PIECE) == it, l


def gather_kernel(js, nch_ref, eg_ref, pos_ref, *refs):
    us = refs[:len(js)]
    x_ref, xbuf, sem = refs[-3:]
    cap = x_ref.shape[0] // pos_ref.shape[0]
    for p, j in enumerate(js):
        nch = nch_ref[j]

        def out(i, slot):
            dst = pl.multiple_of(j * cap + i * CHUNK, CHUNK)
            return pltpu.make_async_copy(xbuf.at[slot], x_ref.at[pl.ds(dst, CHUNK), :], sem.at[slot])

        @loop(nch)
        def _(i):
            slot = parity(i)

            @pl.when(i >= 2)
            def _():
                out(i - 2, slot).wait()

            pm = jnp.concatenate([jnp.where(hit, 1.0, 0.0).astype(BF) for hit, _ in selection(j, i, eg_ref, pos_ref)], axis=0)
            xbuf[slot] = dot(pm, us[p][:]).astype(BF)
            out(i, slot).start()

        for k in (2, 1):
            @pl.when(nch >= k)
            def _():
                out(nch - k, parity(nch - k)).wait()


def gather(js, r, us, x):
    nblk = len(js)
    t, d = us[0].shape
    nb = r.eg.shape[0]
    cap = r.eg.shape[1] * PIECE
    vm = pl.BlockSpec(memory_space=pltpu.VMEM)
    sm = pl.BlockSpec(memory_space=pltpu.SMEM)
    hb = pl.BlockSpec(memory_space=pl.ANY)
    return pl.pallas_call(
        functools.partial(gather_kernel, js),
        in_specs=[sm, sm, vm] + [vm] * nblk + ([hb] if x is not None else []),
        out_specs=hb,
        out_shape=jax.ShapeDtypeStruct((nb * cap, d), BF),
        input_output_aliases={3 + nblk: 0} if x is not None else {},
        scratch_shapes=[pltpu.VMEM((2, CHUNK, d), BF), DMA2],
        compiler_params=params(),
        cost_estimate=cost(t * d, 4 * CHUNK * d),
    )(r.nch, r.eg.reshape(-1), r.pos, *us, *([x] if x is not None else []))


def cold_kernel(nt_ref, tl_ref, tp_ref, tn_ref, tw_ref, tf_ref, nx_ref, pc_ref, x_ref, *refs):
    own, other, z_ref, refs = refs[:3], refs[3:6], refs[6], refs[7:]
    bufs, (xbuf, zbuf, wsem, xsem, zsem) = refs[:3], refs[3:]
    nt = nt_ref[0]

    def xin(q, slot):
        p0 = tp_ref[q]

        @loop(tn_ref[q])
        def _(i):
            src = pl.ds(pl.multiple_of(pc_ref[p0 + i] * PIECE, PIECE), PIECE)
            dst = pl.ds(pl.multiple_of(i * PIECE, PIECE), PIECE)
            pltpu.make_async_copy(x_ref.at[src, :], xbuf.at[slot, dst, :], xsem.at[slot]).start()

    def zout(q, slot):
        p0 = tp_ref[q]

        @loop(tn_ref[q])
        def _(i):
            src = pl.ds(pl.multiple_of(i * PIECE, PIECE), PIECE)
            dst = pl.ds(pl.multiple_of(pc_ref[p0 + i] * PIECE, PIECE), PIECE)
            pltpu.make_async_copy(zbuf.at[slot, src, :], z_ref.at[dst, :], zsem.at[slot]).start()

    def drain(n, fn):
        bit = 1
        while bit <= MT // PIECE:
            @pl.when(lax.rem(lax.div(n, bit), 2) == 1)
            def _(bit=bit):
                fn(pl.ds(0, bit * PIECE))

            bit *= 2

    def xwait(q, slot):
        drain(tn_ref[q], lambda r: pltpu.make_async_copy(x_ref.at[r, :], xbuf.at[slot, r, :], xsem.at[slot]).wait())

    def zwait(q, slot):
        drain(tn_ref[q], lambda r: pltpu.make_async_copy(zbuf.at[slot, r, :], z_ref.at[r, :], zsem.at[slot]).wait())

    @pl.when(nt > 0)
    def _():
        fetch_expert(tl_ref[0], 0, own, other, bufs, wsem)
        xin(0, 0)

    @loop(nt)
    def _(q):
        slot = parity(q)
        ws = parity(tw_ref[q])

        @pl.when(tf_ref[q] == 1)
        def _():
            wait_expert(ws, own, bufs, wsem)

            @pl.when(nx_ref[q] >= 0)
            def _():
                fetch_expert(nx_ref[q], 1 - ws, own, other, bufs, wsem)

        @pl.when(q + 1 < nt)
        def _():
            xin(q + 1, 1 - slot)

        xwait(q, slot)

        @pl.when(q >= 2)
        def _():
            zwait(q - 2, slot)

        zbuf[slot] = ffn(xbuf[slot], bufs[0][ws], bufs[1][ws], bufs[2][ws])
        zout(q, slot)

    for k in (2, 1):
        @pl.when(nt >= k)
        def _():
            zwait(nt - k, parity(nt - k))


def cold(plan, x, own, other):
    d, ff = own[0].shape[1:]
    sm = pl.BlockSpec(memory_space=pltpu.SMEM)
    hb = pl.BlockSpec(memory_space=pl.ANY)
    return pl.pallas_call(
        cold_kernel,
        in_specs=[sm] * len(plan) + [hb] * 7,
        out_specs=hb,
        out_shape=jax.ShapeDtypeStruct(x.shape, BF),
        scratch_shapes=[*expert_buffers(d, ff),
                        pltpu.VMEM((2, MT, d), BF), pltpu.VMEM((2, MT, d), BF),
                        DMA2, DMA2, DMA2],
        input_output_aliases={len(plan): 0},
        compiler_params=params(),
        cost_estimate=cost(6 * 16 * MT * d * ff, 96 * d * ff),
    )(*plan, x, *own, *other)


def final_kernel(h_ref, *refs):
    y_ref = refs[-1]
    acc, parts = refs[0], refs[1:-1]
    y = h_ref[:].astype(F32) + acc[:]
    for v in parts:
        y = y + v[:].astype(F32)
    y_ref[:] = y.astype(BF)


def final(h, accs, parts):
    t, d = h.shape
    half = t // 2
    tm = min(128, half)
    n = half // tm

    def body(h_ref, *refs):
        for p in range(2):
            @pl.when(pl.program_id(0) // n == p)
            def _():
                final_kernel(h_ref, refs[p], *refs[2 + p:-1:2], refs[-1])

    spec = lambda p: pl.BlockSpec((tm, d), lambda i: (jnp.minimum(i, n - 1) if p == 0 else jnp.maximum(i - n, 0), 0))
    return pl.pallas_call(
        body, grid=(2 * n,),
        in_specs=[pl.BlockSpec((tm, d), lambda i: (i, 0))] + [spec(0), spec(1)] * (1 + len(parts)),
        out_specs=pl.BlockSpec((tm, d), lambda i: (i, 0)),
        out_shape=jax.ShapeDtypeStruct((t, d), BF),
        compiler_params=params(),
        cost_estimate=cost(6 * t * d, 20 * t * d),
    )(h, *accs, *[v for part in parts for v in part])


class Routing(typing.NamedTuple):
    nh: typing.Any
    hl: typing.Any
    nch: typing.Any
    eg: typing.Any
    pos: typing.Any
    gt: typing.Any


def routing_plan(lid, local, nl):
    nb, t, k = lid.shape
    le = jnp.arange(nl, dtype=I32)
    hit = jnp.any((lid[:, None] == le[:, None, None]) & local[:, None], axis=-1)
    tri = (jnp.arange(t)[:, None] <= jnp.arange(t)[None, :]).astype(BF)
    rank = lax.dot_general(hit.astype(BF), tri, (((2,), (0,)), ((), ())), preferred_element_type=F32).astype(I32)
    cnt = rank[:, :, -1]
    hotm = cnt >= t // 2
    scnt = jnp.where(hotm, 0, cnt)
    pcs = (scnt + PIECE - 1) // PIECE
    pend = jnp.cumsum(pcs, axis=1)
    base = (pend - pcs) * PIECE
    pos = jnp.where(hit & ~hotm[..., None], base[..., None] + rank - 1, -1)
    rows = t * k + nl * PIECE
    npb = -(-rows // CHUNK) * CHUNK // PIECE
    nch = jnp.maximum(-(-pend[:, -1] * PIECE // CHUNK), 1)
    below = lambda ends, q: jnp.sum((ends <= q).astype(I32), axis=-1)
    eg = jnp.minimum(below(pend[:, None, :], jnp.arange(npb, dtype=I32)[None, :, None]), nl - 1)
    flat = pcs.T.reshape(-1)
    fend = jnp.cumsum(flat)
    p = jnp.arange(nb * npb, dtype=I32)[:, None]
    seg = jnp.minimum(below(fend[None, :], p), nl * nb - 1)
    inseg = seg[:, None] == jnp.arange(nl * nb, dtype=I32)
    shift_ = jnp.tile(jnp.arange(nb, dtype=I32) * npb, nl) + (pend - pcs).T.reshape(-1) - (fend - flat)
    pc = jnp.clip(p[:, 0] + jnp.sum(jnp.where(inseg, shift_, 0), axis=1), 0, nb * npb - 1)
    ppt = MT // PIECE
    ptot = jnp.sum(pcs, axis=0)
    pstart = jnp.cumsum(ptot) - ptot
    tiles = (ptot + ppt - 1) // ppt
    tend = jnp.cumsum(tiles)
    nq = -(-(nb * npb) // ppt) + nl
    q = jnp.arange(nq, dtype=I32)
    tl = jnp.minimum(below(tend[None, :], q[:, None]), nl - 1)
    one = tl[:, None] == le
    pick = lambda v: jnp.sum(jnp.where(one, v[None, :], 0), axis=1)
    ti = q - pick(tend - tiles)
    tp = pick(pstart) + ti * ppt
    tn = jnp.clip(pick(ptot) - ti * ppt, 0, ppt)
    active = (tiles > 0).astype(I32)
    tw = pick(jnp.cumsum(active) - active)
    tf = (ti == 0).astype(I32)
    later = (le[None, :] > tl[:, None]) & (active[None, :] > 0)
    nxt = jnp.min(jnp.where(later, le[None, :], nl), axis=1)
    nxt = jnp.where(nxt < nl, nxt, -1)
    plan = tuple(v.astype(I32) for v in (tend[-1:], tl, tp, tn, tw, tf, nxt, pc))
    hend = jnp.cumsum(hotm.astype(I32), axis=1)
    hl = jnp.minimum(below(hend[:, None, :], le[None, :, None]), nl - 1)
    return Routing(hend[:, -1], hl, nch, eg, pos, None), plan


ON = (True,)


def solution(mesh):
    nd = mesh.shape['ep']
    nx = nd // 2
    tok_spec = P(('replica', 'ep'), None, None)
    rows_ep = P('ep', None)
    by_expert = P('ep', None, None)

    def shift(v, s):
        return lax.ppermute(v, 'ep', [(2 * i + c, 2 * ((i + s) % nx) + c) for i in range(nx) for c in range(2)])

    def partner(v):
        return lax.ppermute(v, 'ep', [(i, i ^ 1) for i in range(nd)])

    def local(x, wq, wk, wv, wo, wr, w1, w3, w2, idx):
        b, s, d = x.shape
        t, k, ne = b * s, idx.shape[-1], w1.shape[0]
        nl = 2 * ne
        half = t // 2
        me = lax.axis_index('ep')
        x = x.reshape(t, d)
        ids = idx.reshape(t, k)

        ids4 = jnp.stack([ids, shift(ids, 1), shift(ids, -1), shift(ids, 2)])
        hd = HEAD // 2
        freq = THETA ** (-jnp.arange(hd, dtype=F32) / hd)
        ang = (jnp.arange(t) % s).astype(F32)[:, None] * freq
        c, sn = jnp.cos(ang), jnp.sin(ang)
        cos, sin = jnp.concatenate([c, c], axis=1), jnp.concatenate([-sn, sn], axis=1)
        x, cos, sin, ids4 = lax.optimization_barrier((x, cos, sin, ids4))
        h, ut, ub, o1, o3 = attention_layer(nx, x, wv, wk, wq, wo, cos, sin, w1, w3)
        ids4, w2, ut, ub = lax.optimization_barrier((ids4, w2, ut, ub))
        o2 = partner(w2)
        own, other = (w1, w3, w2), (o1, o3, o2)

        halves = lambda v: v.reshape(2 * v.shape[0], half, *v.shape[2:])
        is_local = halves(ids4 // nl == me // 2)
        lid = halves((ids4 - me * ne) % nl)
        r, plan = routing_plan(lid, is_local, nl)
        ohl = (lid[:, None] == jnp.arange(nl, dtype=I32)[:, None, None]) & is_local[:, None]
        A, R, L, O = (0, 1), (2, 3), (4, 5), (6, 7)
        ra = r._replace(pos=r.pos[:2])

        u1t, u2b = shift(ut, 1), shift(ub, -1)
        logits = jnp.dot(rmsnorm(h), wr, precision=lax.Precision.HIGHEST, preferred_element_type=F32)
        oh = ids[..., None] == jnp.arange(wr.shape[1], dtype=I32)
        g = jax.nn.softmax(jnp.sum(jnp.where(oh, logits[:, None, :], 0.0), axis=-1), axis=-1)
        ut2, ub2, g = lax.optimization_barrier((ut, ub, g))
        g4 = [g, shift(g, 1), shift(g, -1), shift(g, 2)]
        u1b, u2t = shift(ub2, 1), shift(ut2, -1)
        spread = lambda o, v: jnp.sum(jnp.where(o, halves(v)[:, None], 0.0), axis=3)
        ra = ra._replace(gt=spread(ohl[:2], g[None]))
        r = r._replace(gt=spread(ohl, jnp.stack(g4)))

        x = gather(A, r, (ut, ub), None)
        a0, = block((0,), ra, None, (ut,), (None,), own, other, F32, ON, comb=False)
        a0, x, u1t, u2b = lax.optimization_barrier((a0, x, u1t, u2b))
        u3t, u3b = shift(u1t, 1), shift(u2b, -1)
        d2, = block((2,), r, None, (u1t,), (None,), own, other, F32, ON, comb=False)
        u1b, d2 = lax.optimization_barrier((u1b, d2))
        x = gather(R, r, (u1t, u1b), x)
        x = gather(L, r, (u2t, u2b), x)
        u2bx, x = lax.optimization_barrier((u2b, x))
        d5, = block((5,), r, None, (u2bx,), (None,), own, other, F32, ON, comb=False)
        u3t, d5 = lax.optimization_barrier((u3t, d5))
        x = gather(O, r, (u3t, u3b), x)
        z = cold(plan, x, own, other)

        tie = lambda r, *v: (lambda w: (r._replace(nch=w[0]), *w[1:]))(lax.optimization_barrier((r.nch, *v)))
        b6, b7 = block(O, r, z, (u3t, u3b), (None, None), own, other, BF, 2 * ON)
        r, b6, b7 = tie(r, b6, b7)
        c6, c7 = shift(b6, 1), shift(b7, -1)
        b2, b5 = block((2, 5), r, z, (), (d2, d5), own, other, BF, (False, False))
        r, b2, b5 = tie(r, b2, b5)
        b2, b5 = shift(b2, -1), shift(b5, 1)
        b3, = block((3,), r, z, (u1b,), (None,), own, other, BF, ON)
        r, b3, c6, c7 = tie(r, b3, c6, c7)
        b6, b7 = shift(c6, 1), shift(c7, -1)
        b3 = shift(b3, -1)
        b4, = block((4,), r, z, (u2t,), (None,), own, other, BF, ON)
        r, b4 = tie(r, b4)
        b4 = shift(b4, 1)
        accs = block(A, r, z, (ut, ub), (a0, None), own, other, F32, (False, True))
        y = final(h, accs, [(b2, b3), (b4, b5), (b6, b7)])
        return y.reshape(b, s, d)

    return jax.shard_map(local, mesh=mesh,
                         in_specs=(tok_spec, rows_ep, rows_ep, rows_ep, rows_ep, P(None, None),
                                   by_expert, by_expert, by_expert, tok_spec),
                         out_specs=tok_spec, check_vma=False)
```

```python
import functools
import math
import typing
import jax
import jax.numpy as jnp
from jax import lax
from jax.experimental import pallas as pl
from jax.experimental.pallas import tpu as pltpu
from jax.sharding import PartitionSpec as P

HEAD = 128
EPS = 1e-6
THETA = 10000.0
PIECE = 8
CHUNK = 256
MT = 352
HM = 256
VMEM = 66_000_000
BF, F32, I32 = jnp.bfloat16, jnp.float32, jnp.int32


def rmsnorm(v):
    v = v.astype(F32)
    return v * lax.rsqrt(jnp.mean(v * v, axis=-1, keepdims=True) + EPS)


def dot(a, b):
    return jnp.dot(a, b, preferred_element_type=F32)


NT = (((1,), (1,)), ((), ()))
TN = (((0,), (0,)), ((), ()))
DMA2 = pltpu.SemaphoreType.DMA((2,))


def cost(flops, bytes_):
    return pl.CostEstimate(flops=flops, bytes_accessed=bytes_, transcendentals=0)


def parity(i):
    return lax.rem(i, 2)


def expert_buffers(d, ff):
    return [pltpu.VMEM((2, *v), BF) for v in ((d, ff), (d, ff), (ff, d))]


def loop(n):
    return pl.loop(0, n)


def params(**kw):
    return pltpu.CompilerParams(vmem_limit_bytes=VMEM, **kw)


LT, LB, RT, RB, OT, OB, PO, PASS = 0, 1, 2, 3, 4, 5, 6, 7
MESH = pl.DeviceIdType.MESH


def layer_kernel(nx, x_ref, wv_ref, wk_ref, wq_ref, wo_ref, cos_ref, sin_ref, w1_ref, w3_ref, h_ref, ut_ref, ub_ref,
                 o1_ref, o3_ref, w_ref, ab, qb, kb, vb, ssem, rsem, lsem, iosem, swap_send, swap_recv):
    shards = (wv_ref, wk_ref, wq_ref, wo_ref)
    sh = wv_ref.shape[0]
    hs = sh // 2
    t, d = ab.shape
    me = lax.axis_index("ep")
    chip, core = me // 2, me % 2
    right, left, opp = [2 * ((chip + k) % nx) + core for k in (1, nx - 1, 2)]
    partner = 2 * chip + 1 - core

    barrier = pltpu.get_barrier_semaphore()
    for dev in (right, left, partner):
        pl.semaphore_signal(barrier, inc=1, device_id={"ep": dev}, device_id_type=MESH)
    pl.semaphore_wait(barrier, 3)

    def rows(e, half=None):
        if half is None:
            return pl.ds(pl.multiple_of(e * sh, sh), sh)
        return pl.ds(pl.multiple_of(e * sh + half * hs, hs), hs)

    def remote(w, src, dst, dev, s, r):
        return pltpu.make_async_remote_copy(src_ref=src, dst_ref=w_ref.at[w, dst, :], send_sem=ssem.at[w, s],
                                            recv_sem=rsem.at[w, r], device_id={"ep": dev}, device_id_type=MESH)

    def own(w):
        src = shards[w]
        top, bot = src.at[pl.ds(0, hs), :], src.at[pl.ds(hs, hs), :]
        return [remote(w, top, rows(me, 0), right, 0, LT), remote(w, bot, rows(me, 1), left, 1, RB),
                remote(w, bot, rows(me, 1), right, 2, LB), remote(w, top, rows(me, 0), left, 3, RT),
                remote(w, src, rows(me), partner, 6, PO)]

    def mine(w):
        return pltpu.make_async_copy(shards[w], w_ref.at[w, rows(me), :], lsem.at[w])

    where = {LT: (left, 0), LB: (left, 1), RT: (right, 0), RB: (right, 1), OT: (opp, 0), OB: (opp, 1)}

    def onward(w, k):
        e, half = where[LT if k == OT else RB]
        return remote(w, w_ref.at[w, rows(e, half), :], rows(e, half), right if k == OT else left, 4 if k == OT else 5, k)

    def across(w, k):
        r = rows(*where[k])
        return remote(w, w_ref.at[w, r, :], r, partner, PASS + k, PASS + k)

    def arrive(w, k):
        r = rows(me) if k == PO else rows(*where[k % PASS])
        remote(w, w_ref.at[w, r, :], r, partner, 0, k).wait_recv()

    def begin(w):
        for c in own(w):
            c.start()
        mine(w).start()

    def stage_a(w):
        arrive(w, LT)
        onward(w, OT).start()
        arrive(w, RB)
        onward(w, OB).start()
        if w + 1 < 4:
            begin(w + 1)
        across(w, LT).start()
        across(w, RB).start()
        swap()

    def stage_b(w):
        for k in (LB, RT):
            arrive(w, k)
            across(w, k).start()
        if w != 2:
            swap()
        if w == 3:
            swap()

    def stage_c(w):
        for k in (OT, OB):
            arrive(w, k)
            across(w, k).start()
        if w != 2:
            swap()

    def stage_d(w):
        for k in (PO, PASS + LT, PASS + RB, PASS + LB, PASS + RT, PASS + OT, PASS + OB):
            arrive(w, k)
        mine(w).wait()

    pieces = [(src.at[e], dst.at[e]) for e in range(w1_ref.shape[0]) for src, dst in ((w1_ref, o1_ref), (w3_ref, o3_ref))]
    swaps = [pltpu.make_async_remote_copy(src_ref=src, dst_ref=dst, send_sem=swap_send.at[i], recv_sem=swap_recv.at[i],
                                          device_id={"ep": partner}, device_id_type=MESH) for i, (src, dst) in enumerate(pieces)]
    waiting = list(swaps)

    def swap():
        if waiting:
            waiting.pop(0).start()

    begin(0)
    swap()
    xin = pltpu.make_async_copy(x_ref, kb, iosem.at[0])
    xin.start()
    xin.wait()
    rb = min(128, t)

    @loop(t // rb)
    def _(i):
        r = pl.ds(pl.multiple_of(i * rb, rb), rb)
        ab[r, :] = rmsnorm(kb[r, :]).astype(BF)

    tm, tn = min(512, t), min(512, d)

    def project(w, dst, rope):
        @loop(d // tn)
        def _(n):
            @loop(t // tm)
            def _(m):
                r = pl.ds(pl.multiple_of(m * tm, tm), tm)
                z = dot(ab[r, :], w_ref[w, :, pl.ds(pl.multiple_of(n * tn, tn), tn)])
                for j in range(tn // HEAD):
                    zj = z[:, j * HEAD:(j + 1) * HEAD]
                    if rope:
                        zj = zj * cos_ref[r, :] + pltpu.roll(zj, HEAD // 2, 1) * sin_ref[r, :]
                    dst[r, pl.ds(pl.multiple_of(n * tn + j * HEAD, HEAD), HEAD)] = zj.astype(BF)

    for w, (dst, rope) in enumerate(((vb, False), (kb, True), (qb, True))):
        stage_a(w)
        stage_b(w)
        stage_c(w)
        stage_d(w)
        swap()
        if w == 2:
            swap()
        project(w, dst, rope)
    stage_a(3)

    tq = min(256, t)
    scale = math.log2(math.e) / math.sqrt(HEAD)
    causal = lax.broadcasted_iota(I32, (tq, tq), 0) <= lax.broadcasted_iota(I32, (tq, tq), 1)
    group = min(4, d // HEAD)
    steps = d // HEAD // group
    marks = {1: stage_b, steps - 1: stage_c}
    if len(marks) > steps - 1:
        marks = {}
        stage_b(3)
        stage_c(3)

    @loop(steps)
    def _(jj):
        for at, stage in marks.items():
            pl.when(jj == at)(functools.partial(stage, 3))
        for j in range(group):
            c = pl.ds(pl.multiple_of((jj * group + j) * HEAD, HEAD), HEAD)
            for i in range(t // tq):
                r, n = slice(i * tq, (i + 1) * tq), (i + 1) * tq
                sc = lax.dot_general(kb[:n, c], qb[r, c], NT, preferred_element_type=F32)
                diag = jnp.where(causal, sc[i * tq:], -jnp.inf)
                sc = jnp.concatenate([sc[:i * tq], diag], axis=0) if i else diag
                p = jnp.exp2((sc - jnp.max(sc, axis=0, keepdims=True)) * scale)
                p = (p * (1.0 / jnp.sum(p, axis=0, keepdims=True))).astype(BF)
                qb[r, c] = lax.dot_general(p, vb[:n, c], TN, preferred_element_type=F32).astype(BF)

    xin = pltpu.make_async_copy(x_ref, vb, iosem.at[0])
    xin.start()
    stage_d(3)
    xin.wait()

    @loop(d // tn)
    def _(n):
        c = pl.ds(pl.multiple_of(n * tn, tn), tn)

        @loop(t // tm)
        def _(m):
            r = pl.ds(pl.multiple_of(m * tm, tm), tm)
            ab[r, c] = (vb[r, c].astype(F32) + dot(qb[r, :], w_ref[3, :, c])).astype(BF)

    hout = pltpu.make_async_copy(ab, h_ref, iosem.at[0])
    hout.start()

    @loop(t // rb)
    def _(i):
        r = pl.ds(pl.multiple_of(i * rb, rb), rb)
        kb[r, :] = rmsnorm(ab[r, :]).astype(BF)

    uout = [pltpu.make_async_copy(kb.at[pl.ds(p * t // 2, t // 2), :], o, iosem.at[1 + p]) for p, o in enumerate((ut_ref, ub_ref))]
    for c in uout:
        c.start()
    while waiting:
        swap()
    for c in swaps:
        c.wait()
    for w in range(4):
        for c in own(w) + [onward(w, OT), onward(w, OB)] + [across(w, k) for k in where]:
            c.wait_send()
    hout.wait()
    for c in uout:
        c.wait()


def attention_layer(nx, x, wv, wk, wq, wo, cos, sin, w1, w3):
    t, d = x.shape
    hb = pl.BlockSpec(memory_space=pl.ANY)
    vm = pl.BlockSpec(memory_space=pltpu.VMEM)
    half = jax.ShapeDtypeStruct((t // 2, d), BF)
    act = pltpu.VMEM((t, d), BF)
    return pl.pallas_call(
        functools.partial(layer_kernel, nx),
        in_specs=[hb] * 5 + [vm] * 2 + [hb] * 2,
        out_specs=[hb] * 5,
        out_shape=[jax.ShapeDtypeStruct((t, d), BF), half, half, jax.ShapeDtypeStruct(w1.shape, BF),
                   jax.ShapeDtypeStruct(w3.shape, BF)],
        scratch_shapes=[pltpu.VMEM((4, d, d), BF), act, act, act, act,
                        pltpu.SemaphoreType.DMA((4, 13)), pltpu.SemaphoreType.DMA((4, 13)),
                        pltpu.SemaphoreType.DMA((4,)), pltpu.SemaphoreType.DMA((3,)),
                        pltpu.SemaphoreType.DMA((2 * w1.shape[0],)), pltpu.SemaphoreType.DMA((2 * w1.shape[0],))],
        compiler_params=params(collective_id=0, has_side_effects=True),
        cost_estimate=cost(8 * t * d * d, 24 * t * d),
    )(x, wv, wk, wq, wo, cos, sin, w1, w3)


def fetch_expert(l, slot, own, other, bufs, sem):
    ne = own[0].shape[0]

    @pl.when(l < ne)
    def _():
        for src, dst in zip(own, bufs):
            pltpu.make_async_copy(src.at[l], dst.at[slot], sem.at[slot]).start()

    @pl.when(l >= ne)
    def _():
        for src, dst in zip(other, bufs):
            pltpu.make_async_copy(src.at[l - ne], dst.at[slot], sem.at[slot]).start()


def wait_expert(slot, own, bufs, sem):
    for src, dst in zip(own, bufs):
        pltpu.make_async_copy(src.at[0], dst.at[slot], sem.at[slot]).wait()


def ffn(x, w1, w3, w2):
    a1 = dot(x, w1)
    a3 = dot(x, w3)
    act = (jax.nn.silu(a1) * a3).astype(BF)
    return dot(act, w2).astype(BF)


def block_kernel(js, has_acc, comb, dense, *refs):
    refs = list(refs)
    nblk = len(js)
    take = lambda n: [refs.pop(0) for _ in range(n)]
    if any(dense):
        nh_ref, hl_ref = take(2)
    gt_ref, = take(1)
    if comb:
        nch_ref, eg_ref, pos_ref, z_ref = take(4)
        cap = z_ref.shape[0] // pos_ref.shape[0]
    if any(dense):
        us = take(nblk)
        own, other = take(3), take(3)
        nl = 2 * own[0].shape[0]
    accs = [take(1)[0] if h else None for h in has_acc]
    outs = take(nblk)
    acc, asem = take(2)
    if comb:
        cbuf, zbuf, zsem = take(3)
    if any(dense):
        bufs, (ubuf, sem, usem) = take(3), take(3)
    t, d = outs[0].shape

    if any(dense):
        ns = [nh_ref[j] if on else 0 for j, on in zip(js, dense)]
        n = sum(ns)

        def entry(i):
            p = jnp.where(i < ns[0], 0, nblk - 1)
            return p, hl_ref[jnp.where(p == 0, js[0], js[-1]) * nl + i - jnp.where(p == 0, 0, ns[0])]

        @pl.when(n > 0)
        def _():
            fetch_expert(entry(0)[1], 0, own, other, bufs, sem)

        ucp = [pltpu.make_async_copy(us[p], ubuf.at[pl.ds(p * t, t), :], usem) for p in range(nblk)]
        for cp in ucp:
            cp.start()
    for p in range(nblk):
        rows = pl.ds(p * t, t)
        if has_acc[p]:
            pltpu.make_async_copy(accs[p], acc.at[rows, :], asem.at[p]).start()
        else:
            acc[rows, :] = jnp.zeros((t, d), F32)
    for p in range(nblk):
        if has_acc[p]:
            pltpu.make_async_copy(accs[p], acc.at[pl.ds(p * t, t), :], asem.at[p]).wait()

    if comb:
        for p, j in enumerate(js):
            nch = nch_ref[j]

            def get(i, slot):
                src = pl.multiple_of(j * cap + i * CHUNK, CHUNK)
                return pltpu.make_async_copy(z_ref.at[pl.ds(src, CHUNK), :], zbuf.at[slot], zsem.at[slot])

            get(0, 0).start()
            nl = gt_ref.shape[1]
            lane = lax.broadcasted_iota(I32, (1, CHUNK), 1)
            ti = lax.broadcasted_iota(I32, (16, t), 1)
            si = lax.broadcasted_iota(I32, (16, t), 0)
            tparts = jnp.where(si == 0, ti % 256, jnp.where(si == 1, ti // 256, 0)).astype(F32).astype(BF)
            table = jnp.concatenate([*split3(gt_ref[j]), tparts], axis=0)

            @loop(nch)
            def _(i):
                slot = parity(i)

                @pl.when(i + 1 < nch)
                def _():
                    get(i + 1, 1 - slot).start()

                pm, ls = selection(j, i, eg_ref, pos_ref)
                el = jnp.zeros_like(lane)
                for q, l in enumerate(ls):
                    el = jnp.where(lane // PIECE == q, l, el)
                sel = lax.dot_general(table, pm, NT, preferred_element_type=F32)
                tok = (sel[3 * nl:3 * nl + 1] + 256.0 * sel[3 * nl + 1:3 * nl + 2]).astype(I32)
                hot_ = lax.broadcasted_iota(I32, (t, CHUNK), 0) == tok
                sub = lax.broadcasted_iota(I32, (nl, CHUNK), 0) == el
                for k in range(3):
                    gk = jnp.sum(jnp.where(sub, sel[k * nl:(k + 1) * nl], 0.0), axis=0, keepdims=True)
                    cbuf[:, k * CHUNK:(k + 1) * CHUNK] = jnp.where(hot_, gk, 0.0).astype(BF)
                get(i, slot).wait()
                tn = min(1024, d)

                @loop(d // tn)
                def _(m):
                    cs = pl.ds(pl.multiple_of(m * tn, tn), tn)
                    z = zbuf[slot, :, cs]
                    acc[p * t:(p + 1) * t, cs] += dot(cbuf[:], jnp.concatenate([z, z, z], axis=0))

    if any(dense):
        for cp in ucp:
            cp.wait()
        tm = min(HM, t)

        @loop(n)
        def _(i):
            slot = parity(i)
            wait_expert(slot, own, bufs, sem)

            @pl.when(i + 1 < n)
            def _():
                fetch_expert(entry(i + 1)[1], 1 - slot, own, other, bufs, sem)

            p, e = entry(i)
            blk = jnp.where(p == 0, js[0], js[-1])

            @loop(t // tm)
            def _(m):
                rows = pl.ds(pl.multiple_of(p * t + m * tm, tm), tm)
                z = ffn(ubuf[rows, :], bufs[0][slot], bufs[1][slot], bufs[2][slot])
                g = gt_ref[blk, pl.ds(e, 1), pl.ds(pl.multiple_of(m * tm, tm), tm)]
                eye = lax.broadcasted_iota(I32, (tm, tm), 0) == lax.broadcasted_iota(I32, (tm, tm), 1)
                gc = jnp.sum(jnp.where(eye, g, 0.0), axis=1, keepdims=True)
                acc[rows, :] += gc * z.astype(F32)

    if outs[0].dtype == F32:
        done = [pltpu.make_async_copy(acc.at[pl.ds(p * t, t), :], outs[p], asem.at[p]) for p in range(nblk)]
        for cp in done:
            cp.start()
        for cp in done:
            cp.wait()
    else:
        for p in range(nblk):
            outs[p][:] = acc[p * t:(p + 1) * t, :].astype(BF)


def block(js, r, z, us, accs, own, other, dtype, dense, comb=True):
    nblk = len(js)
    t = r.pos.shape[2]
    d = own[0].shape[1]
    ff = own[0].shape[2]
    vm = pl.BlockSpec(memory_space=pltpu.VMEM)
    sm = pl.BlockSpec(memory_space=pltpu.SMEM)
    hb = pl.BlockSpec(memory_space=pl.ANY)
    args, specs, scratch = [], [], []
    if any(dense):
        args += [r.nh, r.hl.reshape(-1)]
        specs += [sm, sm]
    args += [r.gt]
    specs += [vm]
    if comb:
        args += [r.nch, r.eg.reshape(-1), r.pos, z]
        specs += [sm, sm, vm, hb]
    if any(dense):
        args += list(us) + list(own) + list(other)
        specs += [hb] * (nblk + 6)
    args += [v for v in accs if v is not None]
    specs += [hb for v in accs if v is not None]
    scratch += [pltpu.VMEM((nblk * t, d), F32), pltpu.SemaphoreType.DMA((nblk,))]
    if comb:
        scratch += [pltpu.VMEM((t, 3 * CHUNK), BF), pltpu.VMEM((2, CHUNK, d), BF), DMA2]
    if any(dense):
        scratch += [*expert_buffers(d, ff),
                    pltpu.VMEM((nblk * t, d), BF), DMA2, pltpu.SemaphoreType.DMA]
    out = jax.ShapeDtypeStruct((t, d), dtype)
    return pl.pallas_call(
        functools.partial(block_kernel, js, [v is not None for v in accs], comb, dense),
        in_specs=specs, out_specs=[hb if dtype == F32 else vm] * nblk, out_shape=[out] * nblk, scratch_shapes=scratch,
        compiler_params=params(),
        cost_estimate=cost(t * d, 6 * d * ff),
    )(*args)


def split3(g):
    hi = g.astype(BF)
    r = g - hi.astype(F32)
    mid = r.astype(BF)
    lo = (r - mid.astype(F32)).astype(BF)
    return hi, mid, lo


def selection(j, i, eg_ref, pos_ref):
    t = pos_ref.shape[2]
    it = lax.broadcasted_iota(I32, (2 * PIECE, t), 0)
    npc = CHUNK // PIECE
    first = (j * (eg_ref.shape[0] // pos_ref.shape[0] // npc) + i) * npc
    ls = [eg_ref[first + q] for q in range(npc)]
    hits = []
    for q in range(0, npc, 2):
        own, nxt = [pos_ref[j, pl.ds(l, 1), :] for l in ls[q:q + 2]]
        hit = jnp.where(it < PIECE, own, nxt) - (i * CHUNK + q * PIECE) == it
        hits.append(jnp.where(hit, 1.0, 0.0).astype(BF))
    return jnp.concatenate(hits, axis=0), ls


def gather_kernel(js, nch_ref, eg_ref, pos_ref, *refs):
    us = refs[:len(js)]
    x_ref, xbuf, sem = refs[-3:]
    cap = x_ref.shape[0] // pos_ref.shape[0]
    for p, j in enumerate(js):
        nch = nch_ref[j]

        def out(i, slot):
            dst = pl.multiple_of(j * cap + i * CHUNK, CHUNK)
            return pltpu.make_async_copy(xbuf.at[slot], x_ref.at[pl.ds(dst, CHUNK), :], sem.at[slot])

        @loop(nch)
        def _(i):
            slot = parity(i)

            @pl.when(i >= 2)
            def _():
                out(i - 2, slot).wait()

            xbuf[slot] = dot(selection(j, i, eg_ref, pos_ref)[0], us[p][:]).astype(BF)
            out(i, slot).start()

        for k in (2, 1):
            @pl.when(nch >= k)
            def _():
                out(nch - k, parity(nch - k)).wait()


def gather(js, r, us, x):
    nblk = len(js)
    t, d = us[0].shape
    nb = r.eg.shape[0]
    cap = r.eg.shape[1] * PIECE
    vm = pl.BlockSpec(memory_space=pltpu.VMEM)
    sm = pl.BlockSpec(memory_space=pltpu.SMEM)
    hb = pl.BlockSpec(memory_space=pl.ANY)
    return pl.pallas_call(
        functools.partial(gather_kernel, js),
        in_specs=[sm, sm, vm] + [vm] * nblk + ([hb] if x is not None else []),
        out_specs=hb,
        out_shape=jax.ShapeDtypeStruct((nb * cap, d), BF),
        input_output_aliases={3 + nblk: 0} if x is not None else {},
        scratch_shapes=[pltpu.VMEM((2, CHUNK, d), BF), DMA2],
        compiler_params=params(),
        cost_estimate=cost(t * d, 4 * CHUNK * d),
    )(r.nch, r.eg.reshape(-1), r.pos, *us, *([x] if x is not None else []))


def cold_kernel(nt_ref, tl_ref, tp_ref, tn_ref, tw_ref, tf_ref, nx_ref, pc_ref, x_ref, *refs):
    own, other, z_ref, refs = refs[:3], refs[3:6], refs[6], refs[7:]
    bufs, (xbuf, zbuf, wsem, xsem, zsem) = refs[:3], refs[3:]
    nt = nt_ref[0]

    def each(n, fn):
        @loop(lax.div(n, 2))
        def _(i):
            fn(2 * i)
            fn(2 * i + 1)

        @pl.when(parity(n) == 1)
        def _():
            fn(n - 1)

    def xin(q, slot):
        p0 = tp_ref[q]

        def one(i):
            src = pl.ds(pl.multiple_of(pc_ref[p0 + i] * PIECE, PIECE), PIECE)
            dst = pl.ds(pl.multiple_of(i * PIECE, PIECE), PIECE)
            pltpu.make_async_copy(x_ref.at[src, :], xbuf.at[slot, dst, :], xsem.at[slot]).start()

        each(tn_ref[q], one)

    def zout(q, slot):
        p0 = tp_ref[q]

        def one(i):
            src = pl.ds(pl.multiple_of(i * PIECE, PIECE), PIECE)
            dst = pl.ds(pl.multiple_of(pc_ref[p0 + i] * PIECE, PIECE), PIECE)
            pltpu.make_async_copy(zbuf.at[slot, src, :], z_ref.at[dst, :], zsem.at[slot]).start()

        each(tn_ref[q], one)

    def drain(n, fn):
        bit = 1
        while bit <= MT // PIECE:
            @pl.when(lax.rem(lax.div(n, bit), 2) == 1)
            def _(bit=bit):
                fn(pl.ds(0, bit * PIECE))

            bit *= 2

    def xwait(q, slot):
        drain(tn_ref[q], lambda r: pltpu.make_async_copy(x_ref.at[r, :], xbuf.at[slot, r, :], xsem.at[slot]).wait())

    def zwait(q, slot):
        drain(tn_ref[q], lambda r: pltpu.make_async_copy(zbuf.at[slot, r, :], z_ref.at[r, :], zsem.at[slot]).wait())

    @pl.when(nt > 0)
    def _():
        fetch_expert(tl_ref[0], 0, own, other, bufs, wsem)
        xin(0, 0)

    @loop(nt)
    def _(q):
        slot = parity(q)
        ws = parity(tw_ref[q])

        @pl.when(tf_ref[q] == 1)
        def _():
            wait_expert(ws, own, bufs, wsem)

            @pl.when(nx_ref[q] >= 0)
            def _():
                fetch_expert(nx_ref[q], 1 - ws, own, other, bufs, wsem)

        @pl.when(q + 1 < nt)
        def _():
            xin(q + 1, 1 - slot)

        xwait(q, slot)

        @pl.when(q >= 2)
        def _():
            zwait(q - 2, slot)

        zbuf[slot] = ffn(xbuf[slot], bufs[0][ws], bufs[1][ws], bufs[2][ws])
        zout(q, slot)

    for k in (2, 1):
        @pl.when(nt >= k)
        def _():
            zwait(nt - k, parity(nt - k))


def cold(plan, x, own, other):
    d, ff = own[0].shape[1:]
    sm = pl.BlockSpec(memory_space=pltpu.SMEM)
    hb = pl.BlockSpec(memory_space=pl.ANY)
    return pl.pallas_call(
        cold_kernel,
        in_specs=[sm] * len(plan) + [hb] * 7,
        out_specs=hb,
        out_shape=jax.ShapeDtypeStruct(x.shape, BF),
        scratch_shapes=[*expert_buffers(d, ff),
                        pltpu.VMEM((2, MT, d), BF), pltpu.VMEM((2, MT, d), BF),
                        DMA2, DMA2, DMA2],
        input_output_aliases={len(plan): 0},
        compiler_params=params(),
        cost_estimate=cost(6 * 16 * MT * d * ff, 96 * d * ff),
    )(*plan, x, *own, *other)


def final_kernel(h_ref, *refs):
    y_ref = refs[-1]
    acc, parts = refs[0], refs[1:-1]
    y = h_ref[:].astype(F32) + acc[:]
    for v in parts:
        y = y + v[:].astype(F32)
    y_ref[:] = y.astype(BF)


def final(h, accs, parts):
    t, d = h.shape
    half = t // 2
    tm = min(128, half)
    n = half // tm

    def body(h_ref, *refs):
        for p in range(2):
            @pl.when(pl.program_id(0) // n == p)
            def _():
                final_kernel(h_ref, refs[p], *refs[2 + p:-1:2], refs[-1])

    spec = lambda p: pl.BlockSpec((tm, d), lambda i: (jnp.minimum(i, n - 1) if p == 0 else jnp.maximum(i - n, 0), 0))
    return pl.pallas_call(
        body, grid=(2 * n,),
        in_specs=[pl.BlockSpec((tm, d), lambda i: (i, 0))] + [spec(0), spec(1)] * (1 + len(parts)),
        out_specs=pl.BlockSpec((tm, d), lambda i: (i, 0)),
        out_shape=jax.ShapeDtypeStruct((t, d), BF),
        compiler_params=params(),
        cost_estimate=cost(6 * t * d, 20 * t * d),
    )(h, *accs, *[v for part in parts for v in part])


class Routing(typing.NamedTuple):
    nh: typing.Any
    hl: typing.Any
    nch: typing.Any
    eg: typing.Any
    pos: typing.Any
    gt: typing.Any


def routing_plan(lid, local, nl):
    nb, t, k = lid.shape
    le = jnp.arange(nl, dtype=I32)
    hit = jnp.any((lid[:, None] == le[:, None, None]) & local[:, None], axis=-1)
    tri = (jnp.arange(t)[:, None] <= jnp.arange(t)[None, :]).astype(BF)
    rank = lax.dot_general(hit.astype(BF), tri, (((2,), (0,)), ((), ())), preferred_element_type=F32).astype(I32)
    cnt = rank[:, :, -1]
    hotm = cnt >= t // 2
    scnt = jnp.where(hotm, 0, cnt)
    pcs = (scnt + PIECE - 1) // PIECE
    pend = jnp.cumsum(pcs, axis=1)
    base = (pend - pcs) * PIECE
    pos = jnp.where(hit & ~hotm[..., None], base[..., None] + rank - 1, -1)
    rows = t * k + nl * PIECE
    npb = -(-rows // CHUNK) * CHUNK // PIECE
    nch = jnp.maximum(-(-pend[:, -1] * PIECE // CHUNK), 1)
    below = lambda ends, q: jnp.sum((ends <= q).astype(I32), axis=-1)
    eg = jnp.minimum(below(pend[:, None, :], jnp.arange(npb, dtype=I32)[None, :, None]), nl - 1)
    flat = pcs.T.reshape(-1)
    fend = jnp.cumsum(flat)
    p = jnp.arange(nb * npb, dtype=I32)[:, None]
    seg = jnp.minimum(below(fend[None, :], p), nl * nb - 1)
    inseg = seg[:, None] == jnp.arange(nl * nb, dtype=I32)
    shift_ = jnp.tile(jnp.arange(nb, dtype=I32) * npb, nl) + (pend - pcs).T.reshape(-1) - (fend - flat)
    pc = jnp.clip(p[:, 0] + jnp.sum(jnp.where(inseg, shift_, 0), axis=1), 0, nb * npb - 1)
    ppt = MT // PIECE
    ptot = jnp.sum(pcs, axis=0)
    pstart = jnp.cumsum(ptot) - ptot
    tiles = (ptot + ppt - 1) // ppt
    tend = jnp.cumsum(tiles)
    nq = -(-(nb * npb) // ppt) + nl
    q = jnp.arange(nq, dtype=I32)
    tl = jnp.minimum(below(tend[None, :], q[:, None]), nl - 1)
    one = tl[:, None] == le
    pick = lambda v: jnp.sum(jnp.where(one, v[None, :], 0), axis=1)
    ti = q - pick(tend - tiles)
    tp = pick(pstart) + ti * ppt
    tn = jnp.clip(pick(ptot) - ti * ppt, 0, ppt)
    active = (tiles > 0).astype(I32)
    tw = pick(jnp.cumsum(active) - active)
    tf = (ti == 0).astype(I32)
    later = (le[None, :] > tl[:, None]) & (active[None, :] > 0)
    nxt = jnp.min(jnp.where(later, le[None, :], nl), axis=1)
    nxt = jnp.where(nxt < nl, nxt, -1)
    plan = tuple(v.astype(I32) for v in (tend[-1:], tl, tp, tn, tw, tf, nxt, pc))
    hend = jnp.cumsum(hotm.astype(I32), axis=1)
    hl = jnp.minimum(below(hend[:, None, :], le[None, :, None]), nl - 1)
    return Routing(hend[:, -1], hl, nch, eg, pos, None), plan


ON = (True,)


def solution(mesh):
    nd = mesh.shape['ep']
    nx = nd // 2
    tok_spec = P(('replica', 'ep'), None, None)
    rows_ep = P('ep', None)
    by_expert = P('ep', None, None)

    def shift(v, s):
        return lax.ppermute(v, 'ep', [(2 * i + c, 2 * ((i + s) % nx) + c) for i in range(nx) for c in range(2)])

    def partner(v):
        return lax.ppermute(v, 'ep', [(i, i ^ 1) for i in range(nd)])

    def local(x, wq, wk, wv, wo, wr, w1, w3, w2, idx):
        b, s, d = x.shape
        t, k, ne = b * s, idx.shape[-1], w1.shape[0]
        nl = 2 * ne
        half = t // 2
        me = lax.axis_index('ep')
        x = x.reshape(t, d)
        ids = idx.reshape(t, k)

        ids4 = jnp.stack([ids, shift(ids, 1), shift(ids, -1), shift(ids, 2)])
        hd = HEAD // 2
        freq = THETA ** (-jnp.arange(hd, dtype=F32) / hd)
        ang = (jnp.arange(t) % s).astype(F32)[:, None] * freq
        c, sn = jnp.cos(ang), jnp.sin(ang)
        cos, sin = jnp.concatenate([c, c], axis=1), jnp.concatenate([-sn, sn], axis=1)
        x, cos, sin, ids4 = lax.optimization_barrier((x, cos, sin, ids4))
        h, ut, ub, o1, o3 = attention_layer(nx, x, wv, wk, wq, wo, cos, sin, w1, w3)
        ids4, w2, ut, ub = lax.optimization_barrier((ids4, w2, ut, ub))
        o2 = partner(w2)
        own, other = (w1, w3, w2), (o1, o3, o2)

        halves = lambda v: v.reshape(2 * v.shape[0], half, *v.shape[2:])
        is_local = halves(ids4 // nl == me // 2)
        lid = halves((ids4 - me * ne) % nl)
        r, plan = routing_plan(lid, is_local, nl)
        ohl = (lid[:, None] == jnp.arange(nl, dtype=I32)[:, None, None]) & is_local[:, None]
        A, R, L, O = (0, 1), (2, 3), (4, 5), (6, 7)
        ra = r._replace(pos=r.pos[:2])

        u1t, u2b = shift(ut, 1), shift(ub, -1)
        logits = jnp.dot(rmsnorm(h), wr, precision=lax.Precision.HIGHEST, preferred_element_type=F32)
        oh = ids[..., None] == jnp.arange(wr.shape[1], dtype=I32)
        g = jax.nn.softmax(jnp.sum(jnp.where(oh, logits[:, None, :], 0.0), axis=-1), axis=-1)
        ut2, ub2, g = lax.optimization_barrier((ut, ub, g))
        g4 = [g, shift(g, 1), shift(g, -1), shift(g, 2)]
        u1b, u2t = shift(ub2, 1), shift(ut2, -1)
        spread = lambda o, v: jnp.sum(jnp.where(o, halves(v)[:, None], 0.0), axis=3)
        ra = ra._replace(gt=spread(ohl[:2], g[None]))
        r = r._replace(gt=spread(ohl, jnp.stack(g4)))

        x = gather(A, r, (ut, ub), None)
        a0, = block((0,), ra, None, (ut,), (None,), own, other, F32, ON, comb=False)
        a0, x, u1t, u2b = lax.optimization_barrier((a0, x, u1t, u2b))
        u3t, u3b = shift(u1t, 1), shift(u2b, -1)
        d2, d5 = block((2, 5), r, None, (u1t, u2b), (None, None), own, other, F32, 2 * ON, comb=False)
        u1b, d2 = lax.optimization_barrier((u1b, d2))
        x = gather(R, r, (u1t, u1b), x)
        x = gather(L, r, (u2t, u2b), x)
        u3t, x = lax.optimization_barrier((u3t, x))
        x = gather(O, r, (u3t, u3b), x)
        z = cold(plan, x, own, other)

        tie = lambda r, *v: (lambda w: (r._replace(nch=w[0]), *w[1:]))(lax.optimization_barrier((r.nch, *v)))
        b2, b5 = block((2, 5), r, z, (), (d2, d5), own, other, BF, (False, False))
        r, b2, b5 = tie(r, b2, b5)
        b2, b5 = shift(b2, -1), shift(b5, 1)
        b6, b7 = block(O, r, z, (u3t, u3b), (None, None), own, other, BF, 2 * ON)
        r, b6, b7 = tie(r, b6, b7)
        c6, c7 = shift(b6, 1), shift(b7, -1)
        b3, = block((3,), r, z, (u1b,), (None,), own, other, BF, ON)
        r, b3 = tie(r, b3)
        b3 = shift(b3, -1)
        b4, = block((4,), r, z, (u2t,), (None,), own, other, BF, ON)
        r, b4, c6, c7 = tie(r, b4, c6, c7)
        b4 = shift(b4, 1)
        b6, b7 = shift(c6, 1), shift(c7, -1)
        accs = block(A, r, z, (ut, ub), (a0, None), own, other, F32, (False, True))
        y = final(h, accs, [(b2, b3), (b4, b5), (b6, b7)])
        return y.reshape(b, s, d)

    return jax.shard_map(local, mesh=mesh,
                         in_specs=(tok_spec, rows_ep, rows_ep, rows_ep, rows_ep, P(None, None),
                                   by_expert, by_expert, by_expert, tok_spec),
                         out_specs=tok_spec, check_vma=False)
```

```python
import functools
import math
import typing
import jax
import jax.numpy as jnp
import numpy as np
from jax import lax
from jax.experimental import pallas as pl
from jax.experimental.pallas import tpu as pltpu
from jax.sharding import PartitionSpec as P

HEAD = 128
EPS = 1e-6
THETA = 10000.0
PIECE = 8
CHUNK = 256
MT = 352
HM = 256
VMEM = 66_000_000
BF, F32, I32 = jnp.bfloat16, jnp.float32, jnp.int32


def rmsnorm(v):
    v = v.astype(F32)
    return v * lax.rsqrt(jnp.mean(v * v, axis=-1, keepdims=True) + EPS)


def dot(a, b):
    return jnp.dot(a, b, preferred_element_type=F32)


NT = (((1,), (1,)), ((), ()))
TN = (((0,), (0,)), ((), ()))
DMA2 = pltpu.SemaphoreType.DMA((2,))


def cost(flops, bytes_):
    return pl.CostEstimate(flops=flops, bytes_accessed=bytes_, transcendentals=0)


def parity(i):
    return lax.rem(i, 2)


def expert_buffers(d, ff):
    return [pltpu.VMEM((2, *v), BF) for v in ((d, ff), (d, ff), (ff, d))]


def loop(n):
    return pl.loop(0, n)


def params(**kw):
    return pltpu.CompilerParams(vmem_limit_bytes=VMEM, **kw)


def split3(g):
    hi = g.astype(BF)
    r = g - hi.astype(F32)
    mid = r.astype(BF)
    lo = (r - mid.astype(F32)).astype(BF)
    return hi, mid, lo


LT, LB, RT, RB, OT, OB, PO, PASS = 0, 1, 2, 3, 4, 5, 6, 7
MESH = pl.DeviceIdType.MESH


def layer_kernel(nx, x_ref, wv_ref, wk_ref, wq_ref, wo_ref, cos_ref, sin_ref, w1_ref, w3_ref, wr_ref, id_ref,
                 h_ref, ut_ref, ub_ref, o1_ref, o3_ref, lg_ref, id4_ref,
                 w_ref, ab, qb, kb, vb, rb3, ssem, rsem, lsem, iosem, swap_send, swap_recv, id_send, id_recv):
    shards = (wv_ref, wk_ref, wq_ref, wo_ref)
    sh = wv_ref.shape[0]
    hs = sh // 2
    t, d = ab.shape
    me = lax.axis_index("ep")
    chip, core = me // 2, me % 2
    right, left, opp = [2 * ((chip + k) % nx) + core for k in (1, nx - 1, 2)]
    partner = 2 * chip + 1 - core

    barrier = pltpu.get_barrier_semaphore()
    around = (right, left, opp)
    for dev in (*around, partner):
        pl.semaphore_signal(barrier, inc=1, device_id={"ep": dev}, device_id_type=MESH)
    pl.semaphore_wait(barrier, 4)

    def rows(e, half=None):
        if half is None:
            return pl.ds(pl.multiple_of(e * sh, sh), sh)
        return pl.ds(pl.multiple_of(e * sh + half * hs, hs), hs)

    def remote(w, src, dst, dev, s, r):
        return pltpu.make_async_remote_copy(src_ref=src, dst_ref=w_ref.at[w, dst, :], send_sem=ssem.at[w, s],
                                            recv_sem=rsem.at[w, r], device_id={"ep": dev}, device_id_type=MESH)

    def own(w):
        src = shards[w]
        top, bot = src.at[pl.ds(0, hs), :], src.at[pl.ds(hs, hs), :]
        return [remote(w, top, rows(me, 0), right, 0, LT), remote(w, bot, rows(me, 1), left, 1, RB),
                remote(w, bot, rows(me, 1), right, 2, LB), remote(w, top, rows(me, 0), left, 3, RT),
                remote(w, src, rows(me), partner, 6, PO)]

    def mine(w):
        return pltpu.make_async_copy(shards[w], w_ref.at[w, rows(me), :], lsem.at[w])

    where = {LT: (left, 0), LB: (left, 1), RT: (right, 0), RB: (right, 1), OT: (opp, 0), OB: (opp, 1)}

    def onward(w, k):
        e, half = where[LT if k == OT else RB]
        return remote(w, w_ref.at[w, rows(e, half), :], rows(e, half), right if k == OT else left, 4 if k == OT else 5, k)

    def across(w, k):
        r = rows(*where[k])
        return remote(w, w_ref.at[w, r, :], r, partner, PASS + k, PASS + k)

    def arrive(w, k):
        r = rows(me) if k == PO else rows(*where[k % PASS])
        remote(w, w_ref.at[w, r, :], r, partner, 0, k).wait_recv()

    def begin(w):
        for c in own(w):
            c.start()
        mine(w).start()

    def stage_a(w):
        arrive(w, LT)
        onward(w, OT).start()
        arrive(w, RB)
        onward(w, OB).start()
        if w + 1 < 4:
            begin(w + 1)
        across(w, LT).start()
        across(w, RB).start()
        swap()

    def stage_b(w):
        for k in (LB, RT):
            arrive(w, k)
            across(w, k).start()
        if w != 2:
            swap()
        if w == 3:
            swap()

    def stage_c(w):
        for k in (OT, OB):
            arrive(w, k)
            across(w, k).start()
        if w != 2:
            swap()

    def stage_d(w):
        for k in (PO, PASS + LT, PASS + RB, PASS + LB, PASS + RT, PASS + OT, PASS + OB):
            arrive(w, k)
        mine(w).wait()

    pieces = [(src.at[e], dst.at[e]) for e in range(w1_ref.shape[0]) for src, dst in ((w1_ref, o1_ref), (w3_ref, o3_ref))]
    swaps = [pltpu.make_async_remote_copy(src_ref=src, dst_ref=dst, send_sem=swap_send.at[i], recv_sem=swap_recv.at[i],
                                          device_id={"ep": partner}, device_id_type=MESH) for i, (src, dst) in enumerate(pieces)]
    waiting = list(swaps)

    def swap():
        if waiting:
            waiting.pop(0).start()

    ids = [pltpu.make_async_remote_copy(src_ref=id_ref, dst_ref=id4_ref.at[k + 1], send_sem=id_send.at[k], recv_sem=id_recv.at[k],
                                        device_id={"ep": dev}, device_id_type=MESH) for k, dev in enumerate(around)]
    ids.append(pltpu.make_async_copy(id_ref, id4_ref.at[0], id_send.at[3]))
    begin(0)
    for c in ids:
        c.start()
    swap()
    xin = pltpu.make_async_copy(x_ref, kb, iosem.at[0])
    xin.start()
    xin.wait()
    rb = min(256, t)
    rb3[:] = jnp.concatenate([*split3(wr_ref[:]), jnp.zeros(wr_ref.shape, BF)], axis=1)

    @loop(t // rb)
    def _(i):
        r = pl.ds(pl.multiple_of(i * rb, rb), rb)
        ab[r, :] = rmsnorm(kb[r, :]).astype(BF)

    tm, tn = min(512, t), min(512, d)

    def project(w, dst, rope):
        @loop(d // tn)
        def _(n):
            @loop(t // tm)
            def _(m):
                r = pl.ds(pl.multiple_of(m * tm, tm), tm)
                z = dot(ab[r, :], w_ref[w, :, pl.ds(pl.multiple_of(n * tn, tn), tn)])
                for j in range(tn // HEAD):
                    zj = z[:, j * HEAD:(j + 1) * HEAD]
                    if rope:
                        zj = zj * cos_ref[r, :] + pltpu.roll(zj, HEAD // 2, 1) * sin_ref[r, :]
                    dst[r, pl.ds(pl.multiple_of(n * tn + j * HEAD, HEAD), HEAD)] = zj.astype(BF)

    for w, (dst, rope) in enumerate(((vb, False), (kb, True), (qb, True))):
        stage_a(w)
        stage_b(w)
        stage_c(w)
        stage_d(w)
        swap()
        if w == 2:
            swap()
        project(w, dst, rope)
    stage_a(3)

    tq = min(256, t)
    scale = math.log2(math.e) / math.sqrt(HEAD)
    causal = lax.broadcasted_iota(I32, (tq, tq), 0) <= lax.broadcasted_iota(I32, (tq, tq), 1)
    group = min(4, d // HEAD)
    steps = d // HEAD // group
    marks = {1: stage_b, steps - 1: stage_c}
    if len(marks) > steps - 1:
        marks = {}
        stage_b(3)
        stage_c(3)

    @loop(steps)
    def _(jj):
        for at, stage in marks.items():
            pl.when(jj == at)(functools.partial(stage, 3))
        for j in range(group):
            c = pl.ds(pl.multiple_of((jj * group + j) * HEAD, HEAD), HEAD)
            for i in range(t // tq):
                r, n = slice(i * tq, (i + 1) * tq), (i + 1) * tq
                sc = lax.dot_general(kb[:n, c], qb[r, c], NT, preferred_element_type=F32)
                diag = jnp.where(causal, sc[i * tq:], -jnp.inf)
                sc = jnp.concatenate([sc[:i * tq], diag], axis=0) if i else diag
                p = jnp.exp2((sc - jnp.max(sc, axis=0, keepdims=True)) * scale)
                p = (p * (1.0 / jnp.sum(p, axis=0, keepdims=True))).astype(BF)
                qb[r, c] = lax.dot_general(p, vb[:n, c], TN, preferred_element_type=F32).astype(BF)

    xin = pltpu.make_async_copy(x_ref, vb, iosem.at[0])
    xin.start()
    stage_d(3)
    xin.wait()

    @loop(d // tn)
    def _(n):
        c = pl.ds(pl.multiple_of(n * tn, tn), tn)

        @loop(t // tm)
        def _(m):
            r = pl.ds(pl.multiple_of(m * tm, tm), tm)
            ab[r, c] = (vb[r, c].astype(F32) + dot(qb[r, :], w_ref[3, :, c])).astype(BF)

    hout = pltpu.make_async_copy(ab, h_ref, iosem.at[0])
    hout.start()

    @loop(t // rb)
    def _(i):
        r = pl.ds(pl.multiple_of(i * rb, rb), rb)
        hi, mid, lo = split3(rmsnorm(ab[r, :]))
        kb[r, :] = hi
        ne = wr_ref.shape[1]
        part = lambda v, k: v[:, k * ne:(k + 1) * ne]
        p1, p2, p3 = dot(hi, rb3[:]), dot(mid, rb3[:, :2 * ne]), dot(lo, rb3[:, :2 * ne])
        lg_ref[r, :] = part(p1, 0) + ((part(p1, 1) + part(p2, 0)) + (part(p1, 2) + part(p2, 1) + part(p3, 0)))

    uout = [pltpu.make_async_copy(kb.at[pl.ds(p * t // 2, t // 2), :], o, iosem.at[1 + p]) for p, o in enumerate((ut_ref, ub_ref))]
    for c in uout:
        c.start()
    while waiting:
        swap()
    for c in swaps + ids:
        c.wait()
    for w in range(4):
        for c in own(w) + [onward(w, OT), onward(w, OB)] + [across(w, k) for k in where]:
            c.wait_send()
    hout.wait()
    for c in uout:
        c.wait()


def attention_layer(nx, x, wv, wk, wq, wo, cos, sin, w1, w3, wr, ids):
    t, d = x.shape
    hb = pl.BlockSpec(memory_space=pl.ANY)
    vm = pl.BlockSpec(memory_space=pltpu.VMEM)
    half = jax.ShapeDtypeStruct((t // 2, d), BF)
    act = pltpu.VMEM((t, d), BF)
    return pl.pallas_call(
        functools.partial(layer_kernel, nx),
        in_specs=[hb] * 5 + [vm] * 2 + [hb] * 2 + [vm, hb],
        out_specs=[hb] * 5 + [vm, hb],
        out_shape=[jax.ShapeDtypeStruct((t, d), BF), half, half, jax.ShapeDtypeStruct(w1.shape, BF),
                   jax.ShapeDtypeStruct(w3.shape, BF), jax.ShapeDtypeStruct((t, wr.shape[1]), F32),
                   jax.ShapeDtypeStruct((nx, *ids.shape), I32)],
        scratch_shapes=[pltpu.VMEM((4, d, d), BF), act, act, act, act, pltpu.VMEM((d, 4 * wr.shape[1]), BF),
                        pltpu.SemaphoreType.DMA((4, 13)), pltpu.SemaphoreType.DMA((4, 13)),
                        pltpu.SemaphoreType.DMA((4,)), pltpu.SemaphoreType.DMA((3,)),
                        pltpu.SemaphoreType.DMA((2 * w1.shape[0],)), pltpu.SemaphoreType.DMA((2 * w1.shape[0],)),
                        pltpu.SemaphoreType.DMA((nx,)), pltpu.SemaphoreType.DMA((nx,))],
        compiler_params=params(collective_id=0, has_side_effects=True),
        cost_estimate=cost(8 * t * d * d, 24 * t * d),
    )(x, wv, wk, wq, wo, cos, sin, w1, w3, wr, ids)


def fetch_expert(l, slot, own, other, bufs, sem):
    ne = own[0].shape[0]

    @pl.when(l < ne)
    def _():
        for src, dst in zip(own, bufs):
            pltpu.make_async_copy(src.at[l], dst.at[slot], sem.at[slot]).start()

    @pl.when(l >= ne)
    def _():
        for src, dst in zip(other, bufs):
            pltpu.make_async_copy(src.at[l - ne], dst.at[slot], sem.at[slot]).start()


def wait_expert(slot, own, bufs, sem):
    for src, dst in zip(own, bufs):
        pltpu.make_async_copy(src.at[0], dst.at[slot], sem.at[slot]).wait()


def ffn(x, w1, w3, w2):
    a1 = dot(x, w1)
    a3 = dot(x, w3)
    act = (jax.nn.silu(a1) * a3).astype(BF)
    return dot(act, w2).astype(BF)


def block_kernel(js, has_acc, comb, dense, *refs):
    refs = list(refs)
    nblk = len(js)
    take = lambda n: [refs.pop(0) for _ in range(n)]
    if any(dense):
        nh_ref, hl_ref = take(2)
    gt_ref, = take(1)
    if comb:
        nch_ref, eg_ref, pos_ref, z_ref = take(4)
        cap = z_ref.shape[0] // pos_ref.shape[0]
    if any(dense):
        us = take(nblk)
        own, other = take(3), take(3)
        nl = 2 * own[0].shape[0]
    accs = [take(1)[0] if h else None for h in has_acc]
    outs = take(nblk)
    acc, asem = take(2)
    if comb:
        cbuf, zbuf, zsem = take(3)
    if any(dense):
        bufs, (ubuf, sem, usem) = take(3), take(3)
    t, d = outs[0].shape

    if any(dense):
        ns = [nh_ref[j] if on else 0 for j, on in zip(js, dense)]
        n = sum(ns)

        def entry(i):
            p, j, k, end = 0, js[0], i, 0
            for q in range(nblk - 1):
                end = end + ns[q]
                past = i >= end
                p, j, k = jnp.where(past, q + 1, p), jnp.where(past, js[q + 1], j), jnp.where(past, i - end, k)
            return p, j, hl_ref[j * nl + k]

        @pl.when(n > 0)
        def _():
            fetch_expert(entry(0)[-1], 0, own, other, bufs, sem)

        ucp = [pltpu.make_async_copy(us[p], ubuf.at[pl.ds(p * t, t), :], usem) for p in range(nblk)]
        for cp in ucp:
            cp.start()
    for p in range(nblk):
        rows = pl.ds(p * t, t)
        if has_acc[p]:
            pltpu.make_async_copy(accs[p], acc.at[rows, :], asem.at[p]).start()
        else:
            acc[rows, :] = jnp.zeros((t, d), F32)
    for p in range(nblk):
        if has_acc[p]:
            pltpu.make_async_copy(accs[p], acc.at[pl.ds(p * t, t), :], asem.at[p]).wait()

    if comb:
        for p, j in enumerate(js):
            nch = nch_ref[j]

            def get(i, slot):
                src = pl.multiple_of(j * cap + i * CHUNK, CHUNK)
                return pltpu.make_async_copy(z_ref.at[pl.ds(src, CHUNK), :], zbuf.at[slot], zsem.at[slot])

            get(0, 0).start()
            nl = gt_ref.shape[1]
            lane = lax.broadcasted_iota(I32, (1, CHUNK), 1)
            ti = lax.broadcasted_iota(I32, (16, t), 1)
            si = lax.broadcasted_iota(I32, (16, t), 0)
            tparts = jnp.where(si == 0, ti % 256, jnp.where(si == 1, ti // 256, 0)).astype(F32).astype(BF)
            table = jnp.concatenate([*split3(gt_ref[j]), tparts], axis=0)

            @loop(nch)
            def _(i):
                slot = parity(i)

                @pl.when(i + 1 < nch)
                def _():
                    get(i + 1, 1 - slot).start()

                pm, ls = selection(j, i, eg_ref, pos_ref)
                el = jnp.zeros_like(lane)
                for q, l in enumerate(ls):
                    el = jnp.where(lane // PIECE == q, l, el)
                sel = lax.dot_general(table, pm, NT, preferred_element_type=F32)
                tok = (sel[3 * nl:3 * nl + 1] + 256.0 * sel[3 * nl + 1:3 * nl + 2]).astype(I32)
                hot_ = lax.broadcasted_iota(I32, (t, CHUNK), 0) == tok
                sub = lax.broadcasted_iota(I32, (nl, CHUNK), 0) == el
                for k in range(3):
                    gk = jnp.sum(jnp.where(sub, sel[k * nl:(k + 1) * nl], 0.0), axis=0, keepdims=True)
                    cbuf[:, k * CHUNK:(k + 1) * CHUNK] = jnp.where(hot_, gk, 0.0).astype(BF)
                get(i, slot).wait()
                tn = min(1024, d)

                @loop(d // tn)
                def _(m):
                    cs = pl.ds(pl.multiple_of(m * tn, tn), tn)
                    z = zbuf[slot, :, cs]
                    acc[p * t:(p + 1) * t, cs] += dot(cbuf[:], jnp.concatenate([z, z, z], axis=0))

    if any(dense):
        for cp in ucp:
            cp.wait()
        tm = min(HM, t)

        @loop(n)
        def _(i):
            slot = parity(i)
            wait_expert(slot, own, bufs, sem)

            @pl.when(i + 1 < n)
            def _():
                fetch_expert(entry(i + 1)[-1], 1 - slot, own, other, bufs, sem)

            p, blk, e = entry(i)

            @loop(t // tm)
            def _(m):
                rows = pl.ds(pl.multiple_of(p * t + m * tm, tm), tm)
                z = ffn(ubuf[rows, :], bufs[0][slot], bufs[1][slot], bufs[2][slot])
                g = gt_ref[blk, pl.ds(e, 1), pl.ds(pl.multiple_of(m * tm, tm), tm)]
                eye = lax.broadcasted_iota(I32, (tm, tm), 0) == lax.broadcasted_iota(I32, (tm, tm), 1)
                gc = jnp.sum(jnp.where(eye, g, 0.0), axis=1, keepdims=True)
                acc[rows, :] += gc * z.astype(F32)

    if outs[0].dtype == F32:
        done = [pltpu.make_async_copy(acc.at[pl.ds(p * t, t), :], outs[p], asem.at[p]) for p in range(nblk)]
        for cp in done:
            cp.start()
        for cp in done:
            cp.wait()
    else:
        for p in range(nblk):
            outs[p][:] = acc[p * t:(p + 1) * t, :].astype(BF)


def block(js, r, z, us, accs, own, other, dtype, dense, comb=True):
    nblk = len(js)
    t = r.pos.shape[2]
    d = own[0].shape[1]
    ff = own[0].shape[2]
    vm = pl.BlockSpec(memory_space=pltpu.VMEM)
    sm = pl.BlockSpec(memory_space=pltpu.SMEM)
    hb = pl.BlockSpec(memory_space=pl.ANY)
    args, specs, scratch = [], [], []
    if any(dense):
        args += [r.nh, r.hl.reshape(-1)]
        specs += [sm, sm]
    args += [r.gt]
    specs += [vm]
    if comb:
        args += [r.nch, r.eg.reshape(-1), r.pos, z]
        specs += [sm, sm, vm, hb]
    if any(dense):
        args += list(us) + list(own) + list(other)
        specs += [hb] * (nblk + 6)
    args += [v for v in accs if v is not None]
    specs += [hb for v in accs if v is not None]
    scratch += [pltpu.VMEM((nblk * t, d), F32), pltpu.SemaphoreType.DMA((nblk,))]
    if comb:
        scratch += [pltpu.VMEM((t, 3 * CHUNK), BF), pltpu.VMEM((2, CHUNK, d), BF), DMA2]
    if any(dense):
        scratch += [*expert_buffers(d, ff),
                    pltpu.VMEM((nblk * t, d), BF), DMA2, pltpu.SemaphoreType.DMA]
    out = jax.ShapeDtypeStruct((t, d), dtype)
    return pl.pallas_call(
        functools.partial(block_kernel, js, [v is not None for v in accs], comb, dense),
        in_specs=specs, out_specs=[hb if dtype == F32 else vm] * nblk, out_shape=[out] * nblk, scratch_shapes=scratch,
        compiler_params=params(),
        cost_estimate=cost(t * d, 6 * d * ff),
    )(*args)


def selection(j, i, eg_ref, pos_ref):
    t = pos_ref.shape[2]
    it = lax.broadcasted_iota(I32, (2 * PIECE, t), 0)
    npc = CHUNK // PIECE
    first = (j * (eg_ref.shape[0] // pos_ref.shape[0] // npc) + i) * npc
    ls = [eg_ref[first + q] for q in range(npc)]
    hits = []
    for q in range(0, npc, 2):
        own, nxt = [pos_ref[j, pl.ds(l, 1), :] for l in ls[q:q + 2]]
        hit = jnp.where(it < PIECE, own, nxt) - (i * CHUNK + q * PIECE) == it
        hits.append(jnp.where(hit, 1.0, 0.0).astype(BF))
    return jnp.concatenate(hits, axis=0), ls


def gather_kernel(nch_ref, eg_ref, pos_ref, *refs):
    us, (x_ref, ubuf, xbuf, usem, sem) = refs[:-5], refs[-5:]
    cap = x_ref.shape[0] // pos_ref.shape[0]
    cps = [pltpu.make_async_copy(u, ubuf.at[j % 2], usem.at[j % 2]) for j, u in enumerate(us)]
    cps[0].start()
    for j in range(len(us)):
        nch = nch_ref[j]

        def out(i, slot):
            dst = pl.multiple_of(j * cap + i * CHUNK, CHUNK)
            return pltpu.make_async_copy(xbuf.at[slot], x_ref.at[pl.ds(dst, CHUNK), :], sem.at[slot])

        if j + 1 < len(us):
            cps[j + 1].start()
        cps[j].wait()

        @loop(nch)
        def _(i):
            slot = parity(i)

            @pl.when(i >= 2)
            def _():
                out(i - 2, slot).wait()

            xbuf[slot] = dot(selection(j, i, eg_ref, pos_ref)[0], ubuf[j % 2]).astype(BF)
            out(i, slot).start()

        for k in (2, 1):
            @pl.when(nch >= k)
            def _():
                out(nch - k, parity(nch - k)).wait()


def gather(r, us):
    t, d = us[0].shape
    rows = r.eg.size * PIECE
    vm = pl.BlockSpec(memory_space=pltpu.VMEM)
    sm = pl.BlockSpec(memory_space=pltpu.SMEM)
    hb = pl.BlockSpec(memory_space=pl.ANY)
    return pl.pallas_call(
        gather_kernel,
        in_specs=[sm, sm, vm] + [hb] * len(us),
        out_specs=hb,
        out_shape=jax.ShapeDtypeStruct((rows, d), BF),
        scratch_shapes=[pltpu.VMEM((2, t, d), BF), pltpu.VMEM((2, CHUNK, d), BF), DMA2, DMA2],
        compiler_params=params(),
        cost_estimate=cost(t * d, 4 * CHUNK * d),
    )(r.nch, r.eg.reshape(-1), r.pos, *us)


def cold_kernel(nt_ref, tl_ref, tp_ref, tn_ref, tw_ref, tf_ref, nx_ref, pc_ref, x_ref, *refs):
    own, other, z_ref, refs = refs[:3], refs[3:6], refs[6], refs[7:]
    bufs, (xbuf, zbuf, wsem, xsem, zsem) = refs[:3], refs[3:]
    nt = nt_ref[0]

    def each(n, fn):
        @loop(lax.div(n, 2))
        def _(i):
            fn(2 * i)
            fn(2 * i + 1)

        @pl.when(parity(n) == 1)
        def _():
            fn(n - 1)

    def xin(q, slot):
        p0 = tp_ref[q]

        def one(i):
            src = pl.ds(pl.multiple_of(pc_ref[p0 + i] * PIECE, PIECE), PIECE)
            dst = pl.ds(pl.multiple_of(i * PIECE, PIECE), PIECE)
            pltpu.make_async_copy(x_ref.at[src, :], xbuf.at[slot, dst, :], xsem.at[slot]).start()

        each(tn_ref[q], one)

    def zout(q, slot):
        p0 = tp_ref[q]

        def one(i):
            src = pl.ds(pl.multiple_of(i * PIECE, PIECE), PIECE)
            dst = pl.ds(pl.multiple_of(pc_ref[p0 + i] * PIECE, PIECE), PIECE)
            pltpu.make_async_copy(zbuf.at[slot, src, :], z_ref.at[dst, :], zsem.at[slot]).start()

        each(tn_ref[q], one)

    def drain(n, fn):
        bit = 1
        while bit <= MT // PIECE:
            @pl.when(lax.rem(lax.div(n, bit), 2) == 1)
            def _(bit=bit):
                fn(pl.ds(0, bit * PIECE))

            bit *= 2

    def xwait(q, slot):
        drain(tn_ref[q], lambda r: pltpu.make_async_copy(x_ref.at[r, :], xbuf.at[slot, r, :], xsem.at[slot]).wait())

    def zwait(q, slot):
        drain(tn_ref[q], lambda r: pltpu.make_async_copy(zbuf.at[slot, r, :], z_ref.at[r, :], zsem.at[slot]).wait())

    @pl.when(nt > 0)
    def _():
        fetch_expert(tl_ref[0], 0, own, other, bufs, wsem)
        xin(0, 0)

    @loop(nt)
    def _(q):
        slot = parity(q)
        ws = parity(tw_ref[q])

        @pl.when(tf_ref[q] == 1)
        def _():
            wait_expert(ws, own, bufs, wsem)

            @pl.when(nx_ref[q] >= 0)
            def _():
                fetch_expert(nx_ref[q], 1 - ws, own, other, bufs, wsem)

        @pl.when(q + 1 < nt)
        def _():
            xin(q + 1, 1 - slot)

        xwait(q, slot)

        @pl.when(q >= 2)
        def _():
            zwait(q - 2, slot)

        zbuf[slot] = ffn(xbuf[slot], bufs[0][ws], bufs[1][ws], bufs[2][ws])
        zout(q, slot)

    for k in (2, 1):
        @pl.when(nt >= k)
        def _():
            zwait(nt - k, parity(nt - k))


def cold(plan, x, own, other):
    d, ff = own[0].shape[1:]
    sm = pl.BlockSpec(memory_space=pltpu.SMEM)
    hb = pl.BlockSpec(memory_space=pl.ANY)
    return pl.pallas_call(
        cold_kernel,
        in_specs=[sm] * len(plan) + [hb] * 7,
        out_specs=hb,
        out_shape=jax.ShapeDtypeStruct(x.shape, BF),
        scratch_shapes=[*expert_buffers(d, ff),
                        pltpu.VMEM((2, MT, d), BF), pltpu.VMEM((2, MT, d), BF),
                        DMA2, DMA2, DMA2],
        input_output_aliases={len(plan): 0},
        compiler_params=params(),
        cost_estimate=cost(6 * 16 * MT * d * ff, 96 * d * ff),
    )(*plan, x, *own, *other)


def final_kernel(h_ref, *refs):
    y_ref = refs[-1]
    acc, parts = refs[0], refs[1:-1]
    y = h_ref[:].astype(F32) + acc[:]
    for v in parts:
        y = y + v[:].astype(F32)
    y_ref[:] = y.astype(BF)


def final(h, accs, parts):
    t, d = h.shape
    half = t // 2
    tm = min(128, half)
    n = half // tm

    def body(h_ref, *refs):
        for p in range(2):
            @pl.when(pl.program_id(0) // n == p)
            def _():
                final_kernel(h_ref, refs[p], *refs[2 + p:-1:2], refs[-1])

    spec = lambda p: pl.BlockSpec((tm, d), lambda i: (jnp.minimum(i, n - 1) if p == 0 else jnp.maximum(i - n, 0), 0))
    return pl.pallas_call(
        body, grid=(2 * n,),
        in_specs=[pl.BlockSpec((tm, d), lambda i: (i, 0))] + [spec(0), spec(1)] * (1 + len(parts)),
        out_specs=pl.BlockSpec((tm, d), lambda i: (i, 0)),
        out_shape=jax.ShapeDtypeStruct((t, d), BF),
        compiler_params=params(),
        cost_estimate=cost(6 * t * d, 20 * t * d),
    )(h, *accs, *[v for part in parts for v in part])


class Routing(typing.NamedTuple):
    nh: typing.Any
    hl: typing.Any
    nch: typing.Any
    eg: typing.Any
    pos: typing.Any
    gt: typing.Any


def routing_plan(lid, local, nl):
    nb, t, k = lid.shape
    le = jnp.arange(nl, dtype=I32)
    hit = jnp.any((lid[:, None] == le[:, None, None]) & local[:, None], axis=-1)
    tri = (jnp.arange(t)[:, None] <= jnp.arange(t)[None, :]).astype(BF)
    rank = lax.dot_general(hit.astype(BF), tri, (((2,), (0,)), ((), ())), preferred_element_type=F32).astype(I32)
    cnt = rank[:, :, -1]
    hotm = cnt >= t // 2
    scnt = jnp.where(hotm, 0, cnt)
    pcs = (scnt + PIECE - 1) // PIECE
    pend = jnp.cumsum(pcs, axis=1)
    base = (pend - pcs) * PIECE
    pos = jnp.where(hit & ~hotm[..., None], base[..., None] + rank - 1, -1)
    rows = t * k + nl * PIECE
    npb = -(-rows // CHUNK) * CHUNK // PIECE
    nch = jnp.maximum(-(-pend[:, -1] * PIECE // CHUNK), 1)
    below = lambda ends, q: jnp.sum((ends <= q).astype(I32), axis=-1)
    eg = jnp.minimum(below(pend[:, None, :], jnp.arange(npb, dtype=I32)[None, :, None]), nl - 1)
    flat = pcs.T.reshape(-1)
    fend = jnp.cumsum(flat)
    p = jnp.arange(nb * npb, dtype=I32)[:, None]
    seg = jnp.minimum(below(fend[None, :], p), nl * nb - 1)
    inseg = seg[:, None] == jnp.arange(nl * nb, dtype=I32)
    shift_ = jnp.tile(jnp.arange(nb, dtype=I32) * npb, nl) + (pend - pcs).T.reshape(-1) - (fend - flat)
    pc = jnp.clip(p[:, 0] + jnp.sum(jnp.where(inseg, shift_, 0), axis=1), 0, nb * npb - 1)
    ppt = MT // PIECE
    ptot = jnp.sum(pcs, axis=0)
    pstart = jnp.cumsum(ptot) - ptot
    tiles = (ptot + ppt - 1) // ppt
    tend = jnp.cumsum(tiles)
    nq = -(-(nb * npb) // ppt) + nl
    q = jnp.arange(nq, dtype=I32)
    tl = jnp.minimum(below(tend[None, :], q[:, None]), nl - 1)
    one = tl[:, None] == le
    pick = lambda v: jnp.sum(jnp.where(one, v[None, :], 0), axis=1)
    ti = q - pick(tend - tiles)
    tp = pick(pstart) + ti * ppt
    tn = jnp.clip(pick(ptot) - ti * ppt, 0, ppt)
    active = (tiles > 0).astype(I32)
    tw = pick(jnp.cumsum(active) - active)
    tf = (ti == 0).astype(I32)
    later = (le[None, :] > tl[:, None]) & (active[None, :] > 0)
    nxt = jnp.min(jnp.where(later, le[None, :], nl), axis=1)
    nxt = jnp.where(nxt < nl, nxt, -1)
    plan = tuple(v.astype(I32) for v in (tend[-1:], tl, tp, tn, tw, tf, nxt, pc))
    hend = jnp.cumsum(hotm.astype(I32), axis=1)
    hl = jnp.minimum(below(hend[:, None, :], le[None, :, None]), nl - 1)
    return Routing(hend[:, -1], hl, nch, eg, pos, None), plan


ON = (True,)


def solution(mesh):
    nd = mesh.shape['ep']
    nx = nd // 2
    tok_spec = P(('replica', 'ep'), None, None)
    rows_ep = P('ep', None)
    by_expert = P('ep', None, None)

    def shift(v, s):
        return lax.ppermute(v, 'ep', [(2 * i + c, 2 * ((i + s) % nx) + c) for i in range(nx) for c in range(2)])

    def partner(v):
        return lax.ppermute(v, 'ep', [(i, i ^ 1) for i in range(nd)])

    def local(x, wq, wk, wv, wo, wr, w1, w3, w2, idx):
        b, s, d = x.shape
        t, k, ne = b * s, idx.shape[-1], w1.shape[0]
        nl = 2 * ne
        half = t // 2
        me = lax.axis_index('ep')
        x = x.reshape(t, d)
        ids = idx.reshape(t, k)

        hd = HEAD // 2
        ang = (np.arange(t) % s).astype(np.float32)[:, None] * np.float32(THETA) ** (-np.arange(hd, dtype=np.float32) / hd)
        c, sn = np.cos(ang), np.sin(ang)
        cos, sin = [jnp.asarray(np.concatenate(v, axis=1), F32) for v in ((c, c), (-sn, sn))]
        h, ut, ub, o1, o3, logits, ids4 = attention_layer(nx, x, wv, wk, wq, wo, cos, sin, w1, w3, wr, ids.T)
        ids4 = jnp.swapaxes(ids4, 1, 2)
        ids4, w2, ut, ub = lax.optimization_barrier((ids4, w2, ut, ub))
        o2 = partner(w2)
        own, other = (w1, w3, w2), (o1, o3, o2)

        halves = lambda v: v.reshape(2 * v.shape[0], half, *v.shape[2:])
        is_local = halves(ids4 // nl == me // 2)
        lid = halves((ids4 - me * ne) % nl)
        r, plan = routing_plan(lid, is_local, nl)
        ohl = (lid[:, None] == jnp.arange(nl, dtype=I32)[:, None, None]) & is_local[:, None]

        u1t, u2b = shift(ut, 1), shift(ub, -1)
        oh = ids[..., None] == jnp.arange(wr.shape[1], dtype=I32)
        g = jax.nn.softmax(jnp.sum(jnp.where(oh, logits[:, None, :], 0.0), axis=-1), axis=-1)
        ut2, ub2, g = lax.optimization_barrier((ut, ub, g))
        g4 = [g, shift(g, 1), shift(g, -1), shift(g, 2)]
        u1b, u2t = shift(ub2, 1), shift(ut2, -1)
        spread = lambda o, v: jnp.sum(jnp.where(o, halves(v)[:, None], 0.0), axis=3)
        r = r._replace(gt=spread(ohl, jnp.stack(g4)))

        u3t, u3b = shift(u1t, 1), shift(u2b, -1)
        a0, d2, d5 = block((0, 2, 5), r, None, (ut, u1t, u2b), 3 * (None,), own, other, F32, 3 * ON, comb=False)
        u1b, d2 = lax.optimization_barrier((u1b, d2))
        x = gather(r, (ut, ub, u1t, u1b, u2t, u2b, u3t, u3b))
        z = cold(plan, x, own, other)

        tie = lambda r, *v: (lambda w: (r._replace(nch=w[0]), *w[1:]))(lax.optimization_barrier((r.nch, *v)))
        b2, b5 = block((2, 5), r, z, (), (d2, d5), own, other, BF, (False, False))
        r, b2, b5 = tie(r, b2, b5)
        b2, b5 = shift(b2, -1), shift(b5, 1)
        b6, = block((6,), r, z, (u3t,), (None,), own, other, BF, ON)
        r, b6 = tie(r, b6)
        c6 = shift(b6, 1)
        b7, = block((7,), r, z, (u3b,), (None,), own, other, BF, ON)
        r, b7 = tie(r, b7)
        c7 = shift(b7, -1)
        b3, = block((3,), r, z, (u1b,), (None,), own, other, BF, ON)
        r, b3, c6 = tie(r, b3, c6)
        b3, b6 = shift(b3, -1), shift(c6, 1)
        b4, = block((4,), r, z, (u2t,), (None,), own, other, BF, ON)
        r, b4, c7 = tie(r, b4, c7)
        b4, b7 = shift(b4, 1), shift(c7, -1)
        accs = block((0, 1), r, z, (ut, ub), (a0, None), own, other, F32, (False, True))
        y = final(h, accs, [(b2, b3), (b4, b5), (b6, b7)])
        return y.reshape(b, s, d)

    return jax.shard_map(local, mesh=mesh,
                         in_specs=(tok_spec, rows_ep, rows_ep, rows_ep, rows_ep, P(None, None),
                                   by_expert, by_expert, by_expert, tok_spec),
                         out_specs=tok_spec, check_vma=False)
```

```python
import functools
import math
import typing
import jax
import jax.numpy as jnp
import numpy as np
from jax import lax
from jax.experimental import pallas as pl
from jax.experimental.pallas import tpu as pltpu
from jax.sharding import PartitionSpec as P

HEAD = 128
EPS = 1e-6
THETA = 10000.0
PIECE = 8
CHUNK = 256
MT = 352
HM = 256
VMEM = 66_000_000
BF, F32, I32 = jnp.bfloat16, jnp.float32, jnp.int32


def rmsnorm(v):
    v = v.astype(F32)
    return v * lax.rsqrt(jnp.mean(v * v, axis=-1, keepdims=True) + EPS)


def dot(a, b):
    return jnp.dot(a, b, preferred_element_type=F32)


NT = (((1,), (1,)), ((), ()))
TN = (((0,), (0,)), ((), ()))
DMA2 = pltpu.SemaphoreType.DMA((2,))


def cost(flops, bytes_):
    return pl.CostEstimate(flops=flops, bytes_accessed=bytes_, transcendentals=0)


def parity(i):
    return lax.rem(i, 2)


def expert_buffers(d, ff):
    return [pltpu.VMEM((2, *v), BF) for v in ((d, ff), (d, ff), (ff, d))]


def loop(n):
    return pl.loop(0, n)


def params(**kw):
    return pltpu.CompilerParams(vmem_limit_bytes=VMEM, **kw)


def split3(g):
    hi = g.astype(BF)
    r = g - hi.astype(F32)
    mid = r.astype(BF)
    lo = (r - mid.astype(F32)).astype(BF)
    return hi, mid, lo


LT, LB, RT, RB, OT, OB, PO, PASS = range(8)
SWAPS = "41111111210032329"
MESH = pl.DeviceIdType.MESH


def layer_kernel(nx, x_ref, wv_ref, wk_ref, wq_ref, wo_ref, cos_ref, sin_ref, w1_ref, w3_ref, w2_ref, wr_ref, id_ref,
                 h_ref, ut_ref, ub_ref, o1_ref, o3_ref, o2_ref, lg_ref, id4_ref,
                 w_ref, ab, qb, kb, vb, rb3, ssem, rsem, lsem, iosem, swap_send, swap_recv, id_send, id_recv):
    shards = (wv_ref, wk_ref, wq_ref, wo_ref)
    sh = wv_ref.shape[0]
    hs = sh // 2
    t, d = ab.shape
    me = lax.axis_index("ep")
    chip, core = me // 2, me % 2
    right, left, opp = [2 * ((chip + k) % nx) + core for k in (1, nx - 1, 2)]
    partner = 2 * chip + 1 - core

    barrier = pltpu.get_barrier_semaphore()
    around = (right, left, opp)
    for dev in (*around, partner):
        pl.semaphore_signal(barrier, inc=1, device_id={"ep": dev}, device_id_type=MESH)
    pl.semaphore_wait(barrier, 4)

    def rows(e, half=None):
        if half is None:
            return pl.ds(pl.multiple_of(e * sh, sh), sh)
        return pl.ds(pl.multiple_of(e * sh + half * hs, hs), hs)

    def remote(w, src, dst, dev, s, r):
        return pltpu.make_async_remote_copy(src_ref=src, dst_ref=w_ref.at[w, dst, :], send_sem=ssem.at[w, s],
                                            recv_sem=rsem.at[w, r], device_id={"ep": dev}, device_id_type=MESH)

    def own(w):
        src = shards[w]
        top, bot = src.at[pl.ds(0, hs), :], src.at[pl.ds(hs, hs), :]
        return [remote(w, top, rows(me, 0), right, 0, LT), remote(w, bot, rows(me, 1), left, 1, RB),
                remote(w, bot, rows(me, 1), right, 2, LB), remote(w, top, rows(me, 0), left, 3, RT),
                remote(w, src, rows(me), partner, 6, PO)]

    def mine(w):
        return pltpu.make_async_copy(shards[w], w_ref.at[w, rows(me), :], lsem.at[w])

    where = {LT: (left, 0), LB: (left, 1), RT: (right, 0), RB: (right, 1), OT: (opp, 0), OB: (opp, 1)}

    def onward(w, k):
        e, half = where[LT if k == OT else RB]
        return remote(w, w_ref.at[w, rows(e, half), :], rows(e, half), right if k == OT else left, 4 if k == OT else 5, k)

    def across(w, k):
        r = rows(*where[k])
        return remote(w, w_ref.at[w, r, :], r, partner, PASS + k, PASS + k)

    def arrive(w, k):
        r = rows(me) if k == PO else rows(*where[k % PASS])
        remote(w, w_ref.at[w, r, :], r, partner, 0, k).wait_recv()

    def begin(w):
        for c in own(w):
            c.start()
        mine(w).start()

    def stage_a(w):
        arrive(w, LT)
        onward(w, OT).start()
        arrive(w, RB)
        onward(w, OB).start()
        if w + 1 < 4:
            begin(w + 1)
        across(w, LT).start()
        across(w, RB).start()
        swap()

    def stage_b(w):
        for k in (LB, RT):
            arrive(w, k)
            across(w, k).start()
        swap()

    def stage_c(w):
        for k in (OT, OB):
            arrive(w, k)
            across(w, k).start()
        swap()

    def stage_d(w):
        for k in (PO, PASS + LT, PASS + RB, PASS + LB, PASS + RT, PASS + OT, PASS + OB):
            arrive(w, k)
        mine(w).wait()

    pieces = [(src.at[e], dst.at[e]) for e in range(w1_ref.shape[0]) for src, dst in ((w1_ref, o1_ref), (w3_ref, o3_ref), (w2_ref, o2_ref))]
    swaps = [pltpu.make_async_remote_copy(src_ref=src, dst_ref=dst, send_sem=swap_send.at[i], recv_sem=swap_recv.at[i],
                                          device_id={"ep": partner}, device_id_type=MESH) for i, (src, dst) in enumerate(pieces)]
    waiting, quota = list(swaps), iter(SWAPS)

    def swap():
        for _ in range(min(int(next(quota)), len(waiting))):
            waiting.pop(0).start()

    ids = [pltpu.make_async_remote_copy(src_ref=id_ref, dst_ref=id4_ref.at[k + 1], send_sem=id_send.at[k], recv_sem=id_recv.at[k],
                                        device_id={"ep": dev}, device_id_type=MESH) for k, dev in enumerate(around)]
    ids.append(pltpu.make_async_copy(id_ref, id4_ref.at[0], id_send.at[3]))
    begin(0)
    for c in ids:
        c.start()
    swap()
    xin = pltpu.make_async_copy(x_ref, kb, iosem.at[0])
    xin.start()
    xin.wait()
    rb = min(256, t)
    rb3[:] = jnp.concatenate(split3(wr_ref[:]), axis=0)

    @loop(t // rb)
    def _(i):
        r = pl.ds(pl.multiple_of(i * rb, rb), rb)
        ab[r, :] = rmsnorm(kb[r, :]).astype(BF)

    tm, tn = min(512, t), min(512, d)

    def project(w, dst, rope):
        @loop(d // tn)
        def _(n):
            @loop(t // tm)
            def _(m):
                r = pl.ds(pl.multiple_of(m * tm, tm), tm)
                z = dot(ab[r, :], w_ref[w, :, pl.ds(pl.multiple_of(n * tn, tn), tn)])
                for j in range(tn // HEAD):
                    zj = z[:, j * HEAD:(j + 1) * HEAD]
                    if rope:
                        zj = zj * cos_ref[r, :] + pltpu.roll(zj, HEAD // 2, 1) * sin_ref[r, :]
                    dst[r, pl.ds(pl.multiple_of(n * tn + j * HEAD, HEAD), HEAD)] = zj.astype(BF)

    for w, (dst, rope) in enumerate(((vb, False), (kb, True), (qb, True))):
        stage_a(w)
        stage_b(w)
        stage_c(w)
        stage_d(w)
        swap()
        project(w, dst, rope)
    stage_a(3)

    tq = min(256, t)
    scale = math.log2(math.e) / math.sqrt(HEAD)
    causal = lax.broadcasted_iota(I32, (tq, tq), 0) <= lax.broadcasted_iota(I32, (tq, tq), 1)
    group = min(4, d // HEAD)
    steps = d // HEAD // group
    marks = {1: stage_b, steps - 1: stage_c}
    if len(marks) > steps - 1:
        marks = {}
        stage_b(3)
        stage_c(3)

    @loop(steps)
    def _(jj):
        for at, stage in marks.items():
            pl.when(jj == at)(functools.partial(stage, 3))
        for j in range(group):
            c = pl.ds(pl.multiple_of((jj * group + j) * HEAD, HEAD), HEAD)
            for i in range(t // tq):
                r, n = slice(i * tq, (i + 1) * tq), (i + 1) * tq
                sc = lax.dot_general(kb[:n, c], qb[r, c], NT, preferred_element_type=F32)
                diag = jnp.where(causal, sc[i * tq:], -jnp.inf)
                sc = jnp.concatenate([sc[:i * tq], diag], axis=0) if i else diag
                p = jnp.exp2((sc - jnp.max(sc, axis=0, keepdims=True)) * scale)
                p = (p * (1.0 / jnp.sum(p, axis=0, keepdims=True))).astype(BF)
                qb[r, c] = lax.dot_general(p, vb[:n, c], TN, preferred_element_type=F32).astype(BF)

    swap()
    xin = pltpu.make_async_copy(x_ref, vb, iosem.at[0])
    xin.start()
    stage_d(3)
    xin.wait()

    @loop(d // tn)
    def _(n):
        c = pl.ds(pl.multiple_of(n * tn, tn), tn)

        @loop(t // tm)
        def _(m):
            r = pl.ds(pl.multiple_of(m * tm, tm), tm)
            ab[r, c] = (vb[r, c].astype(F32) + dot(qb[r, :], w_ref[3, :, c])).astype(BF)

    hout = pltpu.make_async_copy(ab, h_ref, iosem.at[0])
    hout.start()

    @loop(t // rb)
    def _(i):
        r = pl.ds(pl.multiple_of(i * rb, rb), rb)
        hi, mid, lo = split3(rmsnorm(ab[r, :]))
        kb[r, :] = hi
        ne = wr_ref.shape[0]
        part = lambda v, k: v[:, k * ne:(k + 1) * ne]
        p1, p2, p3 = [lax.dot_general(v, rb3[:n * ne], NT, preferred_element_type=F32) for v, n in ((hi, 3), (mid, 2), (lo, 1))]
        lg_ref[r, :] = part(p1, 0) + ((part(p1, 1) + part(p2, 0)) + (part(p1, 2) + part(p2, 1) + part(p3, 0)))

    uout = [pltpu.make_async_copy(kb.at[pl.ds(p * t // 2, t // 2), :], o, iosem.at[1 + p]) for p, o in enumerate((ut_ref, ub_ref))]
    for c in uout:
        c.start()
    assert not waiting
    for c in swaps + ids:
        c.wait()
    for w in range(4):
        for c in own(w) + [onward(w, OT), onward(w, OB)] + [across(w, k) for k in where]:
            c.wait_send()
    hout.wait()
    for c in uout:
        c.wait()


def attention_layer(nx, x, wv, wk, wq, wo, cos, sin, w1, w3, w2, wr, ids):
    t, d = x.shape
    hb = pl.BlockSpec(memory_space=pl.ANY)
    vm = pl.BlockSpec(memory_space=pltpu.VMEM)
    half = jax.ShapeDtypeStruct((t // 2, d), BF)
    act = pltpu.VMEM((t, d), BF)
    return pl.pallas_call(
        functools.partial(layer_kernel, nx),
        in_specs=[hb] * 5 + [vm] * 2 + [hb] * 3 + [vm, hb],
        out_specs=[hb] * 6 + [vm, hb],
        out_shape=[jax.ShapeDtypeStruct((t, d), BF), half, half, jax.ShapeDtypeStruct(w1.shape, BF),
                   *[jax.ShapeDtypeStruct(v.shape, BF) for v in (w3, w2)], jax.ShapeDtypeStruct((t, wr.shape[0]), F32),
                   jax.ShapeDtypeStruct((nx, *ids.shape), I32)],
        scratch_shapes=[pltpu.VMEM((4, d, d), BF), act, act, act, act, pltpu.VMEM((3 * wr.shape[0], d), BF),
                        pltpu.SemaphoreType.DMA((4, 13)), pltpu.SemaphoreType.DMA((4, 13)),
                        pltpu.SemaphoreType.DMA((4,)), pltpu.SemaphoreType.DMA((3,)),
                        pltpu.SemaphoreType.DMA((3 * w1.shape[0],)), pltpu.SemaphoreType.DMA((3 * w1.shape[0],)),
                        pltpu.SemaphoreType.DMA((nx,)), pltpu.SemaphoreType.DMA((nx,))],
        compiler_params=params(collective_id=0, has_side_effects=True),
        cost_estimate=cost(8 * t * d * d, 24 * t * d),
    )(x, wv, wk, wq, wo, cos, sin, w1, w3, w2, wr, ids)


def fetch_expert(l, slot, own, other, bufs, sem):
    ne = own[0].shape[0]

    @pl.when(l < ne)
    def _():
        for src, dst in zip(own, bufs):
            pltpu.make_async_copy(src.at[l], dst.at[slot], sem.at[slot]).start()

    @pl.when(l >= ne)
    def _():
        for src, dst in zip(other, bufs):
            pltpu.make_async_copy(src.at[l - ne], dst.at[slot], sem.at[slot]).start()


def wait_expert(slot, own, bufs, sem):
    for src, dst in zip(own, bufs):
        pltpu.make_async_copy(src.at[0], dst.at[slot], sem.at[slot]).wait()


def ffn(x, w1, w3, w2):
    a1 = dot(x, w1)
    a3 = dot(x, w3)
    act = (jax.nn.silu(a1) * a3).astype(BF)
    return dot(act, w2).astype(BF)


def block_kernel(js, has_acc, comb, dense, *refs):
    refs = list(refs)
    nblk = len(js)
    take = lambda n: [refs.pop(0) for _ in range(n)]
    if any(dense):
        nh_ref, hl_ref = take(2)
    gt_ref, = take(1)
    if comb:
        nch_ref, eg_ref, pos_ref, z_ref = take(4)
        cap = z_ref.shape[0] // pos_ref.shape[0]
    if any(dense):
        us = take(nblk)
        own, other = take(3), take(3)
        nl = 2 * own[0].shape[0]
    accs = [take(1)[0] if h else None for h in has_acc]
    outs = take(nblk)
    acc, asem = take(2)
    if comb:
        cbuf, zbuf, zsem = take(3)
    if any(dense):
        bufs, (ubuf, sem, usem) = take(3), take(3)
    t, d = outs[0].shape

    if any(dense):
        ns = [nh_ref[j] if on else 0 for j, on in zip(js, dense)]
        n = sum(ns)

        def entry(i):
            p, j, k, end = 0, js[0], i, 0
            for q in range(nblk - 1):
                end = end + ns[q]
                past = i >= end
                p, j, k = jnp.where(past, q + 1, p), jnp.where(past, js[q + 1], j), jnp.where(past, i - end, k)
            return p, j, hl_ref[j * nl + k]

        @pl.when(n > 0)
        def _():
            fetch_expert(entry(0)[-1], 0, own, other, bufs, sem)

        ucp = [pltpu.make_async_copy(us[p], ubuf.at[pl.ds(p * t, t), :], usem) for p in range(nblk)]
        for cp in ucp:
            cp.start()
    for p in range(nblk):
        rows = pl.ds(p * t, t)
        if has_acc[p]:
            pltpu.make_async_copy(accs[p], acc.at[rows, :], asem.at[p]).start()
        else:
            acc[rows, :] = jnp.zeros((t, d), F32)
    for p in range(nblk):
        if has_acc[p]:
            pltpu.make_async_copy(accs[p], acc.at[pl.ds(p * t, t), :], asem.at[p]).wait()

    if comb:
        for p, j in enumerate(js):
            nch = nch_ref[j]

            def get(i, slot):
                src = pl.multiple_of(j * cap + i * CHUNK, CHUNK)
                return pltpu.make_async_copy(z_ref.at[pl.ds(src, CHUNK), :], zbuf.at[slot], zsem.at[slot])

            get(0, 0).start()
            nl = gt_ref.shape[1]
            lane = lax.broadcasted_iota(I32, (1, CHUNK), 1)
            ti = lax.broadcasted_iota(I32, (16, t), 1)
            si = lax.broadcasted_iota(I32, (16, t), 0)
            tparts = jnp.where(si == 0, ti % 256, jnp.where(si == 1, ti // 256, 0)).astype(F32).astype(BF)
            table = jnp.concatenate([*split3(gt_ref[j]), tparts], axis=0)

            @loop(nch)
            def _(i):
                slot = parity(i)

                @pl.when(i + 1 < nch)
                def _():
                    get(i + 1, 1 - slot).start()

                pm, ls = selection(j, i, eg_ref, pos_ref)
                el = jnp.zeros_like(lane)
                for q, l in enumerate(ls):
                    el = jnp.where(lane // PIECE == q, l, el)
                sel = lax.dot_general(table, pm, NT, preferred_element_type=F32)
                tok = (sel[3 * nl:3 * nl + 1] + 256.0 * sel[3 * nl + 1:3 * nl + 2]).astype(I32)
                hot_ = lax.broadcasted_iota(I32, (t, CHUNK), 0) == tok
                sub = lax.broadcasted_iota(I32, (nl, CHUNK), 0) == el
                for k in range(3):
                    gk = jnp.sum(jnp.where(sub, sel[k * nl:(k + 1) * nl], 0.0), axis=0, keepdims=True)
                    cbuf[:, k * CHUNK:(k + 1) * CHUNK] = jnp.where(hot_, gk, 0.0).astype(BF)
                get(i, slot).wait()
                tn = min(1024, d)

                @loop(d // tn)
                def _(m):
                    cs = pl.ds(pl.multiple_of(m * tn, tn), tn)
                    z = zbuf[slot, :, cs]
                    acc[p * t:(p + 1) * t, cs] += dot(cbuf[:], jnp.concatenate([z, z, z], axis=0))

    if any(dense):
        for cp in ucp:
            cp.wait()
        tm = min(HM, t)

        @loop(n)
        def _(i):
            slot = parity(i)
            wait_expert(slot, own, bufs, sem)

            @pl.when(i + 1 < n)
            def _():
                fetch_expert(entry(i + 1)[-1], 1 - slot, own, other, bufs, sem)

            p, blk, e = entry(i)

            @loop(t // tm)
            def _(m):
                rows = pl.ds(pl.multiple_of(p * t + m * tm, tm), tm)
                z = ffn(ubuf[rows, :], bufs[0][slot], bufs[1][slot], bufs[2][slot])
                g = gt_ref[blk, pl.ds(e, 1), pl.ds(pl.multiple_of(m * tm, tm), tm)]
                eye = lax.broadcasted_iota(I32, (tm, tm), 0) == lax.broadcasted_iota(I32, (tm, tm), 1)
                gc = jnp.sum(jnp.where(eye, g, 0.0), axis=1, keepdims=True)
                acc[rows, :] += gc * z.astype(F32)

    if outs[0].dtype == F32:
        done = [pltpu.make_async_copy(acc.at[pl.ds(p * t, t), :], outs[p], asem.at[p]) for p in range(nblk)]
        for cp in done:
            cp.start()
        for cp in done:
            cp.wait()
    else:
        for p in range(nblk):
            outs[p][:] = acc[p * t:(p + 1) * t, :].astype(BF)


def block(js, r, z, us, accs, own, other, dtype, dense, comb=True):
    nblk = len(js)
    t = r.pos.shape[2]
    d = own[0].shape[1]
    ff = own[0].shape[2]
    vm = pl.BlockSpec(memory_space=pltpu.VMEM)
    sm = pl.BlockSpec(memory_space=pltpu.SMEM)
    hb = pl.BlockSpec(memory_space=pl.ANY)
    args, specs, scratch = [], [], []
    if any(dense):
        args += [r.nh, r.hl.reshape(-1)]
        specs += [sm, sm]
    args += [r.gt]
    specs += [vm]
    if comb:
        args += [r.nch, r.eg.reshape(-1), r.pos, z]
        specs += [sm, sm, vm, hb]
    if any(dense):
        args += list(us) + list(own) + list(other)
        specs += [hb] * (nblk + 6)
    args += [v for v in accs if v is not None]
    specs += [hb for v in accs if v is not None]
    scratch += [pltpu.VMEM((nblk * t, d), F32), pltpu.SemaphoreType.DMA((nblk,))]
    if comb:
        scratch += [pltpu.VMEM((t, 3 * CHUNK), BF), pltpu.VMEM((2, CHUNK, d), BF), DMA2]
    if any(dense):
        scratch += [*expert_buffers(d, ff),
                    pltpu.VMEM((nblk * t, d), BF), DMA2, pltpu.SemaphoreType.DMA]
    out = jax.ShapeDtypeStruct((t, d), dtype)
    return pl.pallas_call(
        functools.partial(block_kernel, js, [v is not None for v in accs], comb, dense),
        in_specs=specs, out_specs=[hb if dtype == F32 else vm] * nblk, out_shape=[out] * nblk, scratch_shapes=scratch,
        compiler_params=params(),
        cost_estimate=cost(t * d, 6 * d * ff),
    )(*args)


def selection(j, i, eg_ref, pos_ref):
    t = pos_ref.shape[2]
    it = lax.broadcasted_iota(I32, (2 * PIECE, t), 0)
    npc = CHUNK // PIECE
    first = (j * (eg_ref.shape[0] // pos_ref.shape[0] // npc) + i) * npc
    ls = [eg_ref[first + q] for q in range(npc)]
    hits = []
    for q in range(0, npc, 2):
        own, nxt = [pos_ref[j, pl.ds(l, 1), :] for l in ls[q:q + 2]]
        hit = jnp.where(it < PIECE, own, nxt) - (i * CHUNK + q * PIECE) == it
        hits.append(jnp.where(hit, 1.0, 0.0).astype(BF))
    return jnp.concatenate(hits, axis=0), ls


def gather_kernel(js, nch_ref, eg_ref, pos_ref, *refs):
    us, (x_ref, ubuf, xbuf, usem, sem) = refs[:len(js)], refs[-5:]
    cap = x_ref.shape[0] // pos_ref.shape[0]
    cps = [pltpu.make_async_copy(u, ubuf.at[p % 2], usem.at[p % 2]) for p, u in enumerate(us)]
    cps[0].start()

    def out(slot, row):
        return pltpu.make_async_copy(xbuf.at[slot], x_ref.at[pl.ds(pl.multiple_of(row, CHUNK), CHUNK), :], sem.at[slot])

    made = 0
    for p, j in enumerate(js):
        if p + 1 < len(js):
            cps[p + 1].start()
        cps[p].wait()

        @loop(nch_ref[j])
        def _(i):
            slot = parity(made + i)

            @pl.when(made + i >= 2)
            def _():
                out(slot, 0).wait()

            xbuf[slot] = dot(selection(j, i, eg_ref, pos_ref)[0], ubuf[p % 2]).astype(BF)
            out(slot, j * cap + i * CHUNK).start()

        made = made + nch_ref[j]
    for k in (2, 1):
        @pl.when(made >= k)
        def _():
            out(parity(made - k), 0).wait()


def gather(js, r, us, x):
    t, d = us[0].shape
    rows = r.eg.size * PIECE
    vm = pl.BlockSpec(memory_space=pltpu.VMEM)
    sm = pl.BlockSpec(memory_space=pltpu.SMEM)
    hb = pl.BlockSpec(memory_space=pl.ANY)
    more = [] if x is None else [x]
    return pl.pallas_call(
        functools.partial(gather_kernel, js),
        in_specs=[sm, sm, vm] + [hb] * len(us + more),
        out_specs=hb,
        out_shape=jax.ShapeDtypeStruct((rows, d), BF),
        input_output_aliases={3 + len(us): 0} if more else {},
        scratch_shapes=[pltpu.VMEM((2, t, d), BF), pltpu.VMEM((2, CHUNK, d), BF), DMA2, DMA2],
        compiler_params=params(),
        cost_estimate=cost(t * d, 4 * CHUNK * d),
    )(r.nch, r.eg.reshape(-1), r.pos, *us, *more)


def cold_kernel(nt_ref, tl_ref, tp_ref, tn_ref, tw_ref, tf_ref, nx_ref, pc_ref, x_ref, *refs):
    own, other, z_ref, refs = refs[:3], refs[3:6], refs[6], refs[7:]
    bufs, (xbuf, zbuf, wsem, xsem, zsem) = refs[:3], refs[3:]
    nt = nt_ref[0]

    def each(n, fn):
        @loop(lax.div(n, 2))
        def _(i):
            fn(2 * i)
            fn(2 * i + 1)

        @pl.when(parity(n) == 1)
        def _():
            fn(n - 1)

    def xin(q, slot):
        p0 = tp_ref[q]

        def one(i):
            src = pl.ds(pl.multiple_of(pc_ref[p0 + i] * PIECE, PIECE), PIECE)
            dst = pl.ds(pl.multiple_of(i * PIECE, PIECE), PIECE)
            pltpu.make_async_copy(x_ref.at[src, :], xbuf.at[slot, dst, :], xsem.at[slot]).start()

        each(tn_ref[q], one)

    def zout(q, slot):
        p0 = tp_ref[q]

        def one(i):
            src = pl.ds(pl.multiple_of(i * PIECE, PIECE), PIECE)
            dst = pl.ds(pl.multiple_of(pc_ref[p0 + i] * PIECE, PIECE), PIECE)
            pltpu.make_async_copy(zbuf.at[slot, src, :], z_ref.at[dst, :], zsem.at[slot]).start()

        each(tn_ref[q], one)

    def drain(n, fn):
        bit = 1
        while bit <= MT // PIECE:
            @pl.when(lax.rem(lax.div(n, bit), 2) == 1)
            def _(bit=bit):
                fn(pl.ds(0, bit * PIECE))

            bit *= 2

    def xwait(q, slot):
        drain(tn_ref[q], lambda r: pltpu.make_async_copy(x_ref.at[r, :], xbuf.at[slot, r, :], xsem.at[slot]).wait())

    def zwait(q, slot):
        drain(tn_ref[q], lambda r: pltpu.make_async_copy(zbuf.at[slot, r, :], z_ref.at[r, :], zsem.at[slot]).wait())

    @pl.when(nt > 0)
    def _():
        fetch_expert(tl_ref[0], 0, own, other, bufs, wsem)
        xin(0, 0)

    @loop(nt)
    def _(q):
        slot = parity(q)
        ws = parity(tw_ref[q])

        @pl.when(tf_ref[q] == 1)
        def _():
            wait_expert(ws, own, bufs, wsem)

            @pl.when(nx_ref[q] >= 0)
            def _():
                fetch_expert(nx_ref[q], 1 - ws, own, other, bufs, wsem)

        @pl.when(q + 1 < nt)
        def _():
            xin(q + 1, 1 - slot)

        xwait(q, slot)

        @pl.when(q >= 2)
        def _():
            zwait(q - 2, slot)

        zbuf[slot] = ffn(xbuf[slot], bufs[0][ws], bufs[1][ws], bufs[2][ws])
        zout(q, slot)

    for k in (2, 1):
        @pl.when(nt >= k)
        def _():
            zwait(nt - k, parity(nt - k))


def cold(plan, x, own, other):
    d, ff = own[0].shape[1:]
    sm = pl.BlockSpec(memory_space=pltpu.SMEM)
    hb = pl.BlockSpec(memory_space=pl.ANY)
    return pl.pallas_call(
        cold_kernel,
        in_specs=[sm] * len(plan) + [hb] * 7,
        out_specs=hb,
        out_shape=jax.ShapeDtypeStruct(x.shape, BF),
        scratch_shapes=[*expert_buffers(d, ff),
                        pltpu.VMEM((2, MT, d), BF), pltpu.VMEM((2, MT, d), BF),
                        DMA2, DMA2, DMA2],
        input_output_aliases={len(plan): 0},
        compiler_params=params(),
        cost_estimate=cost(6 * 16 * MT * d * ff, 96 * d * ff),
    )(*plan, x, *own, *other)


def final_kernel(h_ref, *refs):
    y_ref = refs[-1]
    acc, parts = refs[0], refs[1:-1]
    y = h_ref[:].astype(F32) + acc[:]
    for v in parts:
        y = y + v[:].astype(F32)
    y_ref[:] = y.astype(BF)


def final(h, accs, parts):
    t, d = h.shape
    half = t // 2
    tm = min(256, half)
    n = half // tm

    def body(h_ref, *refs):
        for p in range(2):
            @pl.when(pl.program_id(0) // n == p)
            def _():
                final_kernel(h_ref, refs[p], *refs[2 + p:-1:2], refs[-1])

    spec = lambda p: pl.BlockSpec((tm, d), lambda i: (jnp.minimum(i, n - 1) if p == 0 else jnp.maximum(i - n, 0), 0))
    return pl.pallas_call(
        body, grid=(2 * n,),
        in_specs=[pl.BlockSpec((tm, d), lambda i: (i, 0))] + [spec(0), spec(1)] * (1 + len(parts)),
        out_specs=pl.BlockSpec((tm, d), lambda i: (i, 0)),
        out_shape=jax.ShapeDtypeStruct((t, d), BF),
        compiler_params=params(),
        cost_estimate=cost(6 * t * d, 20 * t * d),
    )(h, *accs, *[v for part in parts for v in part])


class Routing(typing.NamedTuple):
    nh: typing.Any
    hl: typing.Any
    nch: typing.Any
    eg: typing.Any
    pos: typing.Any
    gt: typing.Any


def routing_plan(lid, local, nl):
    nb, t, k = lid.shape
    le = jnp.arange(nl, dtype=I32)
    hit = jnp.any((lid[:, None] == le[:, None, None]) & local[:, None], axis=-1)
    tri = (jnp.arange(t)[:, None] <= jnp.arange(t)[None, :]).astype(BF)
    rank = lax.dot_general(hit.astype(BF), tri, (((2,), (0,)), ((), ())), preferred_element_type=F32).astype(I32)
    cnt = rank[:, :, -1]
    hotm = cnt >= t // 2
    scnt = jnp.where(hotm, 0, cnt)
    pcs = (scnt + PIECE - 1) // PIECE
    pend = jnp.cumsum(pcs, axis=1)
    base = (pend - pcs) * PIECE
    pos = jnp.where(hit & ~hotm[..., None], base[..., None] + rank - 1, -1)
    rows = t * k + nl * PIECE
    npb = -(-rows // CHUNK) * CHUNK // PIECE
    nch = jnp.maximum(-(-pend[:, -1] * PIECE // CHUNK), 1)
    below = lambda ends, q: jnp.sum((ends <= q).astype(I32), axis=-1)
    eg = jnp.minimum(below(pend[:, None, :], jnp.arange(npb, dtype=I32)[None, :, None]), nl - 1)
    flat = pcs.T.reshape(-1)
    fend = jnp.cumsum(flat)
    p = jnp.arange(nb * npb, dtype=I32)[:, None]
    seg = jnp.minimum(below(fend[None, :], p), nl * nb - 1)
    inseg = seg[:, None] == jnp.arange(nl * nb, dtype=I32)
    shift_ = jnp.tile(jnp.arange(nb, dtype=I32) * npb, nl) + (pend - pcs).T.reshape(-1) - (fend - flat)
    pc = jnp.clip(p[:, 0] + jnp.sum(jnp.where(inseg, shift_, 0), axis=1), 0, nb * npb - 1)
    ppt = MT // PIECE
    ptot = jnp.sum(pcs, axis=0)
    pstart = jnp.cumsum(ptot) - ptot
    tiles = (ptot + ppt - 1) // ppt
    tend = jnp.cumsum(tiles)
    nq = -(-(nb * npb) // ppt) + nl
    q = jnp.arange(nq, dtype=I32)
    tl = jnp.minimum(below(tend[None, :], q[:, None]), nl - 1)
    one = tl[:, None] == le
    pick = lambda v: jnp.sum(jnp.where(one, v[None, :], 0), axis=1)
    ti = q - pick(tend - tiles)
    tp = pick(pstart) + ti * ppt
    tn = jnp.clip(pick(ptot) - ti * ppt, 0, ppt)
    active = (tiles > 0).astype(I32)
    tw = pick(jnp.cumsum(active) - active)
    tf = (ti == 0).astype(I32)
    later = (le[None, :] > tl[:, None]) & (active[None, :] > 0)
    nxt = jnp.min(jnp.where(later, le[None, :], nl), axis=1)
    nxt = jnp.where(nxt < nl, nxt, -1)
    plan = tuple(v.astype(I32) for v in (tend[-1:], tl, tp, tn, tw, tf, nxt, pc))
    hend = jnp.cumsum(hotm.astype(I32), axis=1)
    hl = jnp.minimum(below(hend[:, None, :], le[None, :, None]), nl - 1)
    return Routing(hend[:, -1], hl, nch, eg, pos, None), plan


ON = (True,)


def solution(mesh):
    nd = mesh.shape['ep']
    nx = nd // 2
    tok_spec = P(('replica', 'ep'), None, None)
    rows_ep = P('ep', None)
    by_expert = P('ep', None, None)

    def shift(v, s):
        return lax.ppermute(v, 'ep', [(2 * i + c, 2 * ((i + s) % nx) + c) for i in range(nx) for c in range(2)])

    def local(x, wq, wk, wv, wo, wr, w1, w3, w2, idx):
        b, s, d = x.shape
        t, k, ne = b * s, idx.shape[-1], w1.shape[0]
        nl = 2 * ne
        half = t // 2
        me = lax.axis_index('ep')
        x = x.reshape(t, d)
        ids = idx.reshape(t, k)

        hd = HEAD // 2
        ang = (np.arange(t) % s).astype(np.float32)[:, None] * np.float32(THETA) ** (-np.arange(hd, dtype=np.float32) / hd)
        c, sn = np.cos(ang), np.sin(ang)
        cos, sin = [jnp.asarray(np.concatenate(v, axis=1), F32) for v in ((c, c), (-sn, sn))]
        h, ut, ub, o1, o3, o2, logits, ids4 = attention_layer(nx, x, wv, wk, wq, wo, cos, sin, w1, w3, w2, wr.T, ids.T)
        ids4 = jnp.swapaxes(ids4, 1, 2)
        own, other = (w1, w3, w2), (o1, o3, o2)

        halves = lambda v: v.reshape(2 * v.shape[0], half, *v.shape[2:])
        is_local = halves(ids4 // nl == me // 2)
        lid = halves((ids4 - me * ne) % nl)
        r, plan = routing_plan(lid, is_local, nl)
        ohl = (lid[:, None] == jnp.arange(nl, dtype=I32)[:, None, None]) & is_local[:, None]

        u1t, u2b = shift(ut, 1), shift(ub, -1)
        oh = ids[..., None] == jnp.arange(wr.shape[1], dtype=I32)
        g = jax.nn.softmax(jnp.sum(jnp.where(oh, logits[:, None, :], 0.0), axis=-1), axis=-1)
        ut2, ub2, g = lax.optimization_barrier((ut, ub, g))
        g4 = [g, shift(g, 1), shift(g, -1), shift(g, 2)]
        u1b, u2t = shift(ub2, 1), shift(ut2, -1)
        spread = lambda o, v: jnp.sum(jnp.where(o, halves(v)[:, None], 0.0), axis=3)
        ra = r._replace(gt=spread(ohl[:2], g[None]))
        r = r._replace(gt=spread(ohl, jnp.stack(g4)))

        a0, = block((0,), ra, None, (ut,), (None,), own, other, F32, ON, comb=False)
        a0, u1t, u2b = lax.optimization_barrier((a0, u1t, u2b))
        u3t, u3b = shift(u1t, 1), shift(u2b, -1)
        d2, d5 = block((2, 5), r, None, (u1t, u2b), 2 * (None,), own, other, F32, 2 * ON, comb=False)
        u1b, d2 = lax.optimization_barrier((u1b, d2))
        x = gather(tuple(range(6)), r, [ut, ub, u1t, u1b, u2t, u2b], None)
        u3t, x = lax.optimization_barrier((u3t, x))
        x = gather((6, 7), r, [u3t, u3b], x)
        z = cold(plan, x, own, other)

        tie = lambda r, *v: (lambda w: (r._replace(nch=w[0]), *w[1:]))(lax.optimization_barrier((r.nch, *v)))
        b6, = block((6,), r, z, (u3t,), (None,), own, other, BF, ON)
        r, b6 = tie(r, b6)
        c6 = shift(b6, 1)
        b2, b5 = block((2, 5), r, z, (), (d2, d5), own, other, BF, (False, False))
        r, b2, b5 = tie(r, b2, b5)
        b2, b5 = shift(b2, -1), shift(b5, 1)
        b7, = block((7,), r, z, (u3b,), (None,), own, other, BF, ON)
        r, b7, c6 = tie(r, b7, c6)
        c7, b6 = shift(b7, -1), shift(c6, 1)
        b3, = block((3,), r, z, (u1b,), (None,), own, other, BF, ON)
        r, b3 = tie(r, b3)
        b3 = shift(b3, -1)
        b4, = block((4,), r, z, (u2t,), (None,), own, other, BF, ON)
        r, b4, c7 = tie(r, b4, c7)
        b4, b7 = shift(b4, 1), shift(c7, -1)
        accs = block((0, 1), r, z, (ut, ub), (a0, None), own, other, F32, (False, True))
        y = final(h, accs, [(b2, b3), (b4, b5), (b6, b7)])
        return y.reshape(b, s, d)

    return jax.shard_map(local, mesh=mesh,
                         in_specs=(tok_spec, rows_ep, rows_ep, rows_ep, rows_ep, P(None, None),
                                   by_expert, by_expert, by_expert, tok_spec),
                         out_specs=tok_spec, check_vma=False)
```

```python
import functools
import math
import typing
import jax
import jax.numpy as jnp
import numpy as np
from jax import lax
from jax.experimental import pallas as pl
from jax.experimental.pallas import tpu as pltpu
from jax.sharding import PartitionSpec as P

HEAD = 128
EPS = 1e-6
THETA = 10000.0
PIECE = 8
CHUNK = 256
MT = 352
HM = 512
VMEM = 66_000_000
BF, F32, I32 = jnp.bfloat16, jnp.float32, jnp.int32


def rmsnorm(v):
    v = v.astype(F32)
    return v * lax.rsqrt(jnp.mean(v * v, axis=-1, keepdims=True) + EPS)


def dot(a, b):
    return jnp.dot(a, b, preferred_element_type=F32)


NT = (((1,), (1,)), ((), ()))
TN = (((0,), (0,)), ((), ()))
DMA2 = pltpu.SemaphoreType.DMA((2,))


def cost(flops, bytes_):
    return pl.CostEstimate(flops=flops, bytes_accessed=bytes_, transcendentals=0)


def parity(i):
    return lax.rem(i, 2)


def expert_buffers(d, ff):
    return [pltpu.VMEM((2, *v), BF) for v in ((d, ff), (d, ff), (ff, d))]


def loop(n):
    return pl.loop(0, n)


def params(**kw):
    return pltpu.CompilerParams(vmem_limit_bytes=VMEM, **kw)


def split3(g):
    hi = g.astype(BF)
    r = g - hi.astype(F32)
    mid = r.astype(BF)
    lo = (r - mid.astype(F32)).astype(BF)
    return hi, mid, lo


LT, LB, RT, RB, OT, OB, PO, PASS = range(8)
LATE = 3
SWAPS = "41111111110022229"
MESH = pl.DeviceIdType.MESH


def layer_kernel(nx, x_ref, wv_ref, wk_ref, wq_ref, wo_ref, cos_ref, sin_ref, w1_ref, w3_ref, w2_ref, wr_ref, id_ref,
                 h_ref, ut_ref, ub_ref, o1_ref, o3_ref, o2_ref, late_ref, lg_ref, id4_ref,
                 w_ref, ab, qb, kb, vb, rb3, ssem, rsem, lsem, iosem, swap_send, swap_recv, id_send, id_recv):
    shards = (wv_ref, wk_ref, wq_ref, wo_ref)
    sh = wv_ref.shape[0]
    hs = sh // 2
    t, d = ab.shape
    me = lax.axis_index("ep")
    chip, core = me // 2, me % 2
    right, left, opp = [2 * ((chip + k) % nx) + core for k in (1, nx - 1, 2)]
    partner = 2 * chip + 1 - core

    barrier = pltpu.get_barrier_semaphore()
    around = (right, left, opp)
    for dev in (*around, partner):
        pl.semaphore_signal(barrier, inc=1, device_id={"ep": dev}, device_id_type=MESH)
    pl.semaphore_wait(barrier, 4)

    def rows(e, half=None):
        if half is None:
            return pl.ds(pl.multiple_of(e * sh, sh), sh)
        return pl.ds(pl.multiple_of(e * sh + half * hs, hs), hs)

    def remote(w, src, dst, dev, s, r):
        return pltpu.make_async_remote_copy(src_ref=src, dst_ref=w_ref.at[w, dst, :], send_sem=ssem.at[w, s],
                                            recv_sem=rsem.at[w, r], device_id={"ep": dev}, device_id_type=MESH)

    def own(w):
        src = shards[w]
        top, bot = src.at[pl.ds(0, hs), :], src.at[pl.ds(hs, hs), :]
        return [remote(w, top, rows(me, 0), right, 0, LT), remote(w, bot, rows(me, 1), left, 1, RB),
                remote(w, bot, rows(me, 1), right, 2, LB), remote(w, top, rows(me, 0), left, 3, RT),
                remote(w, src, rows(me), partner, 6, PO)]

    def mine(w):
        return pltpu.make_async_copy(shards[w], w_ref.at[w, rows(me), :], lsem.at[w])

    where = {LT: (left, 0), LB: (left, 1), RT: (right, 0), RB: (right, 1), OT: (opp, 0), OB: (opp, 1)}

    def onward(w, k):
        e, half = where[LT if k == OT else RB]
        return remote(w, w_ref.at[w, rows(e, half), :], rows(e, half), right if k == OT else left, 4 if k == OT else 5, k)

    def across(w, k):
        r = rows(*where[k])
        return remote(w, w_ref.at[w, r, :], r, partner, PASS + k, PASS + k)

    def arrive(w, k):
        r = rows(me) if k == PO else rows(*where[k % PASS])
        remote(w, w_ref.at[w, r, :], r, partner, 0, k).wait_recv()

    def begin(w):
        for c in own(w):
            c.start()
        mine(w).start()

    def stage_a(w):
        arrive(w, LT)
        onward(w, OT).start()
        arrive(w, RB)
        onward(w, OB).start()
        if w + 1 < 4:
            begin(w + 1)
        across(w, LT).start()
        across(w, RB).start()
        swap()

    def stage_b(w):
        for k in (LB, RT):
            arrive(w, k)
            across(w, k).start()
        swap()

    def stage_c(w):
        for k in (OT, OB):
            arrive(w, k)
            across(w, k).start()
        swap()

    def stage_d(w):
        for k in (PO, PASS + LT, PASS + RB, PASS + LB, PASS + RT, PASS + OT, PASS + OB):
            arrive(w, k)
        mine(w).wait()

    pieces = [(src.at[e], dst.at[e]) for e in range(w1_ref.shape[0]) for src, dst in ((w1_ref, o1_ref), (w3_ref, o3_ref), (w2_ref, o2_ref))
              if e < dst.shape[0]]
    swaps = [pltpu.make_async_remote_copy(src_ref=src, dst_ref=dst, send_sem=swap_send.at[i], recv_sem=swap_recv.at[i],
                                          device_id={"ep": partner}, device_id_type=MESH) for i, (src, dst) in enumerate(pieces)]
    waiting, quota = list(swaps), iter(SWAPS)

    def swap():
        for _ in range(min(int(next(quota)), len(waiting))):
            waiting.pop(0).start()

    ids = [pltpu.make_async_remote_copy(src_ref=id_ref, dst_ref=id4_ref.at[k + 1], send_sem=id_send.at[k], recv_sem=id_recv.at[k],
                                        device_id={"ep": dev}, device_id_type=MESH) for k, dev in enumerate(around)]
    ids.append(pltpu.make_async_copy(id_ref, id4_ref.at[0], id_send.at[3]))
    begin(0)
    for c in ids:
        c.start()
    swap()
    xin = pltpu.make_async_copy(x_ref, kb, iosem.at[0])
    xin.start()
    xin.wait()
    rb = min(256, t)
    rb3[:] = jnp.concatenate(split3(wr_ref[:]), axis=0)

    for e in range(LATE):
        room = w_ref.at[3, pl.ds(0, w2_ref.shape[1]), :]
        for c in (pltpu.make_async_copy(w2_ref.at[o2_ref.shape[0] + e], room, iosem.at[3]),
                  pltpu.make_async_copy(room, late_ref.at[e], iosem.at[3])):
            c.start()
            c.wait()

    @loop(t // rb)
    def _(i):
        r = pl.ds(pl.multiple_of(i * rb, rb), rb)
        ab[r, :] = rmsnorm(kb[r, :]).astype(BF)

    tm, tn = min(512, t), min(512, d)

    def project(w, dst, rope):
        @loop(d // tn)
        def _(n):
            @loop(t // tm)
            def _(m):
                r = pl.ds(pl.multiple_of(m * tm, tm), tm)
                z = dot(ab[r, :], w_ref[w, :, pl.ds(pl.multiple_of(n * tn, tn), tn)])
                for j in range(tn // HEAD):
                    zj = z[:, j * HEAD:(j + 1) * HEAD]
                    if rope:
                        zj = zj * cos_ref[r, :] + pltpu.roll(zj, HEAD // 2, 1) * sin_ref[r, :]
                    dst[r, pl.ds(pl.multiple_of(n * tn + j * HEAD, HEAD), HEAD)] = zj.astype(BF)

    for w, (dst, rope) in enumerate(((vb, False), (kb, True), (qb, True))):
        stage_a(w)
        stage_b(w)
        stage_c(w)
        stage_d(w)
        swap()
        project(w, dst, rope)
    stage_a(3)

    tq = min(256, t)
    scale = math.log2(math.e) / math.sqrt(HEAD)
    causal = lax.broadcasted_iota(I32, (tq, tq), 0) <= lax.broadcasted_iota(I32, (tq, tq), 1)
    group = min(4, d // HEAD)
    steps = d // HEAD // group
    marks = {1: stage_b, steps - 1: stage_c}
    if len(marks) > steps - 1:
        marks = {}
        stage_b(3)
        stage_c(3)

    @loop(steps)
    def _(jj):
        for at, stage in marks.items():
            pl.when(jj == at)(functools.partial(stage, 3))
        for j in range(group):
            c = pl.ds(pl.multiple_of((jj * group + j) * HEAD, HEAD), HEAD)
            for i in range(t // tq):
                r, n = slice(i * tq, (i + 1) * tq), (i + 1) * tq
                sc = lax.dot_general(kb[:n, c], qb[r, c], NT, preferred_element_type=F32)
                diag = jnp.where(causal, sc[i * tq:], -jnp.inf)
                sc = jnp.concatenate([sc[:i * tq], diag], axis=0) if i else diag
                p = jnp.exp2((sc - jnp.max(sc, axis=0, keepdims=True)) * scale)
                p = (p * (1.0 / jnp.sum(p, axis=0, keepdims=True))).astype(BF)
                qb[r, c] = lax.dot_general(p, vb[:n, c], TN, preferred_element_type=F32).astype(BF)

    swap()
    xin = pltpu.make_async_copy(x_ref, vb, iosem.at[0])
    xin.start()
    stage_d(3)
    xin.wait()

    @loop(d // tn)
    def _(n):
        c = pl.ds(pl.multiple_of(n * tn, tn), tn)

        @loop(t // tm)
        def _(m):
            r = pl.ds(pl.multiple_of(m * tm, tm), tm)
            ab[r, c] = (vb[r, c].astype(F32) + dot(qb[r, :], w_ref[3, :, c])).astype(BF)

    hout = pltpu.make_async_copy(ab, h_ref, iosem.at[0])
    hout.start()

    @loop(t // rb)
    def _(i):
        r = pl.ds(pl.multiple_of(i * rb, rb), rb)
        hi, mid, lo = split3(rmsnorm(ab[r, :]))
        kb[r, :] = hi
        ne = wr_ref.shape[0]
        part = lambda v, k: v[:, k * ne:(k + 1) * ne]
        p1, p2, p3 = [lax.dot_general(v, rb3[:n * ne], NT, preferred_element_type=F32) for v, n in ((hi, 3), (mid, 2), (lo, 1))]
        lg_ref[r, :] = part(p1, 0) + ((part(p1, 1) + part(p2, 0)) + (part(p1, 2) + part(p2, 1) + part(p3, 0)))

    uout = [pltpu.make_async_copy(kb.at[pl.ds(p * t // 2, t // 2), :], o, iosem.at[1 + p]) for p, o in enumerate((ut_ref, ub_ref))]
    for c in uout:
        c.start()
    assert not waiting
    for c in swaps + ids:
        c.wait()
    for w in range(4):
        for c in own(w) + [onward(w, OT), onward(w, OB)] + [across(w, k) for k in where]:
            c.wait_send()
    hout.wait()
    for c in uout:
        c.wait()


def attention_layer(nx, x, wv, wk, wq, wo, cos, sin, w1, w3, w2, wr, ids):
    t, d = x.shape
    hb = pl.BlockSpec(memory_space=pl.ANY)
    vm = pl.BlockSpec(memory_space=pltpu.VMEM)
    half = jax.ShapeDtypeStruct((t // 2, d), BF)
    act = pltpu.VMEM((t, d), BF)
    return pl.pallas_call(
        functools.partial(layer_kernel, nx),
        in_specs=[hb] * 5 + [vm] * 2 + [hb] * 3 + [vm, hb],
        out_specs=[hb] * 7 + [vm, hb],
        out_shape=[jax.ShapeDtypeStruct((t, d), BF), half, half, jax.ShapeDtypeStruct(w1.shape, BF),
                   jax.ShapeDtypeStruct(w3.shape, BF),
                   *[jax.ShapeDtypeStruct((n, *w2.shape[1:]), BF) for n in (w2.shape[0] - LATE, LATE)], jax.ShapeDtypeStruct((t, wr.shape[0]), F32),
                   jax.ShapeDtypeStruct((nx, *ids.shape), I32)],
        scratch_shapes=[pltpu.VMEM((4, d, d), BF), act, act, act, act, pltpu.VMEM((3 * wr.shape[0], d), BF),
                        pltpu.SemaphoreType.DMA((4, 13)), pltpu.SemaphoreType.DMA((4, 13)),
                        pltpu.SemaphoreType.DMA((4,)), pltpu.SemaphoreType.DMA((4,)),
                        pltpu.SemaphoreType.DMA((3 * w1.shape[0],)), pltpu.SemaphoreType.DMA((3 * w1.shape[0],)),
                        pltpu.SemaphoreType.DMA((nx,)), pltpu.SemaphoreType.DMA((nx,))],
        compiler_params=params(collective_id=0, has_side_effects=True),
        cost_estimate=cost(8 * t * d * d, 24 * t * d),
    )(x, wv, wk, wq, wo, cos, sin, w1, w3, w2, wr, ids)


def fetch_expert(l, slot, own, other, bufs, sem):
    ne, split = own[0].shape[0], other[2].shape[0]
    start = lambda src, dst: pltpu.make_async_copy(src, dst.at[slot], sem.at[slot]).start()

    @pl.when(l < ne)
    def _():
        for src, dst in zip(own, bufs):
            start(src.at[l], dst)

    @pl.when(l >= ne)
    def _():
        for src, dst in zip(other[:2], bufs):
            start(src.at[l - ne], dst)

    @pl.when(jnp.logical_and(l >= ne, l < ne + split))
    def _():
        start(other[2].at[l - ne], bufs[2])

    @pl.when(l >= ne + split)
    def _():
        start(other[3].at[l - ne - split], bufs[2])


def wait_expert(slot, own, bufs, sem):
    for src, dst in zip(own, bufs):
        pltpu.make_async_copy(src.at[0], dst.at[slot], sem.at[slot]).wait()


def ffn(x, w1, w3, w2):
    a1 = dot(x, w1)
    a3 = dot(x, w3)
    act = (jax.nn.silu(a1) * a3).astype(BF)
    return dot(act, w2).astype(BF)


def block_kernel(js, has_acc, comb, dense, *refs):
    refs = list(refs)
    nblk = len(js)
    take = lambda n: [refs.pop(0) for _ in range(n)]
    if any(dense):
        hot_ref, = take(1)
    gt_ref, = take(1)
    if comb:
        nch_ref, eg_ref, pos_ref, z_ref = take(4)
        cap = z_ref.shape[0] // pos_ref.shape[0]
    if any(dense):
        us = take(nblk)
        own, other = take(3), take(4)
        nl = 2 * own[0].shape[0]
    accs = [take(1)[0] if h else None for h in has_acc]
    outs = take(nblk)
    acc, asem = take(2)
    if comb:
        cbuf, zbuf, zsem = take(3)
    if any(dense):
        bufs, (ubuf, sem, usem, ent_ref) = take(3), take(4)
    t, d = outs[0].shape

    if any(dense):
        n = 0
        for p in range(nblk):
            def note(l, n, p=p):
                ent_ref[n] = p * nl + l
                return n + hot_ref[js[p] * nl + l]

            if dense[p]:
                n = lax.fori_loop(0, nl, note, n)

        @pl.when(n > 0)
        def _():
            fetch_expert(lax.rem(ent_ref[0], nl), 0, own, other, bufs, sem)

        ucp = [pltpu.make_async_copy(us[p], ubuf.at[pl.ds(p * t, t), :], usem) for p in range(nblk)]
        for cp in ucp:
            cp.start()
    for p in range(nblk):
        rows = pl.ds(p * t, t)
        if has_acc[p]:
            pltpu.make_async_copy(accs[p], acc.at[rows, :], asem.at[p]).start()
        else:
            acc[rows, :] = jnp.zeros((t, d), F32)
    for p in range(nblk):
        if has_acc[p]:
            pltpu.make_async_copy(accs[p], acc.at[pl.ds(p * t, t), :], asem.at[p]).wait()

    if comb:
        for p, j in enumerate(js):
            nch = nch_ref[j]

            def get(i, slot):
                src = pl.multiple_of(j * cap + i * CHUNK, CHUNK)
                return pltpu.make_async_copy(z_ref.at[pl.ds(src, CHUNK), :], zbuf.at[slot], zsem.at[slot])

            get(0, 0).start()
            nl = gt_ref.shape[1]
            lane = lax.broadcasted_iota(I32, (1, CHUNK), 1)
            ti = lax.broadcasted_iota(I32, (16, t), 1)
            si = lax.broadcasted_iota(I32, (16, t), 0)
            tparts = jnp.where(si == 0, ti % 256, jnp.where(si == 1, ti // 256, 0)).astype(F32).astype(BF)
            table = jnp.concatenate([*split3(gt_ref[j]), tparts], axis=0)

            @loop(nch)
            def _(i):
                slot = parity(i)

                @pl.when(i + 1 < nch)
                def _():
                    get(i + 1, 1 - slot).start()

                pm, ls = selection(j, i, eg_ref, pos_ref)
                el = jnp.zeros_like(lane)
                for q, l in enumerate(ls):
                    el = jnp.where(lane // PIECE == q, l, el)
                sel = lax.dot_general(table, pm, NT, preferred_element_type=F32)
                tok = (sel[3 * nl:3 * nl + 1] + 256.0 * sel[3 * nl + 1:3 * nl + 2]).astype(I32)
                hot_ = lax.broadcasted_iota(I32, (t, CHUNK), 0) == tok
                sub = lax.broadcasted_iota(I32, (nl, CHUNK), 0) == el
                for k in range(3):
                    gk = jnp.sum(jnp.where(sub, sel[k * nl:(k + 1) * nl], 0.0), axis=0, keepdims=True)
                    cbuf[:, k * CHUNK:(k + 1) * CHUNK] = jnp.where(hot_, gk, 0.0).astype(BF)
                get(i, slot).wait()
                tn = min(1024, d)

                @loop(d // tn)
                def _(m):
                    cs = pl.ds(pl.multiple_of(m * tn, tn), tn)
                    z = zbuf[slot, :, cs]
                    acc[p * t:(p + 1) * t, cs] += dot(cbuf[:], jnp.concatenate([z, z, z], axis=0))

    if any(dense):
        for cp in ucp:
            cp.wait()
        tm = min(HM, t)

        @loop(n)
        def _(i):
            slot = parity(i)
            wait_expert(slot, own, bufs, sem)

            @pl.when(i + 1 < n)
            def _():
                fetch_expert(lax.rem(ent_ref[i + 1], nl), 1 - slot, own, other, bufs, sem)

            p, e = lax.div(ent_ref[i], nl), lax.rem(ent_ref[i], nl)
            blk = js[0]
            for q in range(1, nblk):
                blk = jnp.where(p == q, js[q], blk)

            @loop(t // tm)
            def _(m):
                rows = pl.ds(pl.multiple_of(p * t + m * tm, tm), tm)
                z = ffn(ubuf[rows, :], bufs[0][slot], bufs[1][slot], bufs[2][slot])
                g = gt_ref[blk, pl.ds(e, 1), pl.ds(pl.multiple_of(m * tm, tm), tm)]
                eye = lax.broadcasted_iota(I32, (tm, tm), 0) == lax.broadcasted_iota(I32, (tm, tm), 1)
                gc = jnp.sum(jnp.where(eye, g, 0.0), axis=1, keepdims=True)
                acc[rows, :] += gc * z.astype(F32)

    if outs[0].dtype == F32:
        done = [pltpu.make_async_copy(acc.at[pl.ds(p * t, t), :], outs[p], asem.at[p]) for p in range(nblk)]
        for cp in done:
            cp.start()
        for cp in done:
            cp.wait()
    else:
        for p in range(nblk):
            outs[p][:] = acc[p * t:(p + 1) * t, :].astype(BF)


def block(js, r, z, us, accs, own, other, dtype, dense, comb=True):
    nblk = len(js)
    t = r.pos.shape[2]
    d = own[0].shape[1]
    ff = own[0].shape[2]
    nl = r.pos.shape[1]
    vm = pl.BlockSpec(memory_space=pltpu.VMEM)
    sm = pl.BlockSpec(memory_space=pltpu.SMEM)
    hb = pl.BlockSpec(memory_space=pl.ANY)
    args, specs, scratch = [], [], []
    if any(dense):
        args += [r.hot.reshape(-1)]
        specs += [sm]
    args += [r.gt]
    specs += [vm]
    if comb:
        args += [r.nch, r.eg.reshape(-1), r.pos, z]
        specs += [sm, sm, vm, hb]
    if any(dense):
        args += list(us) + list(own) + list(other)
        specs += [hb] * (nblk + 7)
    args += [v for v in accs if v is not None]
    specs += [hb for v in accs if v is not None]
    scratch += [pltpu.VMEM((nblk * t, d), F32), pltpu.SemaphoreType.DMA((nblk,))]
    if comb:
        scratch += [pltpu.VMEM((t, 3 * CHUNK), BF), pltpu.VMEM((2, CHUNK, d), BF), DMA2]
    if any(dense):
        scratch += [*expert_buffers(d, ff),
                    pltpu.VMEM((nblk * t, d), BF), DMA2, pltpu.SemaphoreType.DMA,
                    pltpu.SMEM((nblk * nl,), I32)]
    out = jax.ShapeDtypeStruct((t, d), dtype)
    return pl.pallas_call(
        functools.partial(block_kernel, js, [v is not None for v in accs], comb, dense),
        in_specs=specs, out_specs=[hb if dtype == F32 else vm] * nblk, out_shape=[out] * nblk, scratch_shapes=scratch,
        compiler_params=params(),
        cost_estimate=cost(t * d, 6 * d * ff),
    )(*args)


def selection(j, i, eg_ref, pos_ref):
    t = pos_ref.shape[2]
    it = lax.broadcasted_iota(I32, (2 * PIECE, t), 0)
    npc = CHUNK // PIECE
    first = (j * (eg_ref.shape[0] // pos_ref.shape[0] // npc) + i) * npc
    ls = [eg_ref[first + q] for q in range(npc)]
    hits = []
    for q in range(0, npc, 2):
        own, nxt = [pos_ref[j, pl.ds(l, 1), :] for l in ls[q:q + 2]]
        hit = jnp.where(it < PIECE, own, nxt) - (i * CHUNK + q * PIECE) == it
        hits.append(jnp.where(hit, 1.0, 0.0).astype(BF))
    return jnp.concatenate(hits, axis=0), ls


def gather_kernel(js, nch_ref, eg_ref, pos_ref, *refs):
    us, (x_ref, ubuf, xbuf, usem, sem) = refs[:len(js)], refs[-5:]
    cap = x_ref.shape[0] // pos_ref.shape[0]
    cps = [pltpu.make_async_copy(u, ubuf.at[p % 2], usem.at[p % 2]) for p, u in enumerate(us)]
    cps[0].start()

    def out(slot, row):
        return pltpu.make_async_copy(xbuf.at[slot], x_ref.at[pl.ds(pl.multiple_of(row, CHUNK), CHUNK), :], sem.at[slot])

    made = 0
    for p, j in enumerate(js):
        if p + 1 < len(js):
            cps[p + 1].start()
        cps[p].wait()

        @loop(nch_ref[j])
        def _(i):
            slot = parity(made + i)

            @pl.when(made + i >= 2)
            def _():
                out(slot, 0).wait()

            xbuf[slot] = dot(selection(j, i, eg_ref, pos_ref)[0], ubuf[p % 2]).astype(BF)
            out(slot, j * cap + i * CHUNK).start()

        made = made + nch_ref[j]
    for k in (2, 1):
        @pl.when(made >= k)
        def _():
            out(parity(made - k), 0).wait()


def gather(js, r, us, x):
    t, d = us[0].shape
    rows = r.eg.size * PIECE
    vm = pl.BlockSpec(memory_space=pltpu.VMEM)
    sm = pl.BlockSpec(memory_space=pltpu.SMEM)
    hb = pl.BlockSpec(memory_space=pl.ANY)
    more = [] if x is None else [x]
    return pl.pallas_call(
        functools.partial(gather_kernel, js),
        in_specs=[sm, sm, vm] + [hb] * len(us + more),
        out_specs=hb,
        out_shape=jax.ShapeDtypeStruct((rows, d), BF),
        input_output_aliases={3 + len(us): 0} if more else {},
        scratch_shapes=[pltpu.VMEM((2, t, d), BF), pltpu.VMEM((2, CHUNK, d), BF), DMA2, DMA2],
        compiler_params=params(),
        cost_estimate=cost(t * d, 4 * CHUNK * d),
    )(r.nch, r.eg.reshape(-1), r.pos, *us, *more)


def cold_kernel(np_ref, pc_ref, x_ref, *refs):
    own, other, z_ref, refs = refs[:3], refs[3:7], refs[7], refs[8:]
    bufs, (xbuf, zbuf, wsem, xsem, zsem, tl_ref, tp_ref, tn_ref, tw_ref, nx_ref) = refs[:3], refs[3:]
    ppt = MT // PIECE

    def tiles(l, carry):
        q, turn, p = carry
        n = np_ref[l]
        more = lax.div(n + ppt - 1, ppt)

        @loop(more)
        def _(i):
            tl_ref[q + i] = l
            tp_ref[q + i] = p + i * ppt
            tn_ref[q + i] = jnp.minimum(n - i * ppt, ppt)
            tw_ref[q + i] = turn
            nx_ref[q + i] = jnp.where(i == 0, q + more, 0)

        return q + more, turn + jnp.minimum(n, 1), p + n

    nt = lax.fori_loop(0, np_ref.shape[0], tiles, (0, 0, 0))[0]

    def each(n, fn):
        @loop(lax.div(n, 2))
        def _(i):
            fn(2 * i)
            fn(2 * i + 1)

        @pl.when(parity(n) == 1)
        def _():
            fn(n - 1)

    def xin(q, slot):
        p0 = tp_ref[q]

        def one(i):
            src = pl.ds(pl.multiple_of(pc_ref[p0 + i] * PIECE, PIECE), PIECE)
            dst = pl.ds(pl.multiple_of(i * PIECE, PIECE), PIECE)
            pltpu.make_async_copy(x_ref.at[src, :], xbuf.at[slot, dst, :], xsem.at[slot]).start()

        each(tn_ref[q], one)

    def zout(q, slot):
        p0 = tp_ref[q]

        def one(i):
            src = pl.ds(pl.multiple_of(i * PIECE, PIECE), PIECE)
            dst = pl.ds(pl.multiple_of(pc_ref[p0 + i] * PIECE, PIECE), PIECE)
            pltpu.make_async_copy(zbuf.at[slot, src, :], z_ref.at[dst, :], zsem.at[slot]).start()

        each(tn_ref[q], one)

    def drain(n, fn):
        bit = 1
        while bit <= MT // PIECE:
            @pl.when(lax.rem(lax.div(n, bit), 2) == 1)
            def _(bit=bit):
                fn(pl.ds(0, bit * PIECE))

            bit *= 2

    def xwait(q, slot):
        drain(tn_ref[q], lambda r: pltpu.make_async_copy(x_ref.at[r, :], xbuf.at[slot, r, :], xsem.at[slot]).wait())

    def zwait(q, slot):
        drain(tn_ref[q], lambda r: pltpu.make_async_copy(zbuf.at[slot, r, :], z_ref.at[r, :], zsem.at[slot]).wait())

    @pl.when(nt > 0)
    def _():
        fetch_expert(tl_ref[0], 0, own, other, bufs, wsem)
        xin(0, 0)

    @loop(nt)
    def _(q):
        slot = parity(q)
        ws = parity(tw_ref[q])

        @pl.when(nx_ref[q] > 0)
        def _():
            wait_expert(ws, own, bufs, wsem)

            @pl.when(nx_ref[q] < nt)
            def _():
                fetch_expert(tl_ref[nx_ref[q]], 1 - ws, own, other, bufs, wsem)

        @pl.when(q + 1 < nt)
        def _():
            xin(q + 1, 1 - slot)

        xwait(q, slot)

        @pl.when(q >= 2)
        def _():
            zwait(q - 2, slot)

        zbuf[slot] = ffn(xbuf[slot], bufs[0][ws], bufs[1][ws], bufs[2][ws])
        zout(q, slot)

    for k in (2, 1):
        @pl.when(nt >= k)
        def _():
            zwait(nt - k, parity(nt - k))


def cold(plan, x, own, other):
    d, ff = own[0].shape[1:]
    sm = pl.BlockSpec(memory_space=pltpu.SMEM)
    hb = pl.BlockSpec(memory_space=pl.ANY)
    return pl.pallas_call(
        cold_kernel,
        in_specs=[sm] * len(plan) + [hb] * 8,
        out_specs=hb,
        out_shape=jax.ShapeDtypeStruct(x.shape, BF),
        scratch_shapes=[*expert_buffers(d, ff),
                        pltpu.VMEM((2, MT, d), BF), pltpu.VMEM((2, MT, d), BF),
                        DMA2, DMA2, DMA2, *5 * [pltpu.SMEM((plan[1].size * PIECE // MT + plan[0].size + 1,), I32)]],
        input_output_aliases={len(plan): 0},
        compiler_params=params(),
        cost_estimate=cost(6 * 16 * MT * d * ff, 96 * d * ff),
    )(*plan, x, *own, *other)


def final_kernel(h_ref, *refs):
    y_ref = refs[-1]
    acc, parts = refs[0], refs[1:-1]
    y = h_ref[:].astype(F32) + acc[:]
    for v in parts:
        y = y + v[:].astype(F32)
    y_ref[:] = y.astype(BF)


def final(h, accs, parts):
    t, d = h.shape
    half = t // 2
    tm = min(256, half)
    n = half // tm

    def body(h_ref, *refs):
        for p in range(2):
            @pl.when(pl.program_id(0) // n == p)
            def _():
                final_kernel(h_ref, refs[p], *refs[2 + p:-1:2], refs[-1])

    spec = lambda p: pl.BlockSpec((tm, d), lambda i: (jnp.minimum(i, n - 1) if p == 0 else jnp.maximum(i - n, 0), 0))
    return pl.pallas_call(
        body, grid=(2 * n,),
        in_specs=[pl.BlockSpec((tm, d), lambda i: (i, 0))] + [spec(0), spec(1)] * (1 + len(parts)),
        out_specs=pl.BlockSpec((tm, d), lambda i: (i, 0)),
        out_shape=jax.ShapeDtypeStruct((t, d), BF),
        compiler_params=params(),
        cost_estimate=cost(6 * t * d, 20 * t * d),
    )(h, *accs, *[v for part in parts for v in part])


class Routing(typing.NamedTuple):
    hot: typing.Any
    nch: typing.Any
    eg: typing.Any
    pos: typing.Any
    gt: typing.Any


def routing_plan(lid, local, nl):
    nb, t, k = lid.shape
    le = jnp.arange(nl, dtype=I32)
    hit = jnp.any((lid[:, None] == le[:, None, None]) & local[:, None], axis=-1)
    tri = (jnp.arange(t)[:, None] <= jnp.arange(t)[None, :]).astype(BF)
    rank = lax.dot_general(hit.astype(BF), tri, (((2,), (0,)), ((), ())), preferred_element_type=F32).astype(I32)
    cnt = rank[:, :, -1]
    hotm = cnt >= t // 2
    scnt = jnp.where(hotm, 0, cnt)
    pcs = (scnt + PIECE - 1) // PIECE
    pend = jnp.cumsum(pcs, axis=1)
    base = (pend - pcs) * PIECE
    pos = jnp.where(hit & ~hotm[..., None], base[..., None] + rank - 1, -1)
    rows = t * k + nl * PIECE
    npb = -(-rows // CHUNK) * CHUNK // PIECE
    nch = jnp.maximum(-(-pend[:, -1] * PIECE // CHUNK), 1)
    below = lambda ends, q: jnp.sum((ends <= q).astype(I32), axis=-1)
    eg = jnp.minimum(below(pend[:, None, :], jnp.arange(npb, dtype=I32)[None, :, None]), nl - 1)
    flat = pcs.T.reshape(-1)
    fend = jnp.cumsum(flat)
    p = jnp.arange(nb * npb, dtype=I32)[:, None]
    seg = jnp.minimum(below(fend[None, :], p), nl * nb - 1)
    inseg = seg[:, None] == jnp.arange(nl * nb, dtype=I32)
    shift_ = jnp.tile(jnp.arange(nb, dtype=I32) * npb, nl) + (pend - pcs).T.reshape(-1) - (fend - flat)
    pc = jnp.clip(p[:, 0] + jnp.sum(jnp.where(inseg, shift_, 0), axis=1), 0, nb * npb - 1)
    return Routing(hotm.astype(I32), nch, eg, pos, None), (jnp.sum(pcs, axis=0), pc)


ON = (True,)


def solution(mesh):
    nd = mesh.shape['ep']
    nx = nd // 2
    tok_spec = P(('replica', 'ep'), None, None)
    rows_ep = P('ep', None)
    by_expert = P('ep', None, None)

    def shift(v, s):
        return lax.ppermute(v, 'ep', [(2 * i + c, 2 * ((i + s) % nx) + c) for i in range(nx) for c in range(2)])

    def local(x, wq, wk, wv, wo, wr, w1, w3, w2, idx):
        b, s, d = x.shape
        t, k, ne = b * s, idx.shape[-1], w1.shape[0]
        nl = 2 * ne
        half = t // 2
        me = lax.axis_index('ep')
        x = x.reshape(t, d)
        ids = idx.reshape(t, k)

        hd = HEAD // 2
        ang = (np.arange(t) % s).astype(np.float32)[:, None] * np.float32(THETA) ** (-np.arange(hd, dtype=np.float32) / hd)
        c, sn = np.cos(ang), np.sin(ang)
        cos, sin = [jnp.asarray(np.concatenate(v, axis=1), F32) for v in ((c, c), (-sn, sn))]
        h, ut, ub, o1, o3, o2, late, logits, ids4 = attention_layer(nx, x, wv, wk, wq, wo, cos, sin, w1, w3, w2, wr.T, ids.T)
        ids4 = jnp.swapaxes(ids4, 1, 2)
        late = lax.ppermute(late, 'ep', [(i, i ^ 1) for i in range(nd)])
        own, other = (w1, w3, w2), (o1, o3, o2, late)

        halves = lambda v: v.reshape(2 * v.shape[0], half, *v.shape[2:])
        is_local = halves(ids4 // nl == me // 2)
        lid = halves((ids4 - me * ne) % nl)
        r, plan = routing_plan(lid, is_local, nl)
        ohl = (lid[:, None] == jnp.arange(nl, dtype=I32)[:, None, None]) & is_local[:, None]

        u1t, u2b = shift(ut, 1), shift(ub, -1)
        oh = ids[..., None] == jnp.arange(wr.shape[1], dtype=I32)
        g = jax.nn.softmax(jnp.sum(jnp.where(oh, logits[:, None, :], 0.0), axis=-1), axis=-1)
        ut2, ub2, g = lax.optimization_barrier((ut, ub, g))
        g4 = [g, shift(g, 1), shift(g, -1), shift(g, 2)]
        u1b, u2t = shift(ub2, 1), shift(ut2, -1)
        spread = lambda o, v: jnp.sum(jnp.where(o, halves(v)[:, None], 0.0), axis=3)
        ra = r._replace(gt=spread(ohl[:2], g[None]))
        r = r._replace(gt=spread(ohl, jnp.stack(g4)))

        a0, = block((0,), ra, None, (ut,), (None,), own, other, F32, ON, comb=False)
        a0, u1t, u2b = lax.optimization_barrier((a0, u1t, u2b))
        u3t, u3b = shift(u1t, 1), shift(u2b, -1)
        d2, d5 = block((2, 5), r, None, (u1t, u2b), 2 * (None,), own, other, F32, 2 * ON, comb=False)
        u1b, d2 = lax.optimization_barrier((u1b, d2))
        x = gather(tuple(range(6)), r, [ut, ub, u1t, u1b, u2t, u2b], None)
        u3t, x = lax.optimization_barrier((u3t, x))
        x = gather((6, 7), r, [u3t, u3b], x)
        z = cold(plan, x, own, other)

        tie = lambda r, *v: (lambda w: (r._replace(nch=w[0]), *w[1:]))(lax.optimization_barrier((r.nch, *v)))
        b6, = block((6,), r, z, (u3t,), (None,), own, other, BF, ON)
        r, b6 = tie(r, b6)
        c6 = shift(b6, 1)
        b2, b5 = block((2, 5), r, z, (), (d2, d5), own, other, BF, (False, False))
        r, b2, b5 = tie(r, b2, b5)
        b2, b5 = shift(b2, -1), shift(b5, 1)
        b7, = block((7,), r, z, (u3b,), (None,), own, other, BF, ON)
        r, b7, c6 = tie(r, b7, c6)
        c7, b6 = shift(b7, -1), shift(c6, 1)
        b3, = block((3,), r, z, (u1b,), (None,), own, other, BF, ON)
        r, b3 = tie(r, b3)
        b3 = shift(b3, -1)
        b4, = block((4,), r, z, (u2t,), (None,), own, other, BF, ON)
        r, b4, c7 = tie(r, b4, c7)
        b4, b7 = shift(b4, 1), shift(c7, -1)
        accs = block((0, 1), r, z, (ut, ub), (a0, None), own, other, F32, (False, True))
        y = final(h, accs, [(b2, b3), (b4, b5), (b6, b7)])
        return y.reshape(b, s, d)

    return jax.shard_map(local, mesh=mesh,
                         in_specs=(tok_spec, rows_ep, rows_ep, rows_ep, rows_ep, P(None, None),
                                   by_expert, by_expert, by_expert, tok_spec),
                         out_specs=tok_spec, check_vma=False)
```

```python
import functools
import math
import typing
import jax
import jax.numpy as jnp
import numpy as np
from jax import lax
from jax.experimental import pallas as pl
from jax.experimental.pallas import tpu as pltpu
from jax.sharding import PartitionSpec as P

HEAD = 128
EPS = 1e-6
THETA = 10000.0
PIECE = 8
CHUNK = 256
MT = 352
HM = 512
VMEM = 66_000_000
BF, F32, I32 = jnp.bfloat16, jnp.float32, jnp.int32


def rmsnorm(v):
    v = v.astype(F32)
    return v * lax.rsqrt(jnp.mean(v * v, axis=-1, keepdims=True) + EPS)


def dot(a, b):
    return jnp.dot(a, b, preferred_element_type=F32)


NT = (((1,), (1,)), ((), ()))
TN = (((0,), (0,)), ((), ()))
DMA2 = pltpu.SemaphoreType.DMA((2,))


def cost(flops, bytes_):
    return pl.CostEstimate(flops=flops, bytes_accessed=bytes_, transcendentals=0)


def parity(i):
    return lax.rem(i, 2)


def expert_buffers(d, ff):
    return [pltpu.VMEM((2, *v), BF) for v in ((d, ff), (d, ff), (ff, d))]


def loop(n):
    return pl.loop(0, n)


def params(**kw):
    return pltpu.CompilerParams(vmem_limit_bytes=VMEM, **kw)


def split3(g):
    hi = g.astype(BF)
    r = g - hi.astype(F32)
    mid = r.astype(BF)
    lo = (r - mid.astype(F32)).astype(BF)
    return hi, mid, lo


LT, LB, RT, RB, OT, OB, PO, PASS = range(8)
LATE = 3
SWAPS = "41111111110022229"
MESH = pl.DeviceIdType.MESH


def layer_kernel(nx, x_ref, wv_ref, wk_ref, wq_ref, wo_ref, cos_ref, sin_ref, w1_ref, w3_ref, w2_ref, wr_ref, id_ref,
                 h_ref, ut_ref, ub_ref, o1_ref, o3_ref, o2_ref, late_ref, lg_ref, id4_ref,
                 w_ref, ab, qb, kb, vb, rb3, fb, ssem, rsem, lsem, iosem, swap_send, swap_recv, id_send, id_recv):
    shards = (wv_ref, wk_ref, wq_ref, wo_ref)
    last = len(shards) - 1
    sh = wv_ref.shape[0]
    hs = sh // 2
    t, d = ab.shape
    me = lax.axis_index("ep")
    chip, core = me // 2, me % 2
    right, left, opp = [2 * ((chip + k) % nx) + core for k in (1, nx - 1, 2)]
    partner = 2 * chip + 1 - core

    barrier = pltpu.get_barrier_semaphore()
    around = (right, left, opp)
    for dev in (*around, partner):
        pl.semaphore_signal(barrier, inc=1, device_id={"ep": dev}, device_id_type=MESH)
    pl.semaphore_wait(barrier, 4)

    def rows(e, half=None):
        if half is None:
            return pl.ds(pl.multiple_of(e * sh, sh), sh)
        return pl.ds(pl.multiple_of(e * sh + half * hs, hs), hs)

    def remote(w, src, dst, dev, s, r):
        return pltpu.make_async_remote_copy(src_ref=src, dst_ref=w_ref.at[w, dst, :], send_sem=ssem.at[w, s],
                                            recv_sem=rsem.at[w, r], device_id={"ep": dev}, device_id_type=MESH)

    def own(w):
        src = shards[w]
        top, bot = src.at[:hs, :], src.at[hs:, :]
        return [remote(w, top, rows(me, 0), right, 0, LT), remote(w, bot, rows(me, 1), left, 1, RB),
                remote(w, bot, rows(me, 1), right, 2, LB), remote(w, top, rows(me, 0), left, 3, RT),
                remote(w, src, rows(me), partner, 6, PO)]

    def mine(w):
        return pltpu.make_async_copy(shards[w], w_ref.at[w, rows(me), :], lsem.at[w])

    where = {LT: (left, 0), LB: (left, 1), RT: (right, 0), RB: (right, 1), OT: (opp, 0), OB: (opp, 1)}

    def onward(w, k):
        e, half = where[LT if k == OT else RB]
        return remote(w, w_ref.at[w, rows(e, half), :], rows(e, half), right if k == OT else left, 4 if k == OT else 5, k)

    def across(w, k):
        r = rows(*where[k])
        return remote(w, w_ref.at[w, r, :], r, partner, PASS + k, PASS + k)

    def arrive(w, k):
        r = rows(me) if k == PO else rows(*where[k % PASS])
        remote(w, w_ref.at[w, r, :], r, partner, 0, k).wait_recv()

    def begin(w):
        for c in own(w):
            c.start()
        mine(w).start()

    def stage_a(w):
        arrive(w, LT)
        onward(w, OT).start()
        arrive(w, RB)
        onward(w, OB).start()
        if w < last:
            begin(w + 1)
        across(w, LT).start()
        across(w, RB).start()
        swap()

    def stage_b(w):
        for k in (LB, RT):
            arrive(w, k)
            across(w, k).start()
        swap()

    def stage_c(w):
        for k in (OT, OB):
            arrive(w, k)
            across(w, k).start()
        swap()

    def near(w):
        for k in (PO, PASS + LT, PASS + RB, PASS + LB, PASS + RT):
            arrive(w, k)
        mine(w).wait()

    def far(w):
        for k in (PASS + OT, PASS + OB):
            arrive(w, k)

    pieces = [(src.at[e], dst.at[e]) for e in range(w1_ref.shape[0]) for src, dst in ((w1_ref, o1_ref), (w3_ref, o3_ref), (w2_ref, o2_ref))
              if e < dst.shape[0]]
    swaps = [pltpu.make_async_remote_copy(src_ref=src, dst_ref=dst, send_sem=swap_send.at[i], recv_sem=swap_recv.at[i],
                                          device_id={"ep": partner}, device_id_type=MESH) for i, (src, dst) in enumerate(pieces)]
    waiting, quota = list(swaps), iter(SWAPS)

    def swap():
        for _ in range(min(int(next(quota)), len(waiting))):
            waiting.pop(0).start()

    ids = [pltpu.make_async_remote_copy(src_ref=id_ref, dst_ref=id4_ref.at[k + 1], send_sem=id_send.at[k], recv_sem=id_recv.at[k],
                                        device_id={"ep": dev}, device_id_type=MESH) for k, dev in enumerate(around)]
    ids.append(pltpu.make_async_copy(id_ref, id4_ref.at[0], id_send.at[3]))
    begin(0)
    for c in ids:
        c.start()
    swap()
    xin = pltpu.make_async_copy(x_ref, kb, iosem.at[0])
    xin.start()
    xin.wait()
    rb = min(256, t)
    rb3[:] = jnp.concatenate(split3(wr_ref[:]), axis=0)

    for e in range(LATE):
        room = w_ref.at[last, :w2_ref.shape[1], :]
        for c in (pltpu.make_async_copy(w2_ref.at[o2_ref.shape[0] + e], room, iosem.at[3]),
                  pltpu.make_async_copy(room, late_ref.at[e], iosem.at[3])):
            c.start()
            c.wait()

    @loop(t // rb)
    def _(i):
        r = pl.ds(pl.multiple_of(i * rb, rb), rb)
        ab[r, :] = rmsnorm(kb[r, :]).astype(BF)

    tm, tn = [min(512, v) for v in (t, d)]

    def tiles(lo, hi, fn):
        @pl.loop(lo, hi)
        def _(n):
            @loop(t // tm)
            def _(m):
                fn(pl.ds(pl.multiple_of(m * tm, tm), tm), pl.multiple_of(n * tn, tn))

    def some(a, w, r, n, chips):
        ks = [pl.ds(pl.multiple_of(2 * sh * c, 2 * sh), 2 * sh) for c in chips]
        return functools.reduce(jnp.add, [dot(a[r, k], w_ref[w, k, pl.ds(n, tn)]) for k in ks])

    close, across_ = (chip, left // 2, right // 2), (opp // 2,)

    def ahead(a, w):
        def fn(r, n):
            fb[r, pl.ds(n, tn)] = some(a, w, r, n, close)

        near(w)
        tiles(0, d // tn // 2, fn)
        stage_c(w)
        tiles(d // tn // 2, d // tn, fn)
        far(w)

    def put(dst, rope, r, n, z):
        for j in range(tn // HEAD):
            zj = z[:, j * HEAD:(j + 1) * HEAD]
            if rope:
                zj = zj * cos_ref[r, :] + pltpu.roll(zj, HEAD // 2, 1) * sin_ref[r, :]
            dst[r, pl.ds(pl.multiple_of(n + j * HEAD, HEAD), HEAD)] = zj.astype(BF)

    for w, (dst, rope) in enumerate(((vb, False), (kb, True))):
        stage_a(w)
        stage_b(w)
        stage_c(w)
        near(w)
        far(w)
        swap()
        tiles(0, d // tn, lambda r, n: put(dst, rope, r, n, dot(ab[r, :], w_ref[w, :, pl.ds(n, tn)])))
    w = last - 1
    stage_a(w)
    stage_b(w)
    ahead(ab, w)
    swap()
    tiles(0, d // tn, lambda r, n: put(qb, True, r, n, fb[r, pl.ds(n, tn)] + some(ab, w, r, n, across_)))
    stage_a(last)

    tq = rb
    scale = math.log2(math.e) / math.sqrt(HEAD)
    causal = lax.broadcasted_iota(I32, (tq, tq), 0) <= lax.broadcasted_iota(I32, (tq, tq), 1)
    group = min(4, d // HEAD)
    steps = d // HEAD // group
    if steps == 1:
        stage_b(last)

    @loop(steps)
    def _(jj):
        if steps > 1:
            pl.when(jj == 1)(functools.partial(stage_b, last))
        for j in range(group):
            c = pl.ds(pl.multiple_of((jj * group + j) * HEAD, HEAD), HEAD)
            for i in range(t // tq):
                r, n = slice(i * tq, (i + 1) * tq), (i + 1) * tq
                sc = lax.dot_general(kb[:n, c], qb[r, c], NT, preferred_element_type=F32)
                diag = jnp.where(causal, sc[i * tq:], -jnp.inf)
                sc = jnp.concatenate([sc[:i * tq], diag], axis=0) if i else diag
                p = jnp.exp2((sc - jnp.max(sc, axis=0, keepdims=True)) * scale)
                p = (p * (1.0 / jnp.sum(p, axis=0, keepdims=True))).astype(BF)
                qb[r, c] = lax.dot_general(p, vb[:n, c], TN, preferred_element_type=F32).astype(BF)

    swap()
    xin = pltpu.make_async_copy(x_ref, vb, iosem.at[0])
    xin.start()
    ahead(qb, last)
    xin.wait()

    def residual(r, n):
        c = pl.ds(n, tn)
        ab[r, c] = (vb[r, c].astype(F32) + (fb[r, c] + some(qb, last, r, n, across_))).astype(BF)

    tiles(0, d // tn, residual)
    hout = pltpu.make_async_copy(ab, h_ref, iosem.at[0])
    hout.start()

    @loop(t // rb)
    def _(i):
        r = pl.ds(pl.multiple_of(i * rb, rb), rb)
        hi, mid, lo = split3(rmsnorm(ab[r, :]))
        kb[r, :] = hi
        ne = wr_ref.shape[0]
        part = lambda v, k: v[:, k * ne:(k + 1) * ne]
        p1, p2, p3 = [lax.dot_general(v, rb3[:n * ne], NT, preferred_element_type=F32) for v, n in ((hi, 3), (mid, 2), (lo, 1))]
        lg_ref[r, :] = part(p1, 0) + ((part(p1, 1) + part(p2, 0)) + (part(p1, 2) + part(p2, 1) + part(p3, 0)))

    uout = [pltpu.make_async_copy(kb.at[pl.ds(p * t // 2, t // 2), :], o, iosem.at[1 + p]) for p, o in enumerate((ut_ref, ub_ref))]
    for c in uout:
        c.start()
    assert not waiting
    for c in swaps + ids:
        c.wait()
    for w in range(last + 1):
        for c in own(w) + [onward(w, OT), onward(w, OB)] + [across(w, k) for k in where]:
            c.wait_send()
    hout.wait()
    for c in uout:
        c.wait()


def attention_layer(nx, x, wv, wk, wq, wo, cos, sin, w1, w3, w2, wr, ids):
    t, d = x.shape
    hb = pl.BlockSpec(memory_space=pl.ANY)
    vm = pl.BlockSpec(memory_space=pltpu.VMEM)
    half = jax.ShapeDtypeStruct((t // 2, d), BF)
    act = pltpu.VMEM((t, d), BF)
    return pl.pallas_call(
        functools.partial(layer_kernel, nx),
        in_specs=[hb] * 5 + [vm] * 2 + [hb] * 3 + [vm, hb],
        out_specs=[hb] * 7 + [vm, hb],
        out_shape=[jax.ShapeDtypeStruct((t, d), BF), half, half, jax.ShapeDtypeStruct(w1.shape, BF),
                   jax.ShapeDtypeStruct(w3.shape, BF),
                   *[jax.ShapeDtypeStruct((n, *w2.shape[1:]), BF) for n in (w2.shape[0] - LATE, LATE)], jax.ShapeDtypeStruct((t, wr.shape[0]), F32),
                   jax.ShapeDtypeStruct((nx, *ids.shape), I32)],
        scratch_shapes=[pltpu.VMEM((4, d, d), BF), act, act, act, act, pltpu.VMEM((3 * wr.shape[0], d), BF), pltpu.VMEM((t, d), F32),
                        pltpu.SemaphoreType.DMA((4, 13)), pltpu.SemaphoreType.DMA((4, 13)),
                        pltpu.SemaphoreType.DMA((4,)), pltpu.SemaphoreType.DMA((4,)),
                        pltpu.SemaphoreType.DMA((3 * w1.shape[0],)), pltpu.SemaphoreType.DMA((3 * w1.shape[0],)),
                        pltpu.SemaphoreType.DMA((nx,)), pltpu.SemaphoreType.DMA((nx,))],
        compiler_params=params(collective_id=0, has_side_effects=True),
        cost_estimate=cost(8 * t * d * d, 24 * t * d),
    )(x, wv, wk, wq, wo, cos, sin, w1, w3, w2, wr, ids)


def fetch_expert(l, slot, own, other, bufs, sem):
    ne, split = own[0].shape[0], other[2].shape[0]
    start = lambda src, dst: pltpu.make_async_copy(src, dst.at[slot], sem.at[slot]).start()

    @pl.when(l < ne)
    def _():
        for src, dst in zip(own, bufs):
            start(src.at[l], dst)

    @pl.when(l >= ne)
    def _():
        for src, dst in zip(other[:2], bufs):
            start(src.at[l - ne], dst)

    @pl.when(jnp.logical_and(l >= ne, l < ne + split))
    def _():
        start(other[2].at[l - ne], bufs[2])

    @pl.when(l >= ne + split)
    def _():
        start(other[3].at[l - ne - split], bufs[2])


def wait_expert(slot, own, bufs, sem):
    for src, dst in zip(own, bufs):
        pltpu.make_async_copy(src.at[0], dst.at[slot], sem.at[slot]).wait()


def ffn(x, w1, w3, w2):
    a1 = dot(x, w1)
    a3 = dot(x, w3)
    act = (jax.nn.silu(a1) * a3).astype(BF)
    return dot(act, w2).astype(BF)


def block_kernel(js, has_acc, comb, dense, *refs):
    refs = list(refs)
    nblk = len(js)
    take = lambda n: [refs.pop(0) for _ in range(n)]
    if any(dense):
        hot_ref, = take(1)
    gt_ref, = take(1)
    if comb:
        nch_ref, eg_ref, pos_ref, z_ref = take(4)
        cap = z_ref.shape[0] // pos_ref.shape[0]
    if any(dense):
        us = take(nblk)
        own, other = take(3), take(4)
        nl = 2 * own[0].shape[0]
    accs = [take(1)[0] if h else None for h in has_acc]
    outs = take(nblk)
    acc, asem = take(2)
    if comb:
        cbuf, zbuf, zsem = take(3)
    if any(dense):
        bufs, (ubuf, sem, usem, ent_ref) = take(3), take(4)
    t, d = outs[0].shape

    if any(dense):
        n = 0
        for p in range(nblk):
            def note(l, n, p=p):
                ent_ref[n] = p * nl + l
                return n + hot_ref[js[p] * nl + l]

            if dense[p]:
                n = lax.fori_loop(0, nl, note, n)

        @pl.when(n > 0)
        def _():
            fetch_expert(lax.rem(ent_ref[0], nl), 0, own, other, bufs, sem)

        ucp = [pltpu.make_async_copy(us[p], ubuf.at[pl.ds(p * t, t), :], usem) for p in range(nblk)]
        for cp in ucp:
            cp.start()
    for p in range(nblk):
        rows = pl.ds(p * t, t)
        if has_acc[p]:
            pltpu.make_async_copy(accs[p], acc.at[rows, :], asem.at[p]).start()
        else:
            acc[rows, :] = jnp.zeros((t, d), F32)
    for p in range(nblk):
        if has_acc[p]:
            pltpu.make_async_copy(accs[p], acc.at[pl.ds(p * t, t), :], asem.at[p]).wait()

    if comb:
        for p, j in enumerate(js):
            nch = nch_ref[j]

            def get(i, slot):
                src = pl.multiple_of(j * cap + i * CHUNK, CHUNK)
                return pltpu.make_async_copy(z_ref.at[pl.ds(src, CHUNK), :], zbuf.at[slot], zsem.at[slot])

            get(0, 0).start()
            nl = gt_ref.shape[1]
            lane = lax.broadcasted_iota(I32, (1, CHUNK), 1)
            ti = lax.broadcasted_iota(I32, (16, t), 1)
            si = lax.broadcasted_iota(I32, (16, t), 0)
            tparts = jnp.where(si == 0, ti % 256, jnp.where(si == 1, ti // 256, 0)).astype(F32).astype(BF)
            table = jnp.concatenate([*split3(gt_ref[j]), tparts], axis=0)

            @loop(nch)
            def _(i):
                slot = parity(i)

                @pl.when(i + 1 < nch)
                def _():
                    get(i + 1, 1 - slot).start()

                pm, ls = selection(j, i, eg_ref, pos_ref)
                el = jnp.zeros_like(lane)
                for q, l in enumerate(ls):
                    el = jnp.where(lane // PIECE == q, l, el)
                sel = lax.dot_general(table, pm, NT, preferred_element_type=F32)
                tok = (sel[3 * nl:3 * nl + 1] + 256.0 * sel[3 * nl + 1:3 * nl + 2]).astype(I32)
                hot_ = lax.broadcasted_iota(I32, (t, CHUNK), 0) == tok
                sub = lax.broadcasted_iota(I32, (nl, CHUNK), 0) == el
                for k in range(3):
                    gk = jnp.sum(jnp.where(sub, sel[k * nl:(k + 1) * nl], 0.0), axis=0, keepdims=True)
                    cbuf[:, k * CHUNK:(k + 1) * CHUNK] = jnp.where(hot_, gk, 0.0).astype(BF)
                get(i, slot).wait()
                tn = min(1024, d)

                @loop(d // tn)
                def _(m):
                    cs = pl.ds(pl.multiple_of(m * tn, tn), tn)
                    z = zbuf[slot, :, cs]
                    acc[p * t:(p + 1) * t, cs] += dot(cbuf[:], jnp.concatenate([z, z, z], axis=0))

    if any(dense):
        for cp in ucp:
            cp.wait()
        tm = min(HM, t)

        @loop(n)
        def _(i):
            slot = parity(i)
            wait_expert(slot, own, bufs, sem)

            @pl.when(i + 1 < n)
            def _():
                fetch_expert(lax.rem(ent_ref[i + 1], nl), 1 - slot, own, other, bufs, sem)

            p, e = lax.div(ent_ref[i], nl), lax.rem(ent_ref[i], nl)
            blk = js[0]
            for q in range(1, nblk):
                blk = jnp.where(p == q, js[q], blk)

            @loop(t // tm)
            def _(m):
                rows = pl.ds(pl.multiple_of(p * t + m * tm, tm), tm)
                z = ffn(ubuf[rows, :], bufs[0][slot], bufs[1][slot], bufs[2][slot])
                g = gt_ref[blk, pl.ds(e, 1), pl.ds(pl.multiple_of(m * tm, tm), tm)]
                eye = lax.broadcasted_iota(I32, (tm, tm), 0) == lax.broadcasted_iota(I32, (tm, tm), 1)
                gc = jnp.sum(jnp.where(eye, g, 0.0), axis=1, keepdims=True)
                acc[rows, :] += gc * z.astype(F32)

    if outs[0].dtype == F32:
        done = [pltpu.make_async_copy(acc.at[pl.ds(p * t, t), :], outs[p], asem.at[p]) for p in range(nblk)]
        for cp in done:
            cp.start()
        for cp in done:
            cp.wait()
    else:
        for p in range(nblk):
            outs[p][:] = acc[p * t:(p + 1) * t, :].astype(BF)


def block(js, r, z, us, accs, own, other, dtype, dense, comb=True):
    nblk = len(js)
    t = r.pos.shape[2]
    d = own[0].shape[1]
    ff = own[0].shape[2]
    nl = r.pos.shape[1]
    vm = pl.BlockSpec(memory_space=pltpu.VMEM)
    sm = pl.BlockSpec(memory_space=pltpu.SMEM)
    hb = pl.BlockSpec(memory_space=pl.ANY)
    args, specs, scratch = [], [], []
    if any(dense):
        args += [r.hot.reshape(-1)]
        specs += [sm]
    args += [r.gt]
    specs += [vm]
    if comb:
        args += [r.nch, r.eg.reshape(-1), r.pos, z]
        specs += [sm, sm, vm, hb]
    if any(dense):
        args += list(us) + list(own) + list(other)
        specs += [hb] * (nblk + 7)
    args += [v for v in accs if v is not None]
    specs += [hb for v in accs if v is not None]
    scratch += [pltpu.VMEM((nblk * t, d), F32), pltpu.SemaphoreType.DMA((nblk,))]
    if comb:
        scratch += [pltpu.VMEM((t, 3 * CHUNK), BF), pltpu.VMEM((2, CHUNK, d), BF), DMA2]
    if any(dense):
        scratch += [*expert_buffers(d, ff),
                    pltpu.VMEM((nblk * t, d), BF), DMA2, pltpu.SemaphoreType.DMA,
                    pltpu.SMEM((nblk * nl,), I32)]
    out = jax.ShapeDtypeStruct((t, d), dtype)
    return pl.pallas_call(
        functools.partial(block_kernel, js, [v is not None for v in accs], comb, dense),
        in_specs=specs, out_specs=[hb if dtype == F32 else vm] * nblk, out_shape=[out] * nblk, scratch_shapes=scratch,
        compiler_params=params(),
        cost_estimate=cost(t * d, 6 * d * ff),
    )(*args)


def selection(j, i, eg_ref, pos_ref):
    t = pos_ref.shape[2]
    it = lax.broadcasted_iota(I32, (2 * PIECE, t), 0)
    npc = CHUNK // PIECE
    first = (j * (eg_ref.shape[0] // pos_ref.shape[0] // npc) + i) * npc
    ls = [eg_ref[first + q] for q in range(npc)]
    hits = []
    for q in range(0, npc, 2):
        own, nxt = [pos_ref[j, pl.ds(l, 1), :] for l in ls[q:q + 2]]
        hit = jnp.where(it < PIECE, own, nxt) - (i * CHUNK + q * PIECE) == it
        hits.append(jnp.where(hit, 1.0, 0.0).astype(BF))
    return jnp.concatenate(hits, axis=0), ls


def gather_rows(js, nch_ref, eg_ref, pos_ref, us, x_ref, ubuf, xbuf, usem, sem):
    cap = x_ref.shape[0] // pos_ref.shape[0]
    cps = [pltpu.make_async_copy(u, ubuf.at[p % 2], usem.at[p % 2]) for p, u in enumerate(us)]
    cps[0].start()

    def out(slot, row):
        return pltpu.make_async_copy(xbuf.at[slot], x_ref.at[pl.ds(pl.multiple_of(row, CHUNK), CHUNK), :], sem.at[slot])

    made = 0
    for p, j in enumerate(js):
        if p + 1 < len(js):
            cps[p + 1].start()
        cps[p].wait()

        @loop(nch_ref[j])
        def _(i):
            slot = parity(made + i)

            @pl.when(made + i >= 2)
            def _():
                out(slot, 0).wait()

            xbuf[slot] = dot(selection(j, i, eg_ref, pos_ref)[0], ubuf[p % 2]).astype(BF)
            out(slot, j * cap + i * CHUNK).start()

        made = made + nch_ref[j]
    for k in (2, 1):
        @pl.when(made >= k)
        def _():
            out(parity(made - k), 0).wait()


def gather_kernel(js, nch_ref, eg_ref, pos_ref, *refs):
    gather_rows(js, nch_ref, eg_ref, pos_ref, refs[:len(js)], *refs[len(js):])


def gather(js, r, us):
    t, d = us[0].shape
    vm = pl.BlockSpec(memory_space=pltpu.VMEM)
    sm = pl.BlockSpec(memory_space=pltpu.SMEM)
    hb = pl.BlockSpec(memory_space=pl.ANY)
    return pl.pallas_call(
        functools.partial(gather_kernel, js),
        in_specs=[sm, sm, vm] + [hb] * len(us),
        out_specs=hb,
        out_shape=jax.ShapeDtypeStruct((r.eg.size * PIECE, d), BF),
        scratch_shapes=[pltpu.VMEM((2, t, d), BF), pltpu.VMEM((2, CHUNK, d), BF), DMA2, DMA2],
        compiler_params=params(),
        cost_estimate=cost(t * d, 4 * CHUNK * d),
    )(r.nch, r.eg.reshape(-1), r.pos, *us)


def cold_kernel(js, np_ref, pc_ref, nch_ref, eg_ref, pos_ref, *refs):
    us, refs = refs[:len(js)], refs[len(js) + 1:]
    own, other, z_ref, refs = refs[:3], refs[3:7], refs[7], refs[8:]
    x_ref = z_ref
    bufs, (ubuf, gbuf, usem, gsem, xbuf, zbuf, wsem, xsem, zsem, tl_ref, tp_ref, tn_ref, tw_ref, nx_ref) = refs[:3], refs[3:]
    ppt = MT // PIECE

    def tiles(l, carry):
        q, turn, p = carry
        n = np_ref[l]
        more = lax.div(n + ppt - 1, ppt)

        @loop(more)
        def _(i):
            tl_ref[q + i] = l
            tp_ref[q + i] = p + i * ppt
            tn_ref[q + i] = jnp.minimum(n - i * ppt, ppt)
            tw_ref[q + i] = turn
            nx_ref[q + i] = jnp.where(i == 0, q + more, 0)

        return q + more, turn + jnp.minimum(n, 1), p + n

    nt = lax.fori_loop(0, np_ref.shape[0], tiles, (0, 0, 0))[0]

    def each(n, fn):
        @loop(lax.div(n, 2))
        def _(i):
            fn(2 * i)
            fn(2 * i + 1)

        @pl.when(parity(n) == 1)
        def _():
            fn(n - 1)

    def xin(q, slot):
        p0 = tp_ref[q]

        def one(i):
            src = pl.ds(pl.multiple_of(pc_ref[p0 + i] * PIECE, PIECE), PIECE)
            dst = pl.ds(pl.multiple_of(i * PIECE, PIECE), PIECE)
            pltpu.make_async_copy(x_ref.at[src, :], xbuf.at[slot, dst, :], xsem.at[slot]).start()

        each(tn_ref[q], one)

    def zout(q, slot):
        p0 = tp_ref[q]

        def one(i):
            src = pl.ds(pl.multiple_of(i * PIECE, PIECE), PIECE)
            dst = pl.ds(pl.multiple_of(pc_ref[p0 + i] * PIECE, PIECE), PIECE)
            pltpu.make_async_copy(zbuf.at[slot, src, :], z_ref.at[dst, :], zsem.at[slot]).start()

        each(tn_ref[q], one)

    def drain(n, fn):
        bit = 1
        while bit <= MT // PIECE:
            @pl.when(lax.rem(lax.div(n, bit), 2) == 1)
            def _(bit=bit):
                fn(pl.ds(0, bit * PIECE))

            bit *= 2

    def xwait(q, slot):
        drain(tn_ref[q], lambda r: pltpu.make_async_copy(x_ref.at[r, :], xbuf.at[slot, r, :], xsem.at[slot]).wait())

    def zwait(q, slot):
        drain(tn_ref[q], lambda r: pltpu.make_async_copy(zbuf.at[slot, r, :], z_ref.at[r, :], zsem.at[slot]).wait())

    @pl.when(nt > 0)
    def _():
        fetch_expert(tl_ref[0], 0, own, other, bufs, wsem)

    gather_rows(js, nch_ref, eg_ref, pos_ref, us, z_ref, ubuf, gbuf, usem, gsem)

    @pl.when(nt > 0)
    def _():
        xin(0, 0)

    @loop(nt)
    def _(q):
        slot = parity(q)
        ws = parity(tw_ref[q])

        @pl.when(nx_ref[q] > 0)
        def _():
            wait_expert(ws, own, bufs, wsem)

            @pl.when(nx_ref[q] < nt)
            def _():
                fetch_expert(tl_ref[nx_ref[q]], 1 - ws, own, other, bufs, wsem)

        @pl.when(q + 1 < nt)
        def _():
            xin(q + 1, 1 - slot)

        xwait(q, slot)

        @pl.when(q >= 2)
        def _():
            zwait(q - 2, slot)

        zbuf[slot] = ffn(xbuf[slot], bufs[0][ws], bufs[1][ws], bufs[2][ws])
        zout(q, slot)

    for k in (2, 1):
        @pl.when(nt >= k)
        def _():
            zwait(nt - k, parity(nt - k))


def cold(plan, js, r, us, x, own, other):
    d, ff = own[0].shape[1:]
    t = us[0].shape[0]
    vm = pl.BlockSpec(memory_space=pltpu.VMEM)
    sm = pl.BlockSpec(memory_space=pltpu.SMEM)
    hb = pl.BlockSpec(memory_space=pl.ANY)
    args = (*plan, r.nch, r.eg.reshape(-1), r.pos, *us)
    return pl.pallas_call(
        functools.partial(cold_kernel, js),
        in_specs=[sm] * 4 + [vm] + [hb] * (len(us) + 8),
        out_specs=hb,
        out_shape=jax.ShapeDtypeStruct(x.shape, BF),
        scratch_shapes=[*expert_buffers(d, ff), pltpu.VMEM((2, t, d), BF), pltpu.VMEM((2, CHUNK, d), BF), DMA2, DMA2,
                        pltpu.VMEM((2, MT, d), BF), pltpu.VMEM((2, MT, d), BF),
                        DMA2, DMA2, DMA2, *5 * [pltpu.SMEM((plan[1].size * PIECE // MT + plan[0].size + 1,), I32)]],
        input_output_aliases={len(args): 0},
        compiler_params=params(),
        cost_estimate=cost(6 * 16 * MT * d * ff, 96 * d * ff),
    )(*args, x, *own, *other)


def final_kernel(h_ref, *refs):
    y_ref = refs[-1]
    acc, parts = refs[0], refs[1:-1]
    y = h_ref[:].astype(F32) + acc[:]
    for v in parts:
        y = y + v[:].astype(F32)
    y_ref[:] = y.astype(BF)


def final(h, accs, parts):
    t, d = h.shape
    half = t // 2
    tm = min(256, half)
    n = half // tm

    def body(h_ref, *refs):
        for p in range(2):
            @pl.when(pl.program_id(0) // n == p)
            def _():
                final_kernel(h_ref, refs[p], *refs[2 + p:-1:2], refs[-1])

    spec = lambda p: pl.BlockSpec((tm, d), lambda i: (jnp.minimum(i, n - 1) if p == 0 else jnp.maximum(i - n, 0), 0))
    return pl.pallas_call(
        body, grid=(2 * n,),
        in_specs=[pl.BlockSpec((tm, d), lambda i: (i, 0))] + [spec(0), spec(1)] * (1 + len(parts)),
        out_specs=pl.BlockSpec((tm, d), lambda i: (i, 0)),
        out_shape=jax.ShapeDtypeStruct((t, d), BF),
        compiler_params=params(),
        cost_estimate=cost(6 * t * d, 20 * t * d),
    )(h, *accs, *[v for part in parts for v in part])


class Routing(typing.NamedTuple):
    hot: typing.Any
    nch: typing.Any
    eg: typing.Any
    pos: typing.Any
    gt: typing.Any


def routing_plan(lid, local, nl):
    nb, t, k = lid.shape
    le = jnp.arange(nl, dtype=I32)
    hit = jnp.any((lid[:, None] == le[:, None, None]) & local[:, None], axis=-1)
    tri = (jnp.arange(t)[:, None] <= jnp.arange(t)[None, :]).astype(BF)
    rank = lax.dot_general(hit.astype(BF), tri, (((2,), (0,)), ((), ())), preferred_element_type=F32).astype(I32)
    cnt = rank[:, :, -1]
    hotm = cnt >= t // 2
    scnt = jnp.where(hotm, 0, cnt)
    pcs = (scnt + PIECE - 1) // PIECE
    pend = jnp.cumsum(pcs, axis=1)
    base = (pend - pcs) * PIECE
    pos = jnp.where(hit & ~hotm[..., None], base[..., None] + rank - 1, -1)
    rows = t * k + nl * PIECE
    npb = -(-rows // CHUNK) * CHUNK // PIECE
    nch = jnp.maximum(-(-pend[:, -1] * PIECE // CHUNK), 1)
    below = lambda ends, q: jnp.sum((ends <= q).astype(I32), axis=-1)
    eg = jnp.minimum(below(pend[:, None, :], jnp.arange(npb, dtype=I32)[None, :, None]), nl - 1)
    flat = pcs.T.reshape(-1)
    fend = jnp.cumsum(flat)
    p = jnp.arange(nb * npb, dtype=I32)[:, None]
    seg = jnp.minimum(below(fend[None, :], p), nl * nb - 1)
    inseg = seg[:, None] == jnp.arange(nl * nb, dtype=I32)
    shift_ = jnp.tile(jnp.arange(nb, dtype=I32) * npb, nl) + (pend - pcs).T.reshape(-1) - (fend - flat)
    pc = jnp.clip(p[:, 0] + jnp.sum(jnp.where(inseg, shift_, 0), axis=1), 0, nb * npb - 1)
    return Routing(hotm.astype(I32), nch, eg, pos, None), (jnp.sum(pcs, axis=0), pc)


ON = (True,)


def solution(mesh):
    nd = mesh.shape['ep']
    nx = nd // 2
    tok_spec = P(('replica', 'ep'), None, None)
    rows_ep = P('ep', None)
    by_expert = P('ep', None, None)

    def shift(v, s):
        return lax.ppermute(v, 'ep', [(2 * i + c, 2 * ((i + s) % nx) + c) for i in range(nx) for c in range(2)])

    def local(x, wq, wk, wv, wo, wr, w1, w3, w2, idx):
        b, s, d = x.shape
        t, k, ne = b * s, idx.shape[-1], w1.shape[0]
        nl = 2 * ne
        half = t // 2
        me = lax.axis_index('ep')
        x = x.reshape(t, d)
        ids = idx.reshape(t, k)

        hd = HEAD // 2
        ang = (np.arange(t) % s).astype(np.float32)[:, None] * np.float32(THETA) ** (-np.arange(hd, dtype=np.float32) / hd)
        c, sn = np.cos(ang), np.sin(ang)
        cos, sin = [jnp.asarray(np.concatenate(v, axis=1), F32) for v in ((c, c), (-sn, sn))]
        h, ut, ub, o1, o3, o2, late, logits, ids4 = attention_layer(nx, x, wv, wk, wq, wo, cos, sin, w1, w3, w2, wr.T, ids.T)
        ids4 = jnp.swapaxes(ids4, 1, 2)
        late = lax.ppermute(late, 'ep', [(i, i ^ 1) for i in range(nd)])
        own, other = (w1, w3, w2), (o1, o3, o2, late)

        halves = lambda v: v.reshape(2 * v.shape[0], half, *v.shape[2:])
        is_local = halves(ids4 // nl == me // 2)
        lid = halves((ids4 - me * ne) % nl)
        r, plan = routing_plan(lid, is_local, nl)
        ohl = (lid[:, None] == jnp.arange(nl, dtype=I32)[:, None, None]) & is_local[:, None]

        u1t, u2b = shift(ut, 1), shift(ub, -1)
        oh = ids[..., None] == jnp.arange(wr.shape[1], dtype=I32)
        g = jax.nn.softmax(jnp.sum(jnp.where(oh, logits[:, None, :], 0.0), axis=-1), axis=-1)
        ut2, ub2, g = lax.optimization_barrier((ut, ub, g))
        g4 = [g, shift(g, 1), shift(g, -1), shift(g, 2)]
        u1b, u2t = shift(ub2, 1), shift(ut2, -1)
        spread = lambda o, v: jnp.sum(jnp.where(o, halves(v)[:, None], 0.0), axis=3)
        ra = r._replace(gt=spread(ohl[:2], g[None]))
        r = r._replace(gt=spread(ohl, jnp.stack(g4)))

        a0, = block((0,), ra, None, (ut,), (None,), own, other, F32, ON, comb=False)
        a0, u1t, u2b = lax.optimization_barrier((a0, u1t, u2b))
        u3t, u3b = shift(u1t, 1), shift(u2b, -1)
        d2, d5 = block((2, 5), r, None, (u1t, u2b), 2 * (None,), own, other, F32, 2 * ON, comb=False)
        u1b, d2 = lax.optimization_barrier((u1b, d2))
        x = gather(tuple(range(6)), r, [ut, ub, u1t, u1b, u2t, u2b])
        u3t, x = lax.optimization_barrier((u3t, x))
        z = cold(plan, (6, 7), r, [u3t, u3b], x, own, other)

        tie = lambda r, *v: (lambda w: (r._replace(nch=w[0]), *w[1:]))(lax.optimization_barrier((r.nch, *v)))
        b6, = block((6,), r, z, (u3t,), (None,), own, other, BF, ON)
        r, b6 = tie(r, b6)
        c6 = shift(b6, 1)
        b2, b5 = block((2, 5), r, z, (), (d2, d5), own, other, BF, (False, False))
        r, b2, b5 = tie(r, b2, b5)
        b2, b5 = shift(b2, -1), shift(b5, 1)
        b7, = block((7,), r, z, (u3b,), (None,), own, other, BF, ON)
        r, b7, c6 = tie(r, b7, c6)
        c7, b6 = shift(b7, -1), shift(c6, 1)
        b3, = block((3,), r, z, (u1b,), (None,), own, other, BF, ON)
        r, b3 = tie(r, b3)
        b3 = shift(b3, -1)
        b4, = block((4,), r, z, (u2t,), (None,), own, other, BF, ON)
        r, b4, c7 = tie(r, b4, c7)
        b4, b7 = shift(b4, 1), shift(c7, -1)
        accs = block((0, 1), r, z, (ut, ub), (a0, None), own, other, F32, (False, True))
        y = final(h, accs, [(b2, b3), (b4, b5), (b6, b7)])
        return y.reshape(b, s, d)

    return jax.shard_map(local, mesh=mesh,
                         in_specs=(tok_spec, rows_ep, rows_ep, rows_ep, rows_ep, P(None, None),
                                   by_expert, by_expert, by_expert, tok_spec),
                         out_specs=tok_spec, check_vma=False)
```

```python
import functools
import math
import typing
import jax
import jax.numpy as jnp
import numpy as np
from jax import lax
from jax.experimental import pallas as pl
from jax.experimental.pallas import tpu as pltpu
from jax.sharding import PartitionSpec as P

HEAD = 128
EPS = 1e-6
THETA = 10000.0
PIECE = 8
CHUNK = 256
MT = 352
HM = 512
VMEM = 66_000_000
BF, F32, I32 = jnp.bfloat16, jnp.float32, jnp.int32


def rmsnorm(v):
    v = v.astype(F32)
    return v * lax.rsqrt(jnp.mean(v * v, axis=-1, keepdims=True) + EPS)


def dot(a, b):
    return jnp.dot(a, b, preferred_element_type=F32)


NT = (((1,), (1,)), ((), ()))
TN = (((0,), (0,)), ((), ()))
DMA2 = pltpu.SemaphoreType.DMA((2,))


def cost(flops, bytes_):
    return pl.CostEstimate(flops=flops, bytes_accessed=bytes_, transcendentals=0)


def parity(i):
    return lax.rem(i, 2)


def expert_buffers(d, ff):
    return [pltpu.VMEM((2, *v), BF) for v in ((d, ff), (d, ff), (ff, d))]


def loop(n):
    return pl.loop(0, n)


def params(**kw):
    return pltpu.CompilerParams(vmem_limit_bytes=VMEM, **kw)


def split3(g):
    hi = g.astype(BF)
    r = g - hi.astype(F32)
    mid = r.astype(BF)
    lo = (r - mid.astype(F32)).astype(BF)
    return hi, mid, lo


LT, LB, RT, RB, OT, OB, PO, PASS = range(8)
LATE = 3
SWAPS = "41111111110022229"
MESH = pl.DeviceIdType.MESH


def layer_kernel(nx, x_ref, wv_ref, wk_ref, wq_ref, wo_ref, cos_ref, sin_ref, w1_ref, w3_ref, w2_ref, wr_ref, id_ref,
                 h_ref, ut_ref, ub_ref, o1_ref, o3_ref, o2_ref, late_ref, lg_ref, id4_ref,
                 w_ref, ab, qb, kb, vb, rb3, ssem, rsem, lsem, iosem, swap_send, swap_recv, id_send, id_recv):
    shards = (wv_ref, wk_ref, wq_ref, wo_ref)
    sh = wv_ref.shape[0]
    hs = sh // 2
    t, d = ab.shape
    me = lax.axis_index("ep")
    chip, core = me // 2, me % 2
    right, left, opp = [2 * ((chip + k) % nx) + core for k in (1, nx - 1, 2)]
    partner = 2 * chip + 1 - core

    barrier = pltpu.get_barrier_semaphore()
    around = (right, left, opp)
    for dev in (*around, partner):
        pl.semaphore_signal(barrier, inc=1, device_id={"ep": dev}, device_id_type=MESH)
    pl.semaphore_wait(barrier, 4)

    def rows(e, half=None):
        if half is None:
            return pl.ds(pl.multiple_of(e * sh, sh), sh)
        return pl.ds(pl.multiple_of(e * sh + half * hs, hs), hs)

    def remote(w, src, dst, dev, s, r):
        return pltpu.make_async_remote_copy(src_ref=src, dst_ref=w_ref.at[w, dst, :], send_sem=ssem.at[w, s],
                                            recv_sem=rsem.at[w, r], device_id={"ep": dev}, device_id_type=MESH)

    def own(w):
        src = shards[w]
        top, bot = src.at[pl.ds(0, hs), :], src.at[pl.ds(hs, hs), :]
        return [remote(w, top, rows(me, 0), right, 0, LT), remote(w, bot, rows(me, 1), left, 1, RB),
                remote(w, bot, rows(me, 1), right, 2, LB), remote(w, top, rows(me, 0), left, 3, RT),
                remote(w, src, rows(me), partner, 6, PO)]

    def mine(w):
        return pltpu.make_async_copy(shards[w], w_ref.at[w, rows(me), :], lsem.at[w])

    where = {LT: (left, 0), LB: (left, 1), RT: (right, 0), RB: (right, 1), OT: (opp, 0), OB: (opp, 1)}

    def onward(w, k):
        e, half = where[LT if k == OT else RB]
        return remote(w, w_ref.at[w, rows(e, half), :], rows(e, half), right if k == OT else left, 4 if k == OT else 5, k)

    def across(w, k):
        r = rows(*where[k])
        return remote(w, w_ref.at[w, r, :], r, partner, PASS + k, PASS + k)

    def arrive(w, k):
        r = rows(me) if k == PO else rows(*where[k % PASS])
        remote(w, w_ref.at[w, r, :], r, partner, 0, k).wait_recv()

    def begin(w):
        for c in own(w):
            c.start()
        mine(w).start()

    def stage_a(w):
        arrive(w, LT)
        onward(w, OT).start()
        arrive(w, RB)
        onward(w, OB).start()
        if w + 1 < 4:
            begin(w + 1)
        across(w, LT).start()
        across(w, RB).start()
        swap()

    def stage_b(w):
        for k in (LB, RT):
            arrive(w, k)
            across(w, k).start()
        swap()

    def stage_c(w):
        for k in (OT, OB):
            arrive(w, k)
            across(w, k).start()
        swap()

    def stage_d(w):
        for k in (PO, PASS + LT, PASS + RB, PASS + LB, PASS + RT, PASS + OT, PASS + OB):
            arrive(w, k)
        mine(w).wait()

    pieces = [(src.at[e], dst.at[e]) for e in range(w1_ref.shape[0]) for src, dst in ((w1_ref, o1_ref), (w3_ref, o3_ref), (w2_ref, o2_ref))
              if e < dst.shape[0]]
    swaps = [pltpu.make_async_remote_copy(src_ref=src, dst_ref=dst, send_sem=swap_send.at[i], recv_sem=swap_recv.at[i],
                                          device_id={"ep": partner}, device_id_type=MESH) for i, (src, dst) in enumerate(pieces)]
    waiting, quota = list(swaps), iter(SWAPS)

    def swap():
        for _ in range(min(int(next(quota)), len(waiting))):
            waiting.pop(0).start()

    ids = [pltpu.make_async_remote_copy(src_ref=id_ref, dst_ref=id4_ref.at[k + 1], send_sem=id_send.at[k], recv_sem=id_recv.at[k],
                                        device_id={"ep": dev}, device_id_type=MESH) for k, dev in enumerate(around)]
    ids.append(pltpu.make_async_copy(id_ref, id4_ref.at[0], id_send.at[3]))
    begin(0)
    for c in ids:
        c.start()
    swap()
    xin = pltpu.make_async_copy(x_ref, kb, iosem.at[0])
    xin.start()
    xin.wait()
    rb = min(256, t)
    rb3[:] = jnp.concatenate(split3(wr_ref[:]), axis=0)

    for e in range(LATE):
        room = w_ref.at[3, pl.ds(0, w2_ref.shape[1]), :]
        for c in (pltpu.make_async_copy(w2_ref.at[o2_ref.shape[0] + e], room, iosem.at[3]),
                  pltpu.make_async_copy(room, late_ref.at[e], iosem.at[3])):
            c.start()
            c.wait()

    @loop(t // rb)
    def _(i):
        r = pl.ds(pl.multiple_of(i * rb, rb), rb)
        ab[r, :] = rmsnorm(kb[r, :]).astype(BF)

    tm, tn = min(512, t), min(512, d)

    def project(w, dst, rope):
        @loop(d // tn)
        def _(n):
            @loop(t // tm)
            def _(m):
                r = pl.ds(pl.multiple_of(m * tm, tm), tm)
                z = dot(ab[r, :], w_ref[w, :, pl.ds(pl.multiple_of(n * tn, tn), tn)])
                for j in range(tn // HEAD):
                    zj = z[:, j * HEAD:(j + 1) * HEAD]
                    if rope:
                        zj = zj * cos_ref[r, :] + pltpu.roll(zj, HEAD // 2, 1) * sin_ref[r, :]
                    dst[r, pl.ds(pl.multiple_of(n * tn + j * HEAD, HEAD), HEAD)] = zj.astype(BF)

    for w, (dst, rope) in enumerate(((vb, False), (kb, True), (qb, True))):
        stage_a(w)
        stage_b(w)
        stage_c(w)
        stage_d(w)
        swap()
        project(w, dst, rope)
    stage_a(3)

    tq = min(256, t)
    scale = math.log2(math.e) / math.sqrt(HEAD)
    causal = lax.broadcasted_iota(I32, (tq, tq), 0) <= lax.broadcasted_iota(I32, (tq, tq), 1)
    group = min(4, d // HEAD)
    steps = d // HEAD // group
    marks = {1: stage_b, steps - 1: stage_c}
    if len(marks) > steps - 1:
        marks = {}
        stage_b(3)
        stage_c(3)

    @loop(steps)
    def _(jj):
        for at, stage in marks.items():
            pl.when(jj == at)(functools.partial(stage, 3))
        for j in range(group):
            c = pl.ds(pl.multiple_of((jj * group + j) * HEAD, HEAD), HEAD)
            for i in range(t // tq):
                r, n = slice(i * tq, (i + 1) * tq), (i + 1) * tq
                sc = lax.dot_general(kb[:n, c], qb[r, c], NT, preferred_element_type=F32)
                diag = jnp.where(causal, sc[i * tq:], -jnp.inf)
                sc = jnp.concatenate([sc[:i * tq], diag], axis=0) if i else diag
                p = jnp.exp2((sc - jnp.max(sc, axis=0, keepdims=True)) * scale)
                p = (p * (1.0 / jnp.sum(p, axis=0, keepdims=True))).astype(BF)
                qb[r, c] = lax.dot_general(p, vb[:n, c], TN, preferred_element_type=F32).astype(BF)

    swap()
    xin = pltpu.make_async_copy(x_ref, vb, iosem.at[0])
    xin.start()
    stage_d(3)
    xin.wait()

    @loop(d // tn)
    def _(n):
        c = pl.ds(pl.multiple_of(n * tn, tn), tn)

        @loop(t // tm)
        def _(m):
            r = pl.ds(pl.multiple_of(m * tm, tm), tm)
            ab[r, c] = (vb[r, c].astype(F32) + dot(qb[r, :], w_ref[3, :, c])).astype(BF)

    hout = pltpu.make_async_copy(ab, h_ref, iosem.at[0])
    hout.start()

    @loop(t // rb)
    def _(i):
        r = pl.ds(pl.multiple_of(i * rb, rb), rb)
        hi, mid, lo = split3(rmsnorm(ab[r, :]))
        kb[r, :] = hi
        ne = wr_ref.shape[0]
        part = lambda v, k: v[:, k * ne:(k + 1) * ne]
        p1, p2, p3 = [lax.dot_general(v, rb3[:n * ne], NT, preferred_element_type=F32) for v, n in ((hi, 3), (mid, 2), (lo, 1))]
        lg_ref[r, :] = part(p1, 0) + ((part(p1, 1) + part(p2, 0)) + (part(p1, 2) + part(p2, 1) + part(p3, 0)))

    uout = [pltpu.make_async_copy(kb.at[pl.ds(p * t // 2, t // 2), :], o, iosem.at[1 + p]) for p, o in enumerate((ut_ref, ub_ref))]
    for c in uout:
        c.start()
    assert not waiting
    for c in swaps + ids:
        c.wait()
    for w in range(4):
        for c in own(w) + [onward(w, OT), onward(w, OB)] + [across(w, k) for k in where]:
            c.wait_send()
    hout.wait()
    for c in uout:
        c.wait()


def attention_layer(nx, x, wv, wk, wq, wo, cos, sin, w1, w3, w2, wr, ids):
    t, d = x.shape
    hb = pl.BlockSpec(memory_space=pl.ANY)
    vm = pl.BlockSpec(memory_space=pltpu.VMEM)
    half = jax.ShapeDtypeStruct((t // 2, d), BF)
    act = pltpu.VMEM((t, d), BF)
    return pl.pallas_call(
        functools.partial(layer_kernel, nx),
        in_specs=[hb] * 5 + [vm] * 2 + [hb] * 3 + [vm, hb],
        out_specs=[hb] * 7 + [vm, hb],
        out_shape=[jax.ShapeDtypeStruct((t, d), BF), half, half, jax.ShapeDtypeStruct(w1.shape, BF),
                   jax.ShapeDtypeStruct(w3.shape, BF),
                   *[jax.ShapeDtypeStruct((n, *w2.shape[1:]), BF) for n in (w2.shape[0] - LATE, LATE)], jax.ShapeDtypeStruct((t, wr.shape[0]), F32),
                   jax.ShapeDtypeStruct((nx, *ids.shape), I32)],
        scratch_shapes=[pltpu.VMEM((4, d, d), BF), act, act, act, act, pltpu.VMEM((3 * wr.shape[0], d), BF),
                        pltpu.SemaphoreType.DMA((4, 13)), pltpu.SemaphoreType.DMA((4, 13)),
                        pltpu.SemaphoreType.DMA((4,)), pltpu.SemaphoreType.DMA((4,)),
                        pltpu.SemaphoreType.DMA((3 * w1.shape[0],)), pltpu.SemaphoreType.DMA((3 * w1.shape[0],)),
                        pltpu.SemaphoreType.DMA((nx,)), pltpu.SemaphoreType.DMA((nx,))],
        compiler_params=params(collective_id=0, has_side_effects=True),
        cost_estimate=cost(8 * t * d * d, 24 * t * d),
    )(x, wv, wk, wq, wo, cos, sin, w1, w3, w2, wr, ids)


def fetch_expert(l, slot, own, other, bufs, sem):
    ne, split = own[0].shape[0], other[2].shape[0]
    start = lambda src, dst: pltpu.make_async_copy(src, dst.at[slot], sem.at[slot]).start()

    @pl.when(l < ne)
    def _():
        for src, dst in zip(own, bufs):
            start(src.at[l], dst)

    @pl.when(l >= ne)
    def _():
        for src, dst in zip(other[:2], bufs):
            start(src.at[l - ne], dst)

    @pl.when(jnp.logical_and(l >= ne, l < ne + split))
    def _():
        start(other[2].at[l - ne], bufs[2])

    @pl.when(l >= ne + split)
    def _():
        start(other[3].at[l - ne - split], bufs[2])


def wait_expert(slot, own, bufs, sem):
    for src, dst in zip(own, bufs):
        pltpu.make_async_copy(src.at[0], dst.at[slot], sem.at[slot]).wait()


def ffn(x, w1, w3, w2):
    a1 = dot(x, w1)
    a3 = dot(x, w3)
    act = (jax.nn.silu(a1) * a3).astype(BF)
    return dot(act, w2).astype(BF)


def block_kernel(js, has_acc, comb, dense, *refs):
    refs = list(refs)
    nblk = len(js)
    take = lambda n: [refs.pop(0) for _ in range(n)]
    if any(dense):
        hot_ref, = take(1)
    gt_ref, = take(1)
    if comb:
        nch_ref, eg_ref, pos_ref, z_ref = take(4)
        cap = z_ref.shape[0] // pos_ref.shape[0]
    if any(dense):
        us = take(nblk)
        own, other = take(3), take(4)
        nl = 2 * own[0].shape[0]
    accs = [take(1)[0] if h else None for h in has_acc]
    outs = take(nblk)
    acc, asem = take(2)
    if comb:
        cbuf, zbuf, zsem = take(3)
    if any(dense):
        bufs, (ubuf, sem, usem, ent_ref) = take(3), take(4)
    t, d = outs[0].shape

    if any(dense):
        n = 0
        for p in range(nblk):
            def note(l, n, p=p):
                ent_ref[n] = p * nl + l
                return n + hot_ref[js[p] * nl + l]

            if dense[p]:
                n = lax.fori_loop(0, nl, note, n)

        @pl.when(n > 0)
        def _():
            fetch_expert(lax.rem(ent_ref[0], nl), 0, own, other, bufs, sem)

        ucp = [pltpu.make_async_copy(us[p], ubuf.at[pl.ds(p * t, t), :], usem) for p in range(nblk)]
        for cp in ucp:
            cp.start()
    for p in range(nblk):
        rows = pl.ds(p * t, t)
        if has_acc[p]:
            pltpu.make_async_copy(accs[p], acc.at[rows, :], asem.at[p]).start()
        else:
            acc[rows, :] = jnp.zeros((t, d), F32)
    for p in range(nblk):
        if has_acc[p]:
            pltpu.make_async_copy(accs[p], acc.at[pl.ds(p * t, t), :], asem.at[p]).wait()

    if comb:
        for p, j in enumerate(js):
            nch = nch_ref[j]

            def get(i, slot):
                src = pl.multiple_of(j * cap + i * CHUNK, CHUNK)
                return pltpu.make_async_copy(z_ref.at[pl.ds(src, CHUNK), :], zbuf.at[slot], zsem.at[slot])

            get(0, 0).start()
            nl = gt_ref.shape[1]
            lane = lax.broadcasted_iota(I32, (1, CHUNK), 1)
            ti = lax.broadcasted_iota(I32, (16, t), 1)
            si = lax.broadcasted_iota(I32, (16, t), 0)
            tparts = jnp.where(si == 0, ti % 256, jnp.where(si == 1, ti // 256, 0)).astype(F32).astype(BF)
            table = jnp.concatenate([*split3(gt_ref[j]), tparts], axis=0)

            @loop(nch)
            def _(i):
                slot = parity(i)

                @pl.when(i + 1 < nch)
                def _():
                    get(i + 1, 1 - slot).start()

                pm, ls = selection(j, i, eg_ref, pos_ref)
                el = jnp.zeros_like(lane)
                for q, l in enumerate(ls):
                    el = jnp.where(lane // PIECE == q, l, el)
                sel = lax.dot_general(table, pm, NT, preferred_element_type=F32)
                tok = (sel[3 * nl:3 * nl + 1] + 256.0 * sel[3 * nl + 1:3 * nl + 2]).astype(I32)
                hot_ = lax.broadcasted_iota(I32, (t, CHUNK), 0) == tok
                sub = lax.broadcasted_iota(I32, (nl, CHUNK), 0) == el
                for k in range(3):
                    gk = jnp.sum(jnp.where(sub, sel[k * nl:(k + 1) * nl], 0.0), axis=0, keepdims=True)
                    cbuf[:, k * CHUNK:(k + 1) * CHUNK] = jnp.where(hot_, gk, 0.0).astype(BF)
                get(i, slot).wait()
                tn = min(1024, d)

                @loop(d // tn)
                def _(m):
                    cs = pl.ds(pl.multiple_of(m * tn, tn), tn)
                    z = zbuf[slot, :, cs]
                    acc[p * t:(p + 1) * t, cs] += dot(cbuf[:], jnp.concatenate([z, z, z], axis=0))

    if any(dense):
        for cp in ucp:
            cp.wait()
        tm = min(HM, t)

        @loop(n)
        def _(i):
            slot = parity(i)
            wait_expert(slot, own, bufs, sem)

            @pl.when(i + 1 < n)
            def _():
                fetch_expert(lax.rem(ent_ref[i + 1], nl), 1 - slot, own, other, bufs, sem)

            p, e = lax.div(ent_ref[i], nl), lax.rem(ent_ref[i], nl)
            blk = js[0]
            for q in range(1, nblk):
                blk = jnp.where(p == q, js[q], blk)

            @loop(t // tm)
            def _(m):
                rows = pl.ds(pl.multiple_of(p * t + m * tm, tm), tm)
                z = ffn(ubuf[rows, :], bufs[0][slot], bufs[1][slot], bufs[2][slot])
                g = gt_ref[blk, pl.ds(e, 1), pl.ds(pl.multiple_of(m * tm, tm), tm)]
                eye = lax.broadcasted_iota(I32, (tm, tm), 0) == lax.broadcasted_iota(I32, (tm, tm), 1)
                gc = jnp.sum(jnp.where(eye, g, 0.0), axis=1, keepdims=True)
                acc[rows, :] += gc * z.astype(F32)

    if outs[0].dtype == F32:
        done = [pltpu.make_async_copy(acc.at[pl.ds(p * t, t), :], outs[p], asem.at[p]) for p in range(nblk)]
        for cp in done:
            cp.start()
        for cp in done:
            cp.wait()
    else:
        for p in range(nblk):
            outs[p][:] = acc[p * t:(p + 1) * t, :].astype(BF)


def block(js, r, z, us, accs, own, other, dtype, dense, comb=True):
    nblk = len(js)
    t = r.pos.shape[2]
    d = own[0].shape[1]
    ff = own[0].shape[2]
    nl = r.pos.shape[1]
    vm = pl.BlockSpec(memory_space=pltpu.VMEM)
    sm = pl.BlockSpec(memory_space=pltpu.SMEM)
    hb = pl.BlockSpec(memory_space=pl.ANY)
    args, specs, scratch = [], [], []
    if any(dense):
        args += [r.hot.reshape(-1)]
        specs += [sm]
    args += [r.gt]
    specs += [vm]
    if comb:
        args += [r.nch, r.eg.reshape(-1), r.pos, z]
        specs += [sm, sm, vm, hb]
    if any(dense):
        args += list(us) + list(own) + list(other)
        specs += [hb] * (nblk + 7)
    args += [v for v in accs if v is not None]
    specs += [hb for v in accs if v is not None]
    scratch += [pltpu.VMEM((nblk * t, d), F32), pltpu.SemaphoreType.DMA((nblk,))]
    if comb:
        scratch += [pltpu.VMEM((t, 3 * CHUNK), BF), pltpu.VMEM((2, CHUNK, d), BF), DMA2]
    if any(dense):
        scratch += [*expert_buffers(d, ff),
                    pltpu.VMEM((nblk * t, d), BF), DMA2, pltpu.SemaphoreType.DMA,
                    pltpu.SMEM((nblk * nl,), I32)]
    out = jax.ShapeDtypeStruct((t, d), dtype)
    return pl.pallas_call(
        functools.partial(block_kernel, js, [v is not None for v in accs], comb, dense),
        in_specs=specs, out_specs=[hb if dtype == F32 else vm] * nblk, out_shape=[out] * nblk, scratch_shapes=scratch,
        compiler_params=params(),
        cost_estimate=cost(t * d, 6 * d * ff),
    )(*args)


def selection(j, i, eg_ref, pos_ref):
    t = pos_ref.shape[2]
    it = lax.broadcasted_iota(I32, (2 * PIECE, t), 0)
    npc = CHUNK // PIECE
    first = (j * (eg_ref.shape[0] // pos_ref.shape[0] // npc) + i) * npc
    ls = [eg_ref[first + q] for q in range(npc)]
    hits = []
    for q in range(0, npc, 2):
        own, nxt = [pos_ref[j, pl.ds(l, 1), :] for l in ls[q:q + 2]]
        hit = jnp.where(it < PIECE, own, nxt) - (i * CHUNK + q * PIECE) == it
        hits.append(jnp.where(hit, 1.0, 0.0).astype(BF))
    return jnp.concatenate(hits, axis=0), ls


def gather_rows(js, nch_ref, eg_ref, pos_ref, us, x_ref, ubuf, xbuf, usem, sem):
    cap = x_ref.shape[0] // pos_ref.shape[0]
    cps = [pltpu.make_async_copy(u, ubuf.at[p % 2], usem.at[p % 2]) for p, u in enumerate(us)]
    cps[0].start()

    def out(slot, row):
        return pltpu.make_async_copy(xbuf.at[slot], x_ref.at[pl.ds(pl.multiple_of(row, CHUNK), CHUNK), :], sem.at[slot])

    made = 0
    for p, j in enumerate(js):
        if p + 1 < len(js):
            cps[p + 1].start()
        cps[p].wait()

        @loop(nch_ref[j])
        def _(i):
            slot = parity(made + i)

            @pl.when(made + i >= 2)
            def _():
                out(slot, 0).wait()

            xbuf[slot] = dot(selection(j, i, eg_ref, pos_ref)[0], ubuf[p % 2]).astype(BF)
            out(slot, j * cap + i * CHUNK).start()

        made = made + nch_ref[j]
    for k in (2, 1):
        @pl.when(made >= k)
        def _():
            out(parity(made - k), 0).wait()


def gather_kernel(js, nch_ref, eg_ref, pos_ref, *refs):
    gather_rows(js, nch_ref, eg_ref, pos_ref, refs[:len(js)], *refs[len(js):])


def gather(js, r, us):
    t, d = us[0].shape
    vm = pl.BlockSpec(memory_space=pltpu.VMEM)
    sm = pl.BlockSpec(memory_space=pltpu.SMEM)
    hb = pl.BlockSpec(memory_space=pl.ANY)
    return pl.pallas_call(
        functools.partial(gather_kernel, js),
        in_specs=[sm, sm, vm] + [hb] * len(us),
        out_specs=hb,
        out_shape=jax.ShapeDtypeStruct((r.eg.size * PIECE, d), BF),
        scratch_shapes=[pltpu.VMEM((2, t, d), BF), pltpu.VMEM((2, CHUNK, d), BF), DMA2, DMA2],
        compiler_params=params(),
        cost_estimate=cost(t * d, 4 * CHUNK * d),
    )(r.nch, r.eg.reshape(-1), r.pos, *us)


def cold_kernel(js, np_ref, pc_ref, nch_ref, eg_ref, pos_ref, *refs):
    us, refs = refs[:len(js)], refs[len(js) + 1:]
    own, other, z_ref, refs = refs[:3], refs[3:7], refs[7], refs[8:]
    x_ref = z_ref
    bufs, (ubuf, gbuf, usem, gsem, xbuf, zbuf, wsem, xsem, zsem, tl_ref, tp_ref, tn_ref, tw_ref, nx_ref) = refs[:3], refs[3:]
    ppt = MT // PIECE

    def tiles(l, carry):
        q, turn, p = carry
        n = np_ref[l]
        more = lax.div(n + ppt - 1, ppt)

        @loop(more)
        def _(i):
            tl_ref[q + i] = l
            tp_ref[q + i] = p + i * ppt
            tn_ref[q + i] = jnp.minimum(n - i * ppt, ppt)
            tw_ref[q + i] = turn
            nx_ref[q + i] = jnp.where(i == 0, q + more, 0)

        return q + more, turn + jnp.minimum(n, 1), p + n

    nt = lax.fori_loop(0, np_ref.shape[0], tiles, (0, 0, 0))[0]

    def each(n, fn):
        whole = lax.div(n, 4)

        @loop(whole)
        def _(i):
            for k in range(4):
                fn(4 * i + k)

        pl.loop(4 * whole, n)(fn)

    def xin(q, slot):
        p0 = tp_ref[q]

        def one(i):
            src = pl.ds(pl.multiple_of(pc_ref[p0 + i] * PIECE, PIECE), PIECE)
            dst = pl.ds(pl.multiple_of(i * PIECE, PIECE), PIECE)
            pltpu.make_async_copy(x_ref.at[src, :], xbuf.at[slot, dst, :], xsem.at[slot]).start()

        each(tn_ref[q], one)

    def zout(q, slot):
        p0 = tp_ref[q]

        def one(i):
            src = pl.ds(pl.multiple_of(i * PIECE, PIECE), PIECE)
            dst = pl.ds(pl.multiple_of(pc_ref[p0 + i] * PIECE, PIECE), PIECE)
            pltpu.make_async_copy(zbuf.at[slot, src, :], z_ref.at[dst, :], zsem.at[slot]).start()

        each(tn_ref[q], one)

    def drain(n, fn):
        bit = 1
        while bit <= MT // PIECE:
            @pl.when(lax.rem(lax.div(n, bit), 2) == 1)
            def _(bit=bit):
                fn(pl.ds(0, bit * PIECE))

            bit *= 2

    def xwait(q, slot):
        drain(tn_ref[q], lambda r: pltpu.make_async_copy(x_ref.at[r, :], xbuf.at[slot, r, :], xsem.at[slot]).wait())

    def zwait(q, slot):
        drain(tn_ref[q], lambda r: pltpu.make_async_copy(zbuf.at[slot, r, :], z_ref.at[r, :], zsem.at[slot]).wait())

    @pl.when(nt > 0)
    def _():
        fetch_expert(tl_ref[0], 0, own, other, bufs, wsem)

    gather_rows(js, nch_ref, eg_ref, pos_ref, us, z_ref, ubuf, gbuf, usem, gsem)

    @pl.when(nt > 0)
    def _():
        xin(0, 0)

    @loop(nt)
    def _(q):
        slot = parity(q)
        ws = parity(tw_ref[q])

        @pl.when(nx_ref[q] > 0)
        def _():
            wait_expert(ws, own, bufs, wsem)

            @pl.when(nx_ref[q] < nt)
            def _():
                fetch_expert(tl_ref[nx_ref[q]], 1 - ws, own, other, bufs, wsem)

        @pl.when(q + 1 < nt)
        def _():
            xin(q + 1, 1 - slot)

        xwait(q, slot)

        @pl.when(q >= 2)
        def _():
            zwait(q - 2, slot)

        zbuf[slot] = ffn(xbuf[slot], bufs[0][ws], bufs[1][ws], bufs[2][ws])
        zout(q, slot)

    for k in (2, 1):
        @pl.when(nt >= k)
        def _():
            zwait(nt - k, parity(nt - k))


def cold(plan, js, r, us, x, own, other):
    d, ff = own[0].shape[1:]
    t = us[0].shape[0]
    vm = pl.BlockSpec(memory_space=pltpu.VMEM)
    sm = pl.BlockSpec(memory_space=pltpu.SMEM)
    hb = pl.BlockSpec(memory_space=pl.ANY)
    args = (*plan, r.nch, r.eg.reshape(-1), r.pos, *us)
    return pl.pallas_call(
        functools.partial(cold_kernel, js),
        in_specs=[sm] * 4 + [vm] + [hb] * (len(us) + 8),
        out_specs=hb,
        out_shape=jax.ShapeDtypeStruct(x.shape, BF),
        scratch_shapes=[*expert_buffers(d, ff), pltpu.VMEM((2, t, d), BF), pltpu.VMEM((2, CHUNK, d), BF), DMA2, DMA2,
                        pltpu.VMEM((2, MT, d), BF), pltpu.VMEM((2, MT, d), BF),
                        DMA2, DMA2, DMA2, *5 * [pltpu.SMEM((plan[1].size * PIECE // MT + plan[0].size + 1,), I32)]],
        input_output_aliases={len(args): 0},
        compiler_params=params(),
        cost_estimate=cost(6 * 16 * MT * d * ff, 96 * d * ff),
    )(*args, x, *own, *other)


def final_kernel(h_ref, *refs):
    y_ref = refs[-1]
    half = refs[0].shape[0]
    for p in range(2):
        rows = pl.ds(p * half, half)
        y = h_ref[rows, :].astype(F32)
        for v in refs[p:-1:2]:
            y = y + v[:].astype(F32)
        y_ref[rows, :] = y.astype(BF)


def final(h, accs, parts):
    t, d = h.shape
    tn = min(256, d)
    cols = lambda rows: pl.BlockSpec((rows, tn), lambda i: (0, i))
    args = [*accs, *[v for part in parts for v in part]]
    return pl.pallas_call(
        final_kernel, grid=(d // tn,),
        in_specs=[cols(t)] + [cols(t // 2)] * len(args),
        out_specs=cols(t),
        out_shape=jax.ShapeDtypeStruct((t, d), BF),
        compiler_params=params(),
        cost_estimate=cost(6 * t * d, 20 * t * d),
    )(h, *args)


class Routing(typing.NamedTuple):
    hot: typing.Any
    nch: typing.Any
    eg: typing.Any
    pos: typing.Any
    gt: typing.Any


def routing_plan(lid, local, nl):
    nb, t, k = lid.shape
    le = jnp.arange(nl, dtype=I32)
    hit = jnp.any((lid[:, None] == le[:, None, None]) & local[:, None], axis=-1)
    tri = (jnp.arange(t)[:, None] <= jnp.arange(t)[None, :]).astype(BF)
    rank = lax.dot_general(hit.astype(BF), tri, (((2,), (0,)), ((), ())), preferred_element_type=F32).astype(I32)
    cnt = rank[:, :, -1]
    hotm = cnt >= t // 2
    scnt = jnp.where(hotm, 0, cnt)
    pcs = (scnt + PIECE - 1) // PIECE
    pend = jnp.cumsum(pcs, axis=1)
    base = (pend - pcs) * PIECE
    pos = jnp.where(hit & ~hotm[..., None], base[..., None] + rank - 1, -1)
    rows = t * k + nl * PIECE
    npb = -(-rows // CHUNK) * CHUNK // PIECE
    nch = jnp.maximum(-(-pend[:, -1] * PIECE // CHUNK), 1)
    below = lambda ends, q: jnp.sum((ends <= q).astype(I32), axis=-1)
    eg = jnp.minimum(below(pend[:, None, :], jnp.arange(npb, dtype=I32)[None, :, None]), nl - 1)
    flat = pcs.T.reshape(-1)
    fend = jnp.cumsum(flat)
    p = jnp.arange(nb * npb, dtype=I32)[:, None]
    seg = jnp.minimum(below(fend[None, :], p), nl * nb - 1)
    inseg = seg[:, None] == jnp.arange(nl * nb, dtype=I32)
    shift_ = jnp.tile(jnp.arange(nb, dtype=I32) * npb, nl) + (pend - pcs).T.reshape(-1) - (fend - flat)
    pc = jnp.clip(p[:, 0] + jnp.sum(jnp.where(inseg, shift_, 0), axis=1), 0, nb * npb - 1)
    return Routing(hotm.astype(I32), nch, eg, pos, None), (jnp.sum(pcs, axis=0), pc)


ON = (True,)


def solution(mesh):
    nd = mesh.shape['ep']
    nx = nd // 2
    tok_spec = P(('replica', 'ep'), None, None)
    rows_ep = P('ep', None)
    by_expert = P('ep', None, None)

    def shift(v, s):
        return lax.ppermute(v, 'ep', [(2 * i + c, 2 * ((i + s) % nx) + c) for i in range(nx) for c in range(2)])

    def local(x, wq, wk, wv, wo, wr, w1, w3, w2, idx):
        b, s, d = x.shape
        t, k, ne = b * s, idx.shape[-1], w1.shape[0]
        nl = 2 * ne
        half = t // 2
        me = lax.axis_index('ep')
        x = x.reshape(t, d)
        ids = idx.reshape(t, k)

        hd = HEAD // 2
        ang = (np.arange(t) % s).astype(np.float32)[:, None] * np.float32(THETA) ** (-np.arange(hd, dtype=np.float32) / hd)
        c, sn = np.cos(ang), np.sin(ang)
        cos, sin = [jnp.asarray(np.concatenate(v, axis=1), F32) for v in ((c, c), (-sn, sn))]
        h, ut, ub, o1, o3, o2, late, logits, ids4 = attention_layer(nx, x, wv, wk, wq, wo, cos, sin, w1, w3, w2, wr.T, ids.T)
        ids4 = jnp.swapaxes(ids4, 1, 2)
        late = lax.ppermute(late, 'ep', [(i, i ^ 1) for i in range(nd)])
        own, other = (w1, w3, w2), (o1, o3, o2, late)

        halves = lambda v: v.reshape(2 * v.shape[0], half, *v.shape[2:])
        is_local = halves(ids4 // nl == me // 2)
        lid = halves((ids4 - me * ne) % nl)
        r, plan = routing_plan(lid, is_local, nl)
        ohl = (lid[:, None] == jnp.arange(nl, dtype=I32)[:, None, None]) & is_local[:, None]

        u1t, u2b = shift(ut, 1), shift(ub, -1)
        oh = ids[..., None] == jnp.arange(wr.shape[1], dtype=I32)
        g = jax.nn.softmax(jnp.sum(jnp.where(oh, logits[:, None, :], 0.0), axis=-1), axis=-1)
        ut2, ub2, g = lax.optimization_barrier((ut, ub, g))
        g4 = [g, shift(g, 1), shift(g, -1), shift(g, 2)]
        u1b, u2t = shift(ub2, 1), shift(ut2, -1)
        spread = lambda o, v: jnp.sum(jnp.where(o, halves(v)[:, None], 0.0), axis=3)
        ra = r._replace(gt=spread(ohl[:2], g[None]))
        r = r._replace(gt=spread(ohl, jnp.stack(g4)))

        a0, = block((0,), ra, None, (ut,), (None,), own, other, F32, ON, comb=False)
        a0, u1t, u2b = lax.optimization_barrier((a0, u1t, u2b))
        u3t, u3b = shift(u1t, 1), shift(u2b, -1)
        d2, d5 = block((2, 5), r, None, (u1t, u2b), 2 * (None,), own, other, F32, 2 * ON, comb=False)
        u1b, d2 = lax.optimization_barrier((u1b, d2))
        x = gather(tuple(range(6)), r, [ut, ub, u1t, u1b, u2t, u2b])
        u3t, x = lax.optimization_barrier((u3t, x))
        z = cold(plan, (6, 7), r, [u3t, u3b], x, own, other)

        tie = lambda r, *v: (lambda w: (r._replace(nch=w[0]), *w[1:]))(lax.optimization_barrier((r.nch, *v)))
        b6, = block((6,), r, z, (u3t,), (None,), own, other, BF, ON)
        r, b6 = tie(r, b6)
        c6 = shift(b6, 1)
        b2, b5 = block((2, 5), r, z, (), (d2, d5), own, other, BF, (False, False))
        r, b2, b5 = tie(r, b2, b5)
        b2, b5 = shift(b2, -1), shift(b5, 1)
        b7, = block((7,), r, z, (u3b,), (None,), own, other, BF, ON)
        r, b7, c6 = tie(r, b7, c6)
        c7, b6 = shift(b7, -1), shift(c6, 1)
        b3, = block((3,), r, z, (u1b,), (None,), own, other, BF, ON)
        r, b3 = tie(r, b3)
        b3 = shift(b3, -1)
        b4, = block((4,), r, z, (u2t,), (None,), own, other, BF, ON)
        r, b4, c7 = tie(r, b4, c7)
        b4, b7 = shift(b4, 1), shift(c7, -1)
        accs = block((0, 1), r, z, (ut, ub), (a0, None), own, other, F32, (False, True))
        y = final(h, accs, [(b2, b3), (b4, b5), (b6, b7)])
        return y.reshape(b, s, d)

    return jax.shard_map(local, mesh=mesh,
                         in_specs=(tok_spec, rows_ep, rows_ep, rows_ep, rows_ep, P(None, None),
                                   by_expert, by_expert, by_expert, tok_spec),
                         out_specs=tok_spec, check_vma=False)
```
